32 devices in a mesh: cells: 8 (over z, y), grp: 4 (over x, core).
Axes of the slice: x: 2, y: 2, z: 4, core: 2. Of those that a mesh axis runs over, the one named last changes fastest.
Arguments:
- latent_coordinates: float32 [50, 131072], P(None, ('cells', 'grp')), may hold values from -40 to 40
- group_means: float32 [16, 50], replicated, may hold values from -4 to 4
- entropy_scaling: float32 [16], replicated, may hold values from 0.5 to 2
- sample_shrinkage_lambda: float32 [200], replicated, may hold values from 164 to 1310
- sample_population: int32 [200], replicated, may hold values from 1 to 1310, 131072 in all
Outputs:
- corrected: float32 [50, 131072], P(None, ('cells', 'grp'))
- new_centroids: float32 [16, 50], P('cells')
The draws below stay inside these ranges and needn't reach their ends.
All inputs are finite; a program needn't handle non-finite values.
Results may differ from the reference program's by a relative error of at most 0.0003.
Values sent between devices are 32-bit elements; how exact they have to be, the bound alone decides.
No kernel may reach another device: no remote copies, remote signals or barrier semaphores. Data moves between devices by JAX's collectives and lax.ppermute only.
A program may use at most 64 MiB of HBM per device.

```python
import math
import jax
import jax.numpy as jnp
import numpy as np
from jax import lax

PCS = 50
GROUP_NUMBER = 16
NB = 200
CELLS = 131072
MOST = 1310


def centre_table(key):
    table = jax.random.normal(jax.random.fold_in(key, 11), (GROUP_NUMBER, PCS), jnp.float32) * 0.5
    return table


def draw_group_means(key, part):
    return jnp.clip(centre_table(key), -4.0, 4.0)


def draw_latent_coordinates(key, part):
    region_len = CELLS // NB
    shifts = jax.random.normal(jax.random.fold_in(key, 2), (PCS, NB + 1), jnp.float32)
    region = jnp.minimum(jnp.arange(CELLS) // region_len, NB)
    offset = shifts[:, region]
    noise = jax.random.normal(jax.random.fold_in(key, 1), (PCS, CELLS), jnp.float32)
    values = noise + offset
    return jnp.clip(values, -40.0, 40.0)


def split_up(count, total, most, skew):
    portions = [(1 << 20) // math.isqrt(rank ** skew) + 1 for rank in range(2, count + 1)]
    rest, given = total - most - (count - 1), [1] * (count - 1)
    while rest > 0:
        movable = [i for i in range(count - 1) if given[i] < most]
        whole, remaining = sum([portions[i] for i in movable]), rest
        for i in movable:
            more = min(most - given[i], max(1, remaining * portions[i] // whole), rest)
            given[i] = given[i] + more
            rest = rest - more
    return np.array([most] + given)


def ragged(rng, count, total, limit, lean):
    if count == 2:
        one = jax.random.randint(rng, (), max(1, total - limit), min(limit, total - 1) + 1)
        return jnp.stack([one, total - one])
    tallies = jnp.asarray(split_up(count, total, limit, lean), jnp.int32)
    twos = (count - 1) // 2
    giver, receiver = tallies[1:1 + 2 * twos:2], tallies[2:2 + 2 * twos:2]
    slack = jnp.minimum(giver - 1, limit - receiver)
    shifted = jax.random.randint(jax.random.fold_in(rng, 1), (twos,), 0, 1 << 20) % (slack + 1)
    tallies = tallies.at[1:1 + 2 * twos:2].set(giver - shifted).at[2:2 + 2 * twos:2].set(receiver + shifted)
    return tallies[jax.random.permutation(jax.random.fold_in(rng, 2), count)]


def setup_inputs(seed: int = 0) -> dict:
    key_list = jax.random.split(jax.random.key(seed), 6)
    latent_coordinates = draw_latent_coordinates(jax.random.fold_in(key_list[5], 71), 0)
    group_means = draw_group_means(jax.random.fold_in(key_list[5], 71), 0)
    entropy_scaling = jnp.clip(jnp.exp(jax.random.uniform(key_list[2], (GROUP_NUMBER,), jnp.float32, math.log(0.5), math.log(2.0))), 0.5, 2.0)
    sample_shrinkage_lambda = jnp.clip(jnp.exp(jax.random.uniform(key_list[3], (NB,), jnp.float32, math.log(164.0), math.log(1310.0))), 164.0, 1310.0)
    sample_population = ragged(key_list[4], NB, CELLS, MOST, 2).astype(jnp.int32)
    return {"latent_coordinates": latent_coordinates, "group_means": group_means, "entropy_scaling": entropy_scaling, "sample_shrinkage_lambda": sample_shrinkage_lambda, "sample_population": sample_population}


diversity = 2.0
intercept_ridge = 1.0
highest = lax.Precision.HIGHEST


def observation_affinity(latent_coordinates, group_means, entropy_scaling):
    pairwise_dots = jnp.dot(group_means, latent_coordinates, precision=highest, preferred_element_type=jnp.float32)
    quadratic_lengths = jnp.sum(group_means * group_means, axis=1)
    return (2.0 * pairwise_dots - quadratic_lengths[:, None]) / (2.0 * entropy_scaling[:, None])


def probabilistic_responsibility(group_affinity):
    top = jnp.max(group_affinity, axis=0, keepdims=True)
    raised = jnp.exp(group_affinity - top)
    return raised / jnp.sum(raised, axis=0, keepdims=True)


def reference(latent_coordinates, group_means, entropy_scaling, sample_shrinkage_lambda, sample_population):
    cells_total = latent_coordinates.shape[1]
    batch_ends = jnp.cumsum(sample_population).astype(jnp.int32)
    batch_starts = (batch_ends - sample_population).astype(jnp.int32)
    padded = jnp.pad(latent_coordinates, ((0, 0), (0, MOST)))
    window = lax.iota(jnp.int32, MOST)

    def batch_cells(start, size):
        contiguous_portion = lax.dynamic_slice(padded, (jnp.int32(0), start), (PCS, MOST))
        inside = (window < size).astype(jnp.float32)
        return contiguous_portion, inside

    def count_step(carry, item):
        start, size = item
        contiguous_portion, inside = batch_cells(start, size)
        expected_occupancy = probabilistic_responsibility(observation_affinity(contiguous_portion, group_means, entropy_scaling))
        return carry, jnp.sum(expected_occupancy * inside[None, :], axis=1)

    unused, counts_t = lax.scan(count_step, jnp.float32(0.0), (batch_starts, sample_population))
    counts = counts_t.T
    totals = jnp.sum(counts, axis=1)
    expected = sample_population.astype(jnp.float32)[None, :] * totals[:, None] / jnp.float32(cells_total)
    penalty = diversity * jnp.log((counts + 1.0) / (expected + 1.0))

    def assign_of(contiguous_portion, single_observation):
        return probabilistic_responsibility(observation_affinity(contiguous_portion, group_means, entropy_scaling) - single_observation[:, None])

    def moment_step(carry, item):
        start, size, single_observation = item
        contiguous_portion, inside = batch_cells(start, size)
        assign = assign_of(contiguous_portion, single_observation) * inside[None, :]
        augmented = jnp.concatenate([jnp.ones((1, MOST), jnp.float32), contiguous_portion], axis=0)
        return carry, jnp.einsum("kn,dn->kd", assign, augmented, precision=highest)

    unused, moments_t = lax.scan(moment_step, jnp.float32(0.0), (batch_starts, sample_population, penalty.T))
    moments = jnp.transpose(moments_t, (1, 2, 0))
    mass = moments[:, 0, :]
    sums = moments[:, 1:, :]
    shrink = sample_shrinkage_lambda[None, :] / (mass + sample_shrinkage_lambda[None, :])
    weight = jnp.sum(mass * shrink, axis=1)
    right_side = jnp.sum(sums * shrink[:, None, :], axis=2)
    intercept = right_side / (intercept_ridge + weight)[:, None]
    coefficients = (sums - mass[:, None, :] * intercept[:, :, None]) / (mass + sample_shrinkage_lambda[None, :])[:, None, :]
    new_centroids = jnp.sum(sums, axis=2) / (1.0 + jnp.sum(mass, axis=1))[:, None]

    def correct_step(carry, item):
        start, size, single_observation, coef = item
        contiguous_portion, inside = batch_cells(start, size)
        assign = assign_of(contiguous_portion, single_observation) * inside[None, :]
        moved = jnp.einsum("kd,kn->dn", coef, assign, precision=highest)
        current = lax.dynamic_slice(carry, (jnp.int32(0), start), (PCS, MOST))
        fresh = jnp.where(inside[None, :] > 0.0, contiguous_portion - moved, current)
        return lax.dynamic_update_slice(carry, fresh, (jnp.int32(0), start)), jnp.float32(0.0)

    result, unused = lax.scan(correct_step, padded, (batch_starts, sample_population, penalty.T, jnp.transpose(coefficients, (2, 0, 1))))
    return result[:, :cells_total], new_centroids
```

```python
import jax
import jax.numpy as jnp
from jax import lax
from jax.experimental import pallas as pl
from jax.experimental.pallas import tpu as pltpu
from jax.sharding import PartitionSpec as P

f32 = jnp.float32
bf16 = jnp.bfloat16
HALF = 64
LANES = 128
AXES = ("cells", "grp")


def split(value):
    high = value.astype(bf16)
    return high, (value - high.astype(f32)).astype(bf16)


def iota(shape, axis):
    return lax.broadcasted_iota(jnp.int32, shape, axis)


def lane_of(value, lane):
    return jnp.broadcast_to(value[:, lane : lane + 1], value.shape)


def halves(value, lane):
    left = iota(value.shape, 1) < HALF
    return jnp.where(left, lane_of(value, lane), lane_of(value, HALF + lane))


def column(row, first, count):
    shape = (count, row.shape[1])
    pick = iota(shape, 1) == iota(shape, 0) + first
    return jnp.sum(jnp.where(pick, jnp.broadcast_to(row, shape), 0.0), axis=1, keepdims=True)


def pack_pairs(ref):
    pairs = ref.shape[0] // 2
    even = ref[pl.ds(0, pairs, stride=2), :]
    odd = ref[pl.ds(1, pairs, stride=2), :]
    return jnp.where(iota(even.shape, 1) < HALF, even, odd)


def unpack_pairs(ref, tile):
    pairs = tile.shape[0]
    left = iota(tile.shape, 1) < HALF
    turned = pltpu.roll(tile, HALF, 1)
    ref[pl.ds(0, pairs, stride=2), :] = jnp.where(left, tile, turned)
    ref[pl.ds(1, pairs, stride=2), :] = jnp.where(left, turned, tile)
    return ref[...]


def repeat(count, step):
    if count <= 8:
        for i in range(count):
            step(i, 0)
    else:
        lax.fori_loop(0, count, step, 0)


class Plan:
    def __init__(self, x, means, pop):
        self.dims, self.cells = x.shape
        self.clusters = means.shape[0]
        self.batches = pop.shape[0]
        self.rows = lax.axis_size("cells")
        self.cols = lax.axis_size("grp")
        self.devices = self.rows * self.cols
        self.total = self.cells * self.devices
        self.most = 2 * self.total // self.batches
        self.reach = (self.most - 2) // self.cells + 1
        outside = -(-(self.total - self.cells) // self.most)
        local = min(self.batches, self.batches - outside + 2)
        self.group = max(1, LANES // self.clusters)
        self.groups = -(-local // self.group)
        self.depth = self.group * self.clusters
        self.blocks = -(-(self.groups * self.group) // LANES)
        self.first_at = self.batches + self.group
        self.table = self.first_at + 2
        self.width = -(-(3 * self.clusters + 4) // LANES) * LANES
        self.pairs = self.clusters // 2
        self.gap = HALF - (self.dims + 1)
        self.gap_rows = -(-(self.dims + 1) // self.gap)
        self.owned_pairs = self.clusters // self.rows // 2

    def offset(self):
        place = lax.axis_index("cells") * self.cols + lax.axis_index("grp")
        return place * self.cells


def segment(plan, starts, offset, index):
    batch = starts[plan.first_at] + index
    return starts[batch] - offset, starts[batch + 1] - offset


def padded(plan, x_ref, xs_ref):
    low = plan.dims // 8 * 8
    tail = (xs_ref.shape[0] - low, plan.cells)
    xs_ref[low:, :] = jnp.where(iota(tail, 0) == plan.dims - low, 1.0, 0.0)
    xs_ref[0 : plan.dims, :] = x_ref[...]


def count_kernel(plan, pop, lam, scale, means, x_ref, send, prior, counts, starts, xs, ms):
    k = plan.clusters
    offset = plan.offset()
    running, first, last = jnp.int32(0), jnp.int32(0), jnp.int32(0)
    for b in range(plan.batches):
        starts[b] = running
        running = running + pop[b]
        first = first + (running <= offset).astype(jnp.int32)
        last = last + (running <= offset + plan.cells - 1).astype(jnp.int32)
    for b in range(plan.batches, plan.first_at):
        starts[b] = running
    starts[plan.first_at] = first
    starts[plan.first_at + 1] = last
    segments = last - first + 1

    padded(plan, x_ref, xs)
    ms[...] = jnp.zeros_like(ms)
    ms[:, 0 : plan.dims] = means[...]
    m = ms[...]
    m1 = m.astype(bf16).astype(f32)
    m2 = (m - m1).astype(bf16).astype(f32)
    m3 = m - m1 - m2
    zero = jnp.zeros_like(m)

    def twice(value):
        return value + pltpu.roll(value, HALF, 1)

    weights = jnp.concatenate(
        [
            jnp.concatenate([twice(m1), m1], axis=1),
            jnp.concatenate([twice(m2), zero], axis=1),
            jnp.concatenate([m3, zero], axis=1),
        ],
        axis=0,
    ).astype(bf16)
    lengths = jnp.sum(m * m, axis=1, keepdims=True)
    soft = jnp.zeros((k, 1), f32)
    row = iota((k, 1), 0)
    for c in range(k):
        soft = jnp.where(row == c, scale[c], soft)
    inverse = 1.0 / (2.0 * soft)
    chunk = min(plan.cells, 1024)
    for c in range(plan.cells // chunk):
        at = slice(c * chunk, (c + 1) * chunk)
        x = xs[:, at]
        x1 = x.astype(bf16)
        r = x - x1.astype(f32)
        x2 = r.astype(bf16)
        x3 = (r - x2.astype(f32)).astype(bf16)
        stacked = jnp.concatenate([x1, x2, x3, jnp.zeros_like(x1)], axis=0)
        dots = jnp.dot(weights, stacked, preferred_element_type=f32)
        dots = dots[0:k] + dots[k : 2 * k] + dots[2 * k : 3 * k]
        scores = (2.0 * dots - lengths) * inverse
        raised = jnp.exp(scores - jnp.max(scores, axis=0, keepdims=True))
        prior[:, at] = raised / jnp.sum(raised, axis=0, keepdims=True)

    counts[...] = jnp.zeros_like(counts)
    lane = iota((k, LANES), 1)
    cell = iota((1, plan.cells), 1)
    step = min(4, plan.group)

    def count(i, carry):
        block = lax.div(i * step, LANES)
        held = counts[block]
        for j in range(step):
            s = i * step + j
            lo, hi = segment(plan, starts, offset, jnp.minimum(s, segments - 1))
            inside = (cell >= lo) & (cell < hi)
            mine = jnp.sum(jnp.where(inside, prior[...], 0.0), axis=1, keepdims=True)
            held = jnp.where(lane == s - block * LANES, mine, held)
        counts[block] = held
        return carry

    lax.fori_loop(0, lax.div(segments + step - 1, step), count, 0)

    total = jnp.sum(prior[...], axis=1, keepdims=True)
    here = segments - 1
    tail = counts[lax.div(here, LANES)]
    last_count = jnp.sum(
        jnp.where(lane == lax.rem(here, LANES), tail, 0.0), axis=1, keepdims=True
    )
    first_count = jnp.where(segments > 1, counts[0][:, 0:1], 0.0)
    wide = (k, plan.width)
    place = iota(wide, 1) - iota(wide, 0)
    out = jnp.where(place == 0, total, 0.0)
    out = jnp.where(place == k, first_count, out)
    out = jnp.where(place == 2 * k, last_count, out)
    out = jnp.sum(out, axis=0, keepdims=True)
    lanes = iota((1, plan.width), 1)
    out = jnp.where(lanes == 3 * k, first.astype(f32), out)
    out = jnp.where(lanes == 3 * k + 1, last.astype(f32), out)
    out = jnp.where(lanes == 3 * k + 2, lam[first], out)
    out = jnp.where(lanes == 3 * k + 3, lam[last], out)
    send[...] = jnp.broadcast_to(out, send.shape)


def masked(plan, a1, a2, stack, starts, offset, group):
    k = plan.clusters
    cell = iota((k, plan.cells), 1)
    for j in range(plan.group):
        lo, hi = segment_in(plan, starts, offset, group * plan.group + j)
        inside = jnp.where((cell >= lo) & (cell < hi), 1.0, 0.0).astype(bf16)
        stack[j * k : (j + 1) * k, :] = a1[...] * inside
        stack[plan.depth + j * k : plan.depth + (j + 1) * k, :] = a2[...] * inside


def segment_in(plan, starts, offset, index):
    batch = jnp.minimum(starts[plan.first_at] + index, plan.first_at - 1)
    following = jnp.minimum(batch + 1, plan.first_at - 1)
    return starts[batch] - offset, starts[following] - offset


def moment_kernel(
    plan, starts, lam, got, prior, counts, x_ref, send, assign, moments, xs, wide, a1, a2, stack, sums, turned
):
    k = plan.clusters
    offset = plan.offset()
    first, last = starts[plan.first_at], starts[plan.first_at + 1]
    segments = last - first + 1
    groups = lax.div(segments + plan.group - 1, plan.group)
    padded(plan, x_ref, xs)

    table = got[...]
    total = column(jnp.sum(table, axis=0, keepdims=True), 0, k)
    heads, tails = table[:, 3 * k : 3 * k + 1], table[:, 3 * k + 1 : 3 * k + 2]

    def complete(batch):
        batch = batch.astype(f32)
        of_heads = jnp.sum(jnp.where(heads == batch, table, 0.0), axis=0, keepdims=True)
        of_tails = jnp.sum(jnp.where(tails == batch, table, 0.0), axis=0, keepdims=True)
        return column(of_heads, k, k) + column(of_tails, 2 * k, k)

    first_count, last_count = complete(first), complete(last)
    share = total / f32(plan.total)
    cell = iota((1, plan.cells), 1)
    lane = iota((k, LANES), 1)
    wide[...] = jnp.zeros_like(wide)

    def weigh(g, carry):
        block = lax.div(g * plan.group, LANES)
        held = counts[block]
        for j in range(plan.group):
            s = g * plan.group + j
            lo, hi = segment_in(plan, starts, offset, s)
            mine = jnp.sum(
                jnp.where(lane == s - block * LANES, held, 0.0), axis=1, keepdims=True
            )
            mine = jnp.where(s == 0, first_count, mine)
            mine = jnp.where(s == segments - 1, last_count, mine)
            expected = (hi - lo).astype(f32) * share
            ratio = (expected + 1.0) / (mine + 1.0)
            inside = (cell >= lo) & (cell < hi)
            wide[...] = jnp.where(inside, ratio * ratio, wide[...])
        return carry

    lax.fori_loop(0, groups, weigh, 0)
    raised = prior[...] * wide[...]
    chosen = raised / jnp.sum(raised, axis=0, keepdims=True)
    assign[...] = chosen
    a1[...], a2[...] = split(chosen)
    x1, x2 = split(xs[...])
    cellwise = jnp.concatenate([x1, x2], axis=0)

    sums[...] = jnp.zeros_like(sums)

    def gather(g, carry):
        masked(plan, a1, a2, stack, starts, offset, g)
        both = lax.dot_general(
            stack[...], cellwise, (((1,), (1,)), ((), ())), preferred_element_type=f32
        )
        both = both[0 : plan.depth] + both[plan.depth :]
        both = both + pltpu.roll(both, HALF, 1)
        moments[pl.ds(pl.multiple_of(g * plan.depth, plan.depth), plan.depth), :] = both
        mass = lane_of(both, plan.dims)
        inner, head, tail, every = sums[0], sums[1], sums[2], sums[3]
        for j in range(plan.group):
            s = g * plan.group + j
            at = slice(j * k, (j + 1) * k)
            ridge = lam[jnp.minimum(first + s, plan.batches - 1)]
            part = both[at]
            every = every + part
            shrunk = part * (ridge / (mass[at] + ridge))
            inner = inner + jnp.where((s > 0) & (s < segments - 1), shrunk, 0.0)
            head = head + jnp.where((s == 0) & (segments > 1), part, 0.0)
            tail = tail + jnp.where(s == segments - 1, part, 0.0)
        sums[0], sums[1], sums[2], sums[3] = inner, head, tail, every
        return carry

    lax.fori_loop(0, groups, gather, 0)
    inner, head, tail, every = [pack_pairs(sums.at[i]) for i in range(4)]
    lanes = lax.rem(iota(inner.shape, 1), HALF)
    inner = jnp.where(lanes <= plan.dims, inner, 0.0)
    every = jnp.where(lanes <= plan.dims, every, 0.0)
    for j in range(plan.gap_rows):
        moved = pltpu.roll(every, (plan.dims + 1 - plan.gap * j) % LANES, 1)
        turned[j] = jnp.where(lanes > plan.dims, moved, 0.0)
    row = iota(inner.shape, 0)

    def put(c, carry):
        mine = inner
        for q in range(plan.owned_pairs):
            for j in range(plan.gap_rows):
                pair = c * plan.owned_pairs + q
                piece = jnp.broadcast_to(turned[j, pl.ds(pair, 1), :], inner.shape)
                mine = mine + jnp.where(row == q * plan.gap_rows + j, piece, 0.0)
        for q in range(plan.cols):
            p = c * plan.cols + q
            send[p, 0 : plan.pairs] = mine
            send[p, plan.pairs : 2 * plan.pairs] = head
            send[p, 2 * plan.pairs :] = tail
        return carry

    repeat(plan.rows, put)


def correct_kernel(
    plan, starts, lam, got, ids, assign, moments, x_ref, out, centroids, a1, a2, stack, rows, spread
):
    k = plan.clusters
    offset = plan.offset()
    first, last = starts[plan.first_at], starts[plan.first_at + 1]
    segments = last - first + 1
    groups = lax.div(segments + plan.group - 1, plan.group)
    a1[...], a2[...] = split(assign[...])

    shape = (plan.devices, LANES)
    device = iota(shape, 0)

    def of(lane):
        return jnp.broadcast_to(ids[:, lane : lane + 1], shape)

    heads, tails = of(3 * k), of(3 * k + 1)
    head_ridge, tail_ridge = of(3 * k + 2), of(3 * k + 3)

    def shifted(value, distance):
        return pltpu.roll(value, distance % plan.devices, 0)

    links = []
    for hop in range(1, plan.reach + 1):
        before = device >= hop
        after = device < plan.devices - hop
        links.append(
            (
                hop,
                jnp.where(before & (shifted(tails, hop) == heads), 1.0, 0.0),
                jnp.where(after & (shifted(heads, -hop) == tails), 1.0, 0.0),
                jnp.where(before & (shifted(tails, hop) == tails), 1.0, 0.0),
                jnp.where(after & (shifted(tails, -hop) == tails), 1.0, 0.0),
            )
        )
    first_f, last_f = first.astype(f32), last.astype(f32)

    def gather(j, carry):
        inner = got[:, pl.ds(j, 1), :].reshape(shape)
        head = got[:, pl.ds(plan.pairs + j, 1), :].reshape(shape)
        tail = got[:, pl.ds(2 * plan.pairs + j, 1), :].reshape(shape)
        head_mass = halves(head, plan.dims)
        tail_mass = halves(tail, plan.dims)
        whole_head, whole_tail = head_mass, tail_mass
        for hop, back, ahead, same_back, same_ahead in links:
            whole_head = whole_head + back * shifted(tail_mass, hop)
            whole_tail = whole_tail + ahead * shifted(head_mass, -hop)
            whole_tail = whole_tail + same_back * shifted(tail_mass, hop)
            whole_tail = whole_tail + same_ahead * shifted(tail_mass, -hop)
        shrunk = head * (head_ridge / (whole_head + head_ridge))
        shrunk = shrunk + tail * (tail_ridge / (whole_tail + tail_ridge))
        right = jnp.sum(inner + shrunk, axis=0, keepdims=True)
        rows[0, pl.ds(j, 1)] = right / (1.0 + halves(right, plan.dims))
        for i, batch in ((1, first_f), (2, last_f)):
            both = jnp.where(heads == batch, head, 0.0) + jnp.where(tails == batch, tail, 0.0)
            rows[i, pl.ds(j, 1)] = jnp.sum(both, axis=0, keepdims=True)
        rows[3, pl.ds(j, 1)] = jnp.sum(inner, axis=0, keepdims=True)
        return carry

    repeat(plan.pairs, gather)

    lanes = lax.rem(iota((1, LANES), 1), HALF)
    for q in range(plan.owned_pairs):
        every = jnp.zeros((1, LANES), f32)
        for j in range(plan.gap_rows):
            at = q * plan.gap_rows + j
            piece = jnp.where(lanes > plan.dims, rows[3, at : at + 1], 0.0)
            moved = pltpu.roll(piece, (plan.gap * j - plan.dims - 1) % LANES, 1)
            inside = (lanes >= plan.gap * j) & (lanes < plan.gap * (j + 1))
            every = every + jnp.where(inside, moved, 0.0)
        every = every / (1.0 + halves(every, plan.dims))
        centroids[2 * q : 2 * q + 1] = every[:, 0 : plan.dims]
        centroids[2 * q + 1 : 2 * q + 2] = pltpu.roll(every, HALF, 1)[:, 0 : plan.dims]

    intercept = unpack_pairs(spread, rows[0])
    first_sum = unpack_pairs(spread, rows[1])
    last_sum = unpack_pairs(spread, rows[2])
    out[...] = x_ref[...]
    left = iota((k, LANES), 1) < HALF

    def apply(g, carry):
        masked(plan, a1, a2, stack, starts, offset, g)
        held = moments[pl.ds(pl.multiple_of(g * plan.depth, plan.depth), plan.depth), :]
        slopes = []
        for j in range(plan.group):
            s = g * plan.group + j
            part = held[j * k : (j + 1) * k]
            part = jnp.where(s == 0, first_sum, part)
            part = jnp.where(s == segments - 1, last_sum, part)
            mass = lane_of(part, plan.dims)
            ridge = lam[jnp.minimum(first + s, plan.batches - 1)]
            slope = (part - mass * intercept) / (mass + ridge)
            s1, s2 = split(slope)
            slopes.append(jnp.where(left, s1.astype(f32), s2.astype(f32)))
        slopes = jnp.concatenate(slopes, axis=0).astype(bf16)
        slopes = jnp.concatenate([slopes, slopes], axis=0)
        chunk = min(plan.cells, 1024)
        for c in range(plan.cells // chunk):
            at = slice(c * chunk, (c + 1) * chunk)
            moved = lax.dot_general(
                slopes, stack[:, at], (((0,), (0,)), ((), ())), preferred_element_type=f32
            )
            moved = moved[0:HALF] + moved[HALF:]
            out[:, at] = out[:, at] - moved[0 : plan.dims]
        return carry

    lax.fori_loop(0, groups, apply, 0)


def vmem():
    return pl.BlockSpec(memory_space=pltpu.VMEM)


def smem():
    return pl.BlockSpec(memory_space=pltpu.SMEM)


def shaped(shape, kind=f32):
    return jax.ShapeDtypeStruct(shape, kind)


def bound(kernel, plan, name):
    def run(*refs):
        kernel(plan, *refs)

    run.__name__ = name
    return run


def body(x, means, scale, lam, pop):
    plan = Plan(x, means, pop)
    k, cells = plan.clusters, plan.cells
    send, prior, counts, starts = pl.pallas_call(
        bound(count_kernel, plan, "count"),
        name="count",
        out_shape=(
            shaped((plan.devices, plan.width)),
            shaped((k, cells)),
            shaped((plan.blocks, k, LANES)),
            shaped((plan.table,), jnp.int32),
        ),
        in_specs=[smem(), smem(), smem(), vmem(), vmem()],
        out_specs=(vmem(), vmem(), vmem(), smem()),
        scratch_shapes=[pltpu.VMEM((HALF, cells), f32), pltpu.VMEM((k, LANES), f32)],
    )(pop, lam, scale, means, x)
    ids = lax.all_to_all(send, AXES, 0, 0, tiled=True)
    send, assign, moments = pl.pallas_call(
        bound(moment_kernel, plan, "moment"),
        name="moment",
        out_shape=(
            shaped((plan.devices, 3 * plan.pairs, LANES)),
            shaped((k, cells)),
            shaped((plan.groups * plan.depth, LANES)),
        ),
        in_specs=[smem(), smem(), vmem(), vmem(), vmem(), vmem()],
        out_specs=(vmem(), vmem(), vmem()),
        scratch_shapes=[
            pltpu.VMEM((HALF, cells), f32),
            pltpu.VMEM((k, cells), f32),
            pltpu.VMEM((k, cells), bf16),
            pltpu.VMEM((k, cells), bf16),
            pltpu.VMEM((2 * plan.depth, cells), bf16),
            pltpu.VMEM((4, k, LANES), f32),
            pltpu.VMEM((plan.gap_rows, plan.pairs, LANES), f32),
        ],
    )(starts, lam, ids, prior, counts, x)
    got = lax.all_to_all(send, AXES, 0, 0, tiled=True)
    corrected, centroids = pl.pallas_call(
        bound(correct_kernel, plan, "correct"),
        name="correct",
        out_shape=(shaped(x.shape), shaped((k // plan.rows, plan.dims))),
        in_specs=[smem(), smem(), vmem(), vmem(), vmem(), vmem(), vmem()],
        out_specs=(vmem(), vmem()),
        scratch_shapes=[
            pltpu.VMEM((k, cells), bf16),
            pltpu.VMEM((k, cells), bf16),
            pltpu.VMEM((2 * plan.depth, cells), bf16),
            pltpu.VMEM((4, plan.pairs, LANES), f32),
            pltpu.VMEM((k, LANES), f32),
        ],
    )(starts, lam, got, ids, assign, moments, x)
    return corrected, centroids


def solution(mesh):
    return jax.shard_map(
        body,
        mesh=mesh,
        in_specs=(P(None, AXES), P(), P(), P(), P()),
        out_specs=(P(None, AXES), P("cells", None)),
        check_vma=False,
    )
```

```python
import jax
import jax.numpy as jnp
from jax import lax
from jax.experimental import pallas as pl
from jax.experimental.pallas import tpu as pltpu
from jax.sharding import PartitionSpec as P

f32 = jnp.float32
bf16 = jnp.bfloat16
i32 = jnp.int32
HALF = 64
LANES = 128
TILE = 16
AXES = ("cells", "grp")
BY_CELLS = (((1,), (1,)), ((), ()))
BY_ROWS = (((0,), (0,)), ((), ()))


def iota(shape, axis):
    return lax.broadcasted_iota(i32, shape, axis)


def split(value, parts):
    out = []
    for i in range(parts):
        out.append(value.astype(bf16))
        if i + 1 < parts:
            value = value - out[-1].astype(f32)
    return out


def lane_of(value, lane):
    return jnp.broadcast_to(value[:, lane : lane + 1], value.shape)


def halves(value, lane):
    left = iota(value.shape, 1) < HALF
    return jnp.where(left, lane_of(value, lane), lane_of(value, HALF + lane))


def column(row, first, count):
    shape = (count, row.shape[1])
    pick = iota(shape, 1) == iota(shape, 0) + first
    return jnp.sum(jnp.where(pick, jnp.broadcast_to(row, shape), 0.0), axis=1, keepdims=True)


def pack_pairs(ref):
    pairs = ref.shape[0] // 2
    even = ref[pl.ds(0, pairs, stride=2), :]
    odd = ref[pl.ds(1, pairs, stride=2), :]
    return jnp.where(iota(even.shape, 1) < HALF, even, odd)


def unpack_pairs(ref, tile):
    pairs = tile.shape[0]
    left = iota(tile.shape, 1) < HALF
    turned = pltpu.roll(tile, HALF, 1)
    ref[pl.ds(0, pairs, stride=2), :] = jnp.where(left, tile, turned)
    ref[pl.ds(1, pairs, stride=2), :] = jnp.where(left, turned, tile)
    return ref[...]


def repeat(count, step):
    if count <= 32:
        for i in range(count):
            step(i, 0)
    else:
        lax.fori_loop(0, count, step, 0)


class Plan:
    def __init__(self, x, means, pop):
        self.dims, self.cells = x.shape
        self.clusters = means.shape[0]
        self.batches = pop.shape[0]
        self.rows = lax.axis_size("cells")
        self.cols = lax.axis_size("grp")
        self.devices = self.rows * self.cols
        self.total = self.cells * self.devices
        self.most = 2 * self.total // self.batches
        self.reach = (self.most - 2) // self.cells + 1
        self.lone = self.most >= self.cells
        outside = -(-(self.total - self.cells) // self.most)
        local = min(self.batches, self.batches - outside + 2)
        self.tiles = -(-local // TILE)
        self.local = self.tiles * TILE
        self.group = max(1, LANES // self.clusters)
        self.groups = self.local // self.group
        self.depth = self.group * self.clusters
        self.width = -(-(3 * self.clusters + 4) // LANES) * LANES
        self.pairs = self.clusters // 2
        self.gap = HALF - (self.dims + 1)
        self.gap_rows = -(-(self.dims + 1) // self.gap)
        self.owned_pairs = self.clusters // self.rows // 2
        self.keep = self.devices * self.pairs * 3 * LANES * 4 <= 1 << 20
        self.chunk = min(self.cells, 1024)
        self.chunks = self.cells // self.chunk

    def at(self, c):
        return slice(c * self.chunk, (c + 1) * self.chunk)


def count_kernel(plan, pop, lam, scale, means, x_hbm, send, prior, counts, sizes, places, parts, xs, info, ridges, ends, ms, seg, sems):
    k = plan.clusters
    copies = [
        pltpu.make_async_copy(x_hbm.at[:, plan.at(c)], xs.at[:, plan.at(c)], sems.at[c])
        for c in range(plan.chunks)
    ]
    for copy in copies:
        copy.start()
    offset = (lax.axis_index("cells") * plan.cols + lax.axis_index("grp")) * plan.cells
    running, first, last = jnp.int32(0), jnp.int32(0), jnp.int32(0)
    for b in range(plan.batches):
        running = running + pop[b]
        ends[b] = running
        first = first + (running <= offset).astype(i32)
        last = last + (running <= offset + plan.cells - 1).astype(i32)
    segments = last - first + 1
    tiles = lax.div(segments + TILE - 1, TILE)
    info[0], info[1], info[2] = first, last, segments

    lane = iota((1, LANES), 1)
    cell = iota((8, plan.cells), 1)
    half = TILE // 2
    seg[...] = jnp.zeros_like(seg)

    def locate(g, carry):
        held = seg[...]
        for j in range(half):
            b = jnp.minimum(first + g * half + j, plan.batches - 1)
            held = held + jnp.where(cell >= ends[b] - offset, 1.0, 0.0)
        seg[...] = held
        return carry

    lax.fori_loop(0, lax.div(segments + half - 1, half), locate, 0)

    def note(g, carry):
        row = jnp.zeros((1, LANES), f32)
        for j in range(TILE):
            b = jnp.minimum(first + g * TILE + j, plan.batches - 1)
            ridges[g * TILE + j] = lam[b]
            row = jnp.where(lane == j, pop[b].astype(f32), row)
        sizes[pl.ds(g, 1), :] = row
        return carry

    lax.fori_loop(0, tiles, note, 0)

    ms[...] = jnp.zeros_like(ms)
    ms[:, 0 : plan.dims] = means[...]
    m = ms[...]
    m1, m2, m3 = [part.astype(f32) for part in split(m, 3)]
    zero = jnp.zeros_like(m)

    def twice(value):
        return value + pltpu.roll(value, HALF, 1)

    weights = jnp.concatenate(
        [
            jnp.concatenate([twice(m1), m1], axis=1),
            jnp.concatenate([twice(m2), zero], axis=1),
            jnp.concatenate([m3, zero], axis=1),
        ],
        axis=0,
    ).astype(bf16)
    lengths = jnp.sum(m * m, axis=1, keepdims=True)
    soft = jnp.ones((k, 1), f32)
    row = iota((k, 1), 0)
    for c in range(k):
        soft = jnp.where(row == c, scale[c], soft)
    inverse = 1.0 / (2.0 * soft)
    low = plan.dims // 8 * 8
    over = plan.dims - low
    shape = (8, plan.chunk)
    tail_row = iota(shape, 0)
    constant = jnp.where(tail_row == over, 1.0, 0.0)
    rest = [jnp.zeros(shape, f32)] * ((HALF - low) // 8 - 1)
    spots = iota((TILE, plan.chunk), 0).astype(f32).astype(bf16)
    found = jnp.zeros((3 * k, TILE), f32)
    for c in range(plan.chunks):
        at = plan.at(c)
        copies[c].wait()
        if over:
            moved = pltpu.roll(xs[plan.dims - 8 : plan.dims, at], over, 0)
            tail = jnp.where(tail_row < over, moved, constant)
        else:
            tail = constant
        x = jnp.concatenate([xs[0:low, at], tail] + rest, axis=0)
        x1, x2, x3 = split(x, 3)
        parts[0:HALF, at] = x1
        parts[HALF:, at] = x2
        stacked = jnp.concatenate([x1, x2, x3, jnp.zeros_like(x1)], axis=0)
        dots = jnp.dot(weights, stacked, preferred_element_type=f32)
        dots = dots[0:k] + dots[k : 2 * k] + dots[2 * k : 3 * k]
        scores = (2.0 * dots - lengths) * inverse
        raised = jnp.exp(scores - jnp.max(scores, axis=0, keepdims=True))
        chance = raised / jnp.sum(raised, axis=0, keepdims=True)
        prior[:, at] = chance
        place = jnp.concatenate([seg[:, at]] * (TILE // 8), axis=0).astype(bf16)
        places[:, at] = place
        hot = jnp.where(place == spots, bf16(1), bf16(0))
        found = found + lax.dot_general(
            jnp.concatenate(split(chance, 3), axis=0), hot, BY_CELLS, preferred_element_type=f32
        )

    def settle(g, found):
        found = found[0:k] + found[k : 2 * k] + found[2 * k :]
        counts[g] = jnp.concatenate([found, jnp.zeros((k, LANES - TILE), f32)], axis=1)

    settle(0, found)

    def count(g, carry):
        rows = (iota((TILE, plan.cells), 0) + g * TILE).astype(f32).astype(bf16)
        hot = jnp.where(places[...] == rows, bf16(1), bf16(0))
        settle(
            g,
            lax.dot_general(
                jnp.concatenate(split(prior[...], 3), axis=0), hot, BY_CELLS, preferred_element_type=f32
            ),
        )
        return carry

    lax.fori_loop(1, tiles, count, 0)

    every = lax.fori_loop(1, tiles, lambda g, total: total + counts[g], counts[0])
    total = jnp.sum(every, axis=1, keepdims=True)
    here = segments - 1
    end = counts[lax.div(here, TILE)]
    wide = iota((k, LANES), 1)
    last_count = jnp.sum(jnp.where(wide == lax.rem(here, TILE), end, 0.0), axis=1, keepdims=True)
    first_count = jnp.where(segments > 1, counts[0][:, 0:1], 0.0)
    spread = (k, plan.width)
    turn = iota(spread, 1) - iota(spread, 0)
    out = jnp.where(turn == 0, total, 0.0)
    out = jnp.where(turn == k, first_count, out)
    out = jnp.where(turn == 2 * k, last_count, out)
    out = jnp.sum(out, axis=0, keepdims=True)
    lanes = iota((1, plan.width), 1)
    out = jnp.where(lanes == 3 * k, first.astype(f32), out)
    out = jnp.where(lanes == 3 * k + 1, last.astype(f32), out)
    out = jnp.where(lanes == 3 * k + 2, lam[first], out)
    out = jnp.where(lanes == 3 * k + 3, lam[last], out)
    send[...] = jnp.broadcast_to(out, send.shape)


def masked(plan, a1, a2, places, g, at):
    k = plan.clusters
    width = at.stop - at.start
    shape = (TILE, width)
    base = jnp.full(shape, (g * plan.group).astype(f32) if not isinstance(g, int) else f32(g * plan.group))
    relative = places[:, at] - base.astype(bf16)
    out = []
    for a in (a1[:, at], a2[:, at]):
        for j in range(plan.group):
            inside = jnp.concatenate([relative] * (k // TILE), axis=0) == bf16(j)
            out.append(jnp.where(inside, a, bf16(0)))
    return jnp.concatenate(out, axis=0)


def moment_kernel(
    plan, info, ridges, got, prior, counts, sizes, places, parts, send, a1, a2, moments, wide, sums, turned
):
    k = plan.clusters
    first, last, segments = info[0], info[1], info[2]
    groups = lax.div(segments + plan.group - 1, plan.group)
    tiles = lax.div(segments + TILE - 1, TILE)

    table = got[...]
    total = column(jnp.sum(table, axis=0, keepdims=True), 0, k)
    heads, tails = table[:, 3 * k : 3 * k + 1], table[:, 3 * k + 1 : 3 * k + 2]

    def complete(batch):
        batch = batch.astype(f32)
        of_heads = jnp.sum(jnp.where(heads == batch, table, 0.0), axis=0, keepdims=True)
        of_tails = jnp.sum(jnp.where(tails == batch, table, 0.0), axis=0, keepdims=True)
        return column(of_heads, k, k) + column(of_tails, 2 * k, k)

    first_count, last_count = complete(first), complete(last)
    share = total / f32(plan.total)
    lane = iota((k, LANES), 1)

    def factors(g):
        held = counts[g]
        held = jnp.where(lane + g * TILE == 0, first_count, held)
        held = jnp.where(lane + g * TILE == segments - 1, last_count, held)
        ratio = (sizes[pl.ds(g, 1), :] * share + 1.0) / (held + 1.0)
        ratio = jnp.where(lane < TILE, ratio * ratio, 0.0)
        w1, w2, w3 = [part.astype(f32) for part in split(ratio, 3)]
        row = w1 + pltpu.roll(w2, TILE, 1) + pltpu.roll(w3, 2 * TILE, 1)
        return row.astype(bf16)[:, 0 : 4 * TILE]

    def factor_of(weights, g, at):
        shape = (TILE, at.stop - at.start)
        rows = (iota(shape, 0) + g * TILE).astype(f32).astype(bf16)
        hot = jnp.where(places[:, at] == rows, bf16(1), bf16(0))
        hot = jnp.concatenate([hot, hot, hot, jnp.zeros_like(hot)], axis=0)
        return jnp.dot(weights, hot, preferred_element_type=f32)

    weights = factors(0)
    for c in range(plan.chunks):
        wide[:, plan.at(c)] = factor_of(weights, 0, plan.at(c))

    def more(g, carry):
        weights = factors(g)
        for c in range(plan.chunks):
            wide[:, plan.at(c)] += factor_of(weights, g, plan.at(c))
        return carry

    lax.fori_loop(1, tiles, more, 0)
    for c in range(plan.chunks):
        at = plan.at(c)
        raised = prior[:, at] * wide[:, at]
        a1[:, at], a2[:, at] = split(raised / jnp.sum(raised, axis=0, keepdims=True), 2)

    sums[...] = jnp.zeros_like(sums)

    def gather(g, carry):
        both = jnp.zeros((2 * plan.depth, LANES), f32)
        for c in range(plan.chunks):
            at = plan.at(c)
            both = both + lax.dot_general(
                masked(plan, a1, a2, places, g, at), parts[:, at], BY_CELLS, preferred_element_type=f32
            )
        both = both[0 : plan.depth] + both[plan.depth :]
        both = both + pltpu.roll(both, HALF, 1)
        moments[pl.ds(pl.multiple_of(g * plan.depth, plan.depth), plan.depth), :] = both
        mass = lane_of(both, plan.dims)
        inner, head, tail, every = sums[0], sums[1], sums[2], sums[3]
        for j in range(plan.group):
            s = g * plan.group + j
            at = slice(j * k, (j + 1) * k)
            ridge = ridges[s]
            part = both[at]
            every = every + part
            shrunk = part * (ridge / (mass[at] + ridge))
            inner = inner + jnp.where((s > 0) & (s < segments - 1), shrunk, 0.0)
            head = head + jnp.where((s == 0) & (segments > 1), part, 0.0)
            tail = tail + jnp.where(s == segments - 1, part, 0.0)
        sums[0], sums[1], sums[2], sums[3] = inner, head, tail, every
        return carry

    lax.fori_loop(0, groups, gather, 0)
    inner, head, tail, every = [pack_pairs(sums.at[i]) for i in range(4)]
    lanes = lax.rem(iota(inner.shape, 1), HALF)
    inner = jnp.where(lanes <= plan.dims, inner, 0.0)
    every = jnp.where(lanes <= plan.dims, every, 0.0)
    for j in range(plan.gap_rows):
        moved = pltpu.roll(every, (plan.dims + 1 - plan.gap * j) % LANES, 1)
        turned[j] = jnp.where(lanes > plan.dims, moved, 0.0)
    row = iota(inner.shape, 0)

    def put(c, carry):
        mine = inner
        for q in range(plan.owned_pairs):
            for j in range(plan.gap_rows):
                pair = c * plan.owned_pairs + q
                piece = jnp.broadcast_to(turned[j, pl.ds(pair, 1), :], inner.shape)
                mine = mine + jnp.where(row == q * plan.gap_rows + j, piece, 0.0)
        for q in range(plan.cols):
            p = c * plan.cols + q
            send[p, 0 : plan.pairs] = mine
            send[p, plan.pairs : 2 * plan.pairs] = head
            send[p, 2 * plan.pairs :] = tail
        return carry

    repeat(plan.rows, put)


def correct_kernel(
    plan, info, ridges, got, ids, a1, a2, moments, places, xs, out_hbm, centroids, marks, slopes, rows, spread, out, sems
):
    k = plan.clusters
    first, last, segments = info[0], info[1], info[2]
    groups = lax.div(segments + plan.group - 1, plan.group)
    shape = (plan.devices, LANES)
    device = iota(shape, 0)

    def of(lane):
        return jnp.broadcast_to(ids[:, lane : lane + 1], shape)

    heads, tails = of(3 * k), of(3 * k + 1)
    first_f, last_f = first.astype(f32), last.astype(f32)

    def shifted(value, distance):
        return pltpu.roll(value, distance % plan.devices, 0)

    marks[0], marks[1] = of(3 * k + 2), of(3 * k + 3)
    for i, (side, batch) in enumerate(
        ((heads, first_f), (tails, first_f), (heads, last_f), (tails, last_f))
    ):
        marks[2 + i] = jnp.where(side == batch, 1.0, 0.0)
    links = []

    def link(hop, mine, theirs, into, source):
        inside = (device + hop >= 0) & (device + hop < plan.devices)
        at = 6 + len(links)
        marks[at] = jnp.where(inside & (shifted(theirs, -hop) == mine), 1.0, 0.0)
        links.append((at, hop, into, source))

    for hop in range(1, plan.reach + 1):
        link(-hop, heads, tails, 0, 1)
        link(hop, tails, heads, 1, 0)
        if plan.lone:
            link(-hop, tails, tails, 1, 1)
            link(hop, tails, tails, 1, 1)

    p = plan.pairs
    block = (p, LANES)

    def mark(i, r):
        return jnp.broadcast_to(marks[i, pl.ds(r, 1), :], block)

    def side_of(r, side):
        return got[r, (1 + side) * p : (2 + side) * p]

    def gather(r, carry):
        right, inner, first_sum, last_sum = carry
        sides = [side_of(r, 0), side_of(r, 1)]
        whole = [halves(side, plan.dims) for side in sides]
        for at, hop, into, source in links:
            if isinstance(r, int):
                if not 0 <= r + hop < plan.devices:
                    continue
                other = r + hop
            else:
                other = jnp.clip(r + hop, 0, plan.devices - 1)
            whole[into] = whole[into] + mark(at, r) * halves(side_of(other, source), plan.dims)
        mine = got[r, 0:p]
        inner = inner + mine
        right = right + mine
        for i in range(2):
            ridge = mark(i, r)
            right = right + sides[i] * (ridge / (whole[i] + ridge))
            first_sum = first_sum + sides[i] * mark(2 + i, r)
            last_sum = last_sum + sides[i] * mark(4 + i, r)
        return right, inner, first_sum, last_sum

    state = (jnp.zeros(block, f32),) * 4
    if plan.devices <= 32:
        for r in range(plan.devices):
            state = gather(r, state)
    else:
        state = lax.fori_loop(0, plan.devices, gather, state)
    right, inner, first_sum, last_sum = state
    intercept = unpack_pairs(spread, right / (1.0 + halves(right, plan.dims)))
    first_sum = unpack_pairs(spread, first_sum)
    last_sum = unpack_pairs(spread, last_sum)
    left = iota((k, LANES), 1) < HALF

    def slope(g, carry):
        start = pl.multiple_of(g * plan.depth, plan.depth)
        held = moments[pl.ds(start, plan.depth), :]
        made = []
        for j in range(plan.group):
            s = g * plan.group + j
            part = held[j * k : (j + 1) * k]
            part = jnp.where(s == 0, first_sum, part)
            part = jnp.where(s == segments - 1, last_sum, part)
            mass = lane_of(part, plan.dims)
            ridge = ridges[s]
            s1, s2 = split((part - mass * intercept) / (mass + ridge), 2)
            made.append(jnp.where(left, s1.astype(f32), s2.astype(f32)))
        slopes[g] = jnp.transpose(jnp.concatenate(made, axis=0)).astype(bf16)
        return carry

    lax.fori_loop(0, groups, slope, 0)

    def move(g, at):
        mine = slopes[g]
        moved = jnp.dot(
            jnp.concatenate([mine, mine], axis=1),
            masked(plan, a1, a2, places, g, at),
            preferred_element_type=f32,
        )
        return (moved[0:HALF] + moved[HALF:])[0 : plan.dims]

    copies = []
    for c in range(plan.chunks):
        at = plan.at(c)
        out[:, at] = xs[:, at]

        def again(g, carry):
            out[:, at] = out[:, at] - move(g, at)
            return carry

        lax.fori_loop(0, groups, again, 0)
        copies.append(pltpu.make_async_copy(out.at[:, at], out_hbm.at[:, at], sems.at[c]))
        copies[-1].start()

    rows[...] = inner
    lanes = lax.rem(iota((1, LANES), 1), HALF)
    for q in range(plan.owned_pairs):
        every = jnp.zeros((1, LANES), f32)
        for j in range(plan.gap_rows):
            at = q * plan.gap_rows + j
            piece = jnp.where(lanes > plan.dims, rows[at : at + 1], 0.0)
            moved = pltpu.roll(piece, (plan.gap * j - plan.dims - 1) % LANES, 1)
            inside = (lanes >= plan.gap * j) & (lanes < plan.gap * (j + 1))
            every = every + jnp.where(inside, moved, 0.0)
        every = every / (1.0 + halves(every, plan.dims))
        centroids[2 * q : 2 * q + 1] = every[:, 0 : plan.dims]
        centroids[2 * q + 1 : 2 * q + 2] = pltpu.roll(every, HALF, 1)[:, 0 : plan.dims]
    for copy in copies:
        copy.wait()


VMEM = pl.BlockSpec(memory_space=pltpu.VMEM)
SMEM = pl.BlockSpec(memory_space=pltpu.SMEM)
WHERE = pl.BlockSpec(memory_space=pltpu.HBM)


def hold_scalars(value):
    return pltpu.with_memory_space_constraint(value, pltpu.SMEM)


def bound(kernel, plan, name):
    def run(*refs):
        kernel(plan, *refs)

    run.__name__ = name
    return run


def body(x, means, scale, lam, pop):
    plan = Plan(x, means, pop)
    k, cells = plan.clusters, plan.cells
    params = pltpu.CompilerParams(vmem_limit_bytes=(16 << 20) if plan.keep else None)

    def kept(shape, kind=f32):
        return pltpu.VMEM(shape, kind) if plan.keep else jax.ShapeDtypeStruct(shape, kind)

    def hold(value):
        return pltpu.with_memory_space_constraint(value, pltpu.VMEM) if plan.keep else value

    send, prior, counts, sizes, places, parts, xs, info, ridges = pl.pallas_call(
        bound(count_kernel, plan, "count"),
        name="count",
        out_shape=(
            kept((plan.devices, plan.width)),
            kept((k, cells)),
            kept((plan.tiles, k, LANES)),
            kept((plan.tiles, LANES)),
            kept((TILE, cells), bf16),
            kept((2 * HALF, cells), bf16),
            kept((plan.dims, cells)),
            pltpu.SMEM((4,), i32),
            pltpu.SMEM((plan.local,), f32),
        ),
        in_specs=[SMEM, SMEM, SMEM, VMEM, WHERE],
        out_specs=(VMEM,) * 7 + (SMEM,) * 2,
        scratch_shapes=[
            pltpu.SMEM((plan.batches,), i32),
            pltpu.VMEM((k, LANES), f32),
            pltpu.VMEM((8, cells), f32),
            pltpu.SemaphoreType.DMA((plan.chunks,)),
        ],
    )(pop, lam, scale, means, x)
    prior, counts, sizes, places, parts, xs = map(hold, (prior, counts, sizes, places, parts, xs))
    info, ridges = hold_scalars(info), hold_scalars(ridges)
    ids = hold(lax.all_to_all(send, AXES, 0, 0, tiled=True))
    send, a1, a2, moments = pl.pallas_call(
        bound(moment_kernel, plan, "moment"),
        name="moment",
        compiler_params=params,
        out_shape=(
            kept((plan.devices, 3 * plan.pairs, LANES)),
            kept((k, cells), bf16),
            kept((k, cells), bf16),
            kept((plan.groups * plan.depth, LANES)),
        ),
        in_specs=[SMEM] * 2 + [VMEM] * 6,
        out_specs=(VMEM,) * 4,
        scratch_shapes=[
            pltpu.VMEM((k, cells), f32),
            pltpu.VMEM((4, k, LANES), f32),
            pltpu.VMEM((plan.gap_rows, plan.pairs, LANES), f32),
        ],
    )(info, ridges, ids, prior, counts, sizes, places, parts)
    a1, a2, moments = map(hold, (a1, a2, moments))
    got = hold(lax.all_to_all(send, AXES, 0, 0, tiled=True))
    marks = 6 + plan.reach * (4 if plan.lone else 2)
    corrected, centroids = pl.pallas_call(
        bound(correct_kernel, plan, "correct"),
        name="correct",
        compiler_params=params,
        out_shape=(
            jax.ShapeDtypeStruct(x.shape, f32),
            jax.ShapeDtypeStruct((k // plan.rows, plan.dims), f32),
        ),
        in_specs=[SMEM] * 2 + [VMEM] * 7,
        out_specs=(WHERE, VMEM),
        scratch_shapes=[
            pltpu.VMEM((marks, plan.devices, LANES), f32),
            pltpu.VMEM((plan.groups, LANES, plan.depth), bf16),
            pltpu.VMEM((plan.pairs, LANES), f32),
            pltpu.VMEM((k, LANES), f32),
            pltpu.VMEM((plan.dims, cells), f32),
            pltpu.SemaphoreType.DMA((plan.chunks,)),
        ],
    )(info, ridges, got, ids, a1, a2, moments, places, xs)
    return corrected, centroids


def solution(mesh):
    return jax.shard_map(
        body,
        mesh=mesh,
        in_specs=(P(None, AXES), P(), P(), P(), P()),
        out_specs=(P(None, AXES), P("cells", None)),
        check_vma=False,
    )
```

```python
import jax
import jax.numpy as jnp
from jax import lax
from jax.experimental import pallas as pl
from jax.experimental.pallas import tpu as pltpu
from jax.sharding import PartitionSpec as P

f32 = jnp.float32
bf16 = jnp.bfloat16
i32 = jnp.int32
HALF = 64
LANES = 128
TILE = 16
AXES = ("cells", "grp")
BY_CELLS = (((1,), (1,)), ((), ()))
BY_ROWS = (((0,), (0,)), ((), ()))


def iota(shape, axis):
    return lax.broadcasted_iota(i32, shape, axis)


def split(value, parts):
    out = []
    for i in range(parts):
        out.append(value.astype(bf16))
        if i + 1 < parts:
            value = value - out[-1].astype(f32)
    return out


def lane_of(value, lane):
    return jnp.broadcast_to(value[:, lane : lane + 1], value.shape)


def halves(value, lane):
    left = iota(value.shape, 1) < HALF
    return jnp.where(left, lane_of(value, lane), lane_of(value, HALF + lane))


def column(row, first, count):
    shape = (count, row.shape[1])
    pick = iota(shape, 1) == iota(shape, 0) + first
    return jnp.sum(jnp.where(pick, jnp.broadcast_to(row, shape), 0.0), axis=1, keepdims=True)


def pack_pairs(ref):
    pairs = ref.shape[0] // 2
    even = ref[pl.ds(0, pairs, stride=2), :]
    odd = ref[pl.ds(1, pairs, stride=2), :]
    return jnp.where(iota(even.shape, 1) < HALF, even, odd)


def unpack_pairs(ref, tile):
    pairs = tile.shape[0]
    left = iota(tile.shape, 1) < HALF
    turned = pltpu.roll(tile, HALF, 1)
    ref[pl.ds(0, pairs, stride=2), :] = jnp.where(left, tile, turned)
    ref[pl.ds(1, pairs, stride=2), :] = jnp.where(left, turned, tile)
    return ref[...]


def repeat(count, step):
    if count <= 32:
        for i in range(count):
            step(i, 0)
    else:
        lax.fori_loop(0, count, step, 0)


class Plan:
    def __init__(self, x, means, pop):
        self.dims, self.cells = x.shape
        self.clusters = means.shape[0]
        self.batches = pop.shape[0]
        self.rows = lax.axis_size("cells")
        self.cols = lax.axis_size("grp")
        self.devices = self.rows * self.cols
        self.total = self.cells * self.devices
        self.most = 2 * self.total // self.batches
        self.reach = (self.most - 2) // self.cells + 1
        self.lone = self.most >= self.cells
        outside = -(-(self.total - self.cells) // self.most)
        local = min(self.batches, self.batches - outside + 2)
        self.tiles = -(-local // TILE)
        self.local = self.tiles * TILE
        self.group = max(1, LANES // self.clusters)
        self.groups = self.local // self.group
        self.depth = self.group * self.clusters
        self.width = -(-(3 * self.clusters + 4) // LANES) * LANES
        self.pairs = self.clusters // 2
        self.part = self.pairs // 2
        self.gap = HALF - (self.dims + 1)
        self.gap_rows = -(-(self.dims + 1) // self.gap)
        self.owned_pairs = self.clusters // self.rows // 2
        self.keep = self.devices * self.pairs * 3 * LANES * 4 <= 1 << 20
        self.fixed_marks = 10
        self.chunk = min(self.cells, 1024)
        self.chunks = self.cells // self.chunk

    def at(self, c):
        return slice(c * self.chunk, (c + 1) * self.chunk)


def count_kernel(
    plan, pop_hbm, lam_hbm, scale_hbm, means_hbm, x_hbm, send, prior, counts, sizes, places, parts, xs, info, ridges,
    pop, lam, scale, means, ends, ms, seg, sems, small,
):
    k = plan.clusters
    inputs = [
        pltpu.make_async_copy(source, target, small.at[i])
        for i, (source, target) in enumerate(
            ((pop_hbm, pop), (means_hbm, means), (scale_hbm, scale), (lam_hbm, lam))
        )
    ]
    copies = [
        pltpu.make_async_copy(x_hbm.at[:, plan.at(c)], xs.at[:, plan.at(c)], sems.at[c])
        for c in range(plan.chunks)
    ]
    for copy in inputs + copies:
        copy.start()
    offset = (lax.axis_index("cells") * plan.cols + lax.axis_index("grp")) * plan.cells
    for copy in inputs:
        copy.wait()
    copies[0].wait()
    running, first = jnp.int32(0), jnp.int32(0)
    for b in range(plan.batches):
        running = running + pop[b]
        ends[b] = running
        first = first + (running <= offset).astype(i32)

    ms[...] = jnp.zeros_like(ms)
    ms[:, 0 : plan.dims] = means[...]
    m = ms[...]
    m1, m2, m3 = [part.astype(f32) for part in split(m, 3)]
    zero = jnp.zeros_like(m)

    def twice(value):
        return value + pltpu.roll(value, HALF, 1)

    weights = jnp.concatenate(
        [
            jnp.concatenate([twice(m1), m1], axis=1),
            jnp.concatenate([twice(m2), zero], axis=1),
            jnp.concatenate([m3, zero], axis=1),
        ],
        axis=0,
    ).astype(bf16)
    lengths = jnp.sum(m * m, axis=1, keepdims=True)
    soft = jnp.ones((k, 1), f32)
    row = iota((k, 1), 0)
    for c in range(k):
        soft = jnp.where(row == c, scale[c], soft)
    inverse = 1.0 / (2.0 * soft)
    low = plan.dims // 8 * 8
    over = plan.dims - low
    shape = (8, plan.chunk)
    tail_row = iota(shape, 0)
    constant = jnp.where(tail_row == over, 1.0, 0.0)
    rest = [jnp.zeros(shape, f32)] * ((HALF - low) // 8 - 1)
    for c in range(plan.chunks):
        at = plan.at(c)
        if c:
            copies[c].wait()
        if over:
            moved = pltpu.roll(xs[plan.dims - 8 : plan.dims, at], over, 0)
            tail = jnp.where(tail_row < over, moved, constant)
        else:
            tail = constant
        x = jnp.concatenate([xs[0:low, at], tail] + rest, axis=0)
        x1, x2, x3 = split(x, 3)
        parts[0:HALF, at] = x1
        parts[HALF:, at] = x2
        stacked = jnp.concatenate([x1, x2, x3, jnp.zeros_like(x1)], axis=0)
        dots = jnp.dot(weights, stacked, preferred_element_type=f32)
        dots = dots[0:k] + dots[k : 2 * k] + dots[2 * k : 3 * k]
        scores = (2.0 * dots - lengths) * inverse
        raised = jnp.exp(scores - jnp.max(scores, axis=0, keepdims=True))
        chance = raised / jnp.sum(raised, axis=0, keepdims=True)
        prior[:, at] = chance

    def following(held):
        return held[0] + 1, ends[held[0] + 1]

    last, unused = lax.while_loop(
        lambda held: held[1] < offset + plan.cells, following, (first, ends[first])
    )
    segments = last - first + 1
    tiles = lax.div(segments + TILE - 1, TILE)
    info[0], info[1], info[2] = first, last, segments

    lane = iota((1, LANES), 1)
    cell = iota((8, plan.cells), 1)
    half = TILE // 2
    seg[...] = jnp.zeros_like(seg)

    def locate(g, carry):
        held = seg[...]
        for j in range(half):
            s = g * half + j
            b = jnp.minimum(first + s, plan.batches - 1)
            held = jnp.where(cell >= ends[b] - offset, (s + 1).astype(f32), held)
        seg[...] = held
        return carry

    lax.fori_loop(0, lax.div(segments + half - 1, half), locate, 0)
    places[...] = jnp.concatenate([seg[...]] * (TILE // 8), axis=0).astype(bf16)

    def note(g, carry):
        row = jnp.zeros((1, LANES), f32)
        for j in range(TILE):
            b = jnp.minimum(first + g * TILE + j, plan.batches - 1)
            ridges[g * TILE + j] = lam[b]
            row = jnp.where(lane == j, pop[b].astype(f32), row)
        sizes[pl.ds(g, 1), :] = row
        return carry

    lax.fori_loop(0, tiles, note, 0)

    def settle(g, found):
        found = found[0:k] + found[k : 2 * k] + found[2 * k :]
        counts[g] = jnp.concatenate([found, jnp.zeros((k, LANES - TILE), f32)], axis=1)

    def count(g, carry):
        rows = (iota((TILE, plan.cells), 0) + g * TILE).astype(f32).astype(bf16)
        hot = jnp.where(places[...] == rows, bf16(1), bf16(0))
        settle(
            g,
            lax.dot_general(
                jnp.concatenate(split(prior[...], 3), axis=0), hot, BY_CELLS, preferred_element_type=f32
            ),
        )
        return carry

    lax.fori_loop(0, tiles, count, 0)

    every = lax.fori_loop(1, tiles, lambda g, total: total + counts[g], counts[0])
    total = jnp.sum(every, axis=1, keepdims=True)
    here = segments - 1
    end = counts[lax.div(here, TILE)]
    wide = iota((k, LANES), 1)
    last_count = jnp.sum(jnp.where(wide == lax.rem(here, TILE), end, 0.0), axis=1, keepdims=True)
    first_count = jnp.where(segments > 1, counts[0][:, 0:1], 0.0)
    spread = (k, plan.width)
    turn = iota(spread, 1) - iota(spread, 0)
    out = jnp.where(turn == 0, total, 0.0)
    out = jnp.where(turn == k, first_count, out)
    out = jnp.where(turn == 2 * k, last_count, out)
    out = jnp.sum(out, axis=0, keepdims=True)
    lanes = iota((1, plan.width), 1)
    out = jnp.where(lanes == 3 * k, first.astype(f32), out)
    out = jnp.where(lanes == 3 * k + 1, last.astype(f32), out)
    out = jnp.where(lanes == 3 * k + 2, lam[first], out)
    out = jnp.where(lanes == 3 * k + 3, lam[last], out)
    send[...] = jnp.broadcast_to(out, send.shape)


def masked(plan, a1, a2, places, g, at):
    k = plan.clusters
    width = at.stop - at.start
    shape = (TILE, width)
    base = jnp.full(shape, (g * plan.group).astype(f32) if not isinstance(g, int) else f32(g * plan.group))
    relative = places[:, at] - base.astype(bf16)
    out = []
    for a in (a1[:, at], a2[:, at]):
        for j in range(plan.group):
            inside = jnp.concatenate([relative] * (k // TILE), axis=0) == bf16(j)
            out.append(jnp.where(inside, a, bf16(0)))
    return jnp.concatenate(out, axis=0)


def moment_kernel(
    plan, info, ridges, got, prior, counts, sizes, places, parts, send, a1, a2, moments, wide, sums, turned
):
    k = plan.clusters
    first, last, segments = info[0], info[1], info[2]
    groups = lax.div(segments + plan.group - 1, plan.group)
    tiles = lax.div(segments + TILE - 1, TILE)

    table = got[...]
    total = column(jnp.sum(table, axis=0, keepdims=True), 0, k)
    heads, tails = table[:, 3 * k : 3 * k + 1], table[:, 3 * k + 1 : 3 * k + 2]

    def complete(batch):
        batch = batch.astype(f32)
        of_heads = jnp.sum(jnp.where(heads == batch, table, 0.0), axis=0, keepdims=True)
        of_tails = jnp.sum(jnp.where(tails == batch, table, 0.0), axis=0, keepdims=True)
        return column(of_heads, k, k) + column(of_tails, 2 * k, k)

    first_count, last_count = complete(first), complete(last)
    share = total / f32(plan.total)
    lane = iota((k, LANES), 1)

    def factors(g):
        held = counts[g]
        held = jnp.where(lane + g * TILE == 0, first_count, held)
        held = jnp.where(lane + g * TILE == segments - 1, last_count, held)
        ratio = (sizes[pl.ds(g, 1), :] * share + 1.0) / (held + 1.0)
        ratio = jnp.where(lane < TILE, ratio * ratio, 0.0)
        w1, w2, w3 = [part.astype(f32) for part in split(ratio, 3)]
        row = w1 + pltpu.roll(w2, TILE, 1) + pltpu.roll(w3, 2 * TILE, 1)
        return row.astype(bf16)[:, 0 : 4 * TILE]

    def factor_of(weights, g, at):
        shape = (TILE, at.stop - at.start)
        rows = (iota(shape, 0) + g * TILE).astype(f32).astype(bf16)
        hot = jnp.where(places[:, at] == rows, bf16(1), bf16(0))
        hot = jnp.concatenate([hot, hot, hot, jnp.zeros_like(hot)], axis=0)
        return jnp.dot(weights, hot, preferred_element_type=f32)

    weights = factors(0)
    for c in range(plan.chunks):
        wide[:, plan.at(c)] = factor_of(weights, 0, plan.at(c))

    def more(g, carry):
        weights = factors(g)
        for c in range(plan.chunks):
            wide[:, plan.at(c)] += factor_of(weights, g, plan.at(c))
        return carry

    lax.fori_loop(1, tiles, more, 0)
    for c in range(plan.chunks):
        at = plan.at(c)
        raised = prior[:, at] * wide[:, at]
        a1[:, at], a2[:, at] = split(raised / jnp.sum(raised, axis=0, keepdims=True), 2)

    sums[...] = jnp.zeros_like(sums)

    def gather(g, carry):
        both = jnp.zeros((2 * plan.depth, LANES), f32)
        for c in range(plan.chunks):
            at = plan.at(c)
            both = both + lax.dot_general(
                masked(plan, a1, a2, places, g, at), parts[:, at], BY_CELLS, preferred_element_type=f32
            )
        both = both[0 : plan.depth] + both[plan.depth :]
        both = both + pltpu.roll(both, HALF, 1)
        moments[pl.ds(pl.multiple_of(g * plan.depth, plan.depth), plan.depth), :] = both
        mass = lane_of(both, plan.dims)
        inner, head, tail, every = sums[0], sums[1], sums[2], sums[3]
        for j in range(plan.group):
            s = g * plan.group + j
            at = slice(j * k, (j + 1) * k)
            ridge = ridges[s]
            part = both[at]
            every = every + part
            shrunk = part * (ridge / (mass[at] + ridge))
            inner = inner + jnp.where((s > 0) & (s < segments - 1), shrunk, 0.0)
            head = head + jnp.where((s == 0) & (segments > 1), part, 0.0)
            tail = tail + jnp.where(s == segments - 1, part, 0.0)
        sums[0], sums[1], sums[2], sums[3] = inner, head, tail, every
        return carry

    lax.fori_loop(0, groups, gather, 0)
    inner, head, tail, every = [pack_pairs(sums.at[i]) for i in range(4)]
    lanes = lax.rem(iota(inner.shape, 1), HALF)
    inner = jnp.where(lanes <= plan.dims, inner, 0.0)
    every = jnp.where(lanes <= plan.dims, every, 0.0)
    for j in range(plan.gap_rows):
        moved = pltpu.roll(every, (plan.dims + 1 - plan.gap * j) % LANES, 1)
        turned[j] = jnp.where(lanes > plan.dims, moved, 0.0)
    row = iota((plan.part, LANES), 0)

    def put(c, carry):
        gaps = jnp.zeros((plan.part, LANES), f32)
        for q in range(plan.owned_pairs):
            for j in range(plan.gap_rows):
                pair = c * plan.owned_pairs + q
                piece = jnp.broadcast_to(turned[j, pl.ds(pair, 1), :], gaps.shape)
                gaps = gaps + jnp.where(row == q * plan.gap_rows + j, piece, 0.0)
        for q in range(plan.cols):
            p = c * plan.cols + q
            for side in range(2):
                low = side * plan.part

                def write(low=low, p=p):
                    start = p * 3 * plan.part
                    send[pl.ds(start, plan.part), :] = inner[low : low + plan.part] + gaps
                    send[pl.ds(start + plan.part, plan.part), :] = head[low : low + plan.part]
                    send[pl.ds(start + 2 * plan.part, plan.part), :] = tail[low : low + plan.part]

                if isinstance(p, int):
                    if p % 2 == side:
                        write()
                else:
                    pl.when(lax.rem(p, 2) == side)(write)
        return carry

    repeat(plan.rows, put)


def reduce_kernel(plan, info, got, ids, mine, theirs, marks):
    k, part = plan.clusters, plan.part
    shape = (plan.devices, LANES)
    device = iota(shape, 0)

    def of(lane):
        return jnp.broadcast_to(ids[:, lane : lane + 1], shape)

    heads, tails = of(3 * k), of(3 * k + 1)
    me = lax.axis_index("cells") * plan.cols + lax.axis_index("grp")
    other = me + 1 - 2 * lax.rem(me, 2)

    def shifted(value, distance):
        return pltpu.roll(value, distance % plan.devices, 0)

    marks[0], marks[1] = of(3 * k + 2), of(3 * k + 3)
    own = ids[pl.ds(me, 1), :]
    pair = ids[pl.ds(other, 1), :]
    for i, (row, lane) in enumerate(((own, 3 * k), (own, 3 * k + 1), (pair, 3 * k), (pair, 3 * k + 1))):
        batch = jnp.broadcast_to(row[:, lane : lane + 1], shape)
        marks[2 + 2 * i] = jnp.where(heads == batch, 1.0, 0.0)
        marks[3 + 2 * i] = jnp.where(tails == batch, 1.0, 0.0)
    links = []

    def link(hop, to_head, from_head, mine, theirs):
        inside = (device + hop >= 0) & (device + hop < plan.devices)
        at = plan.fixed_marks + len(links)
        marks[at] = jnp.where(inside & (shifted(theirs, -hop) == mine), 1.0, 0.0)
        links.append((at, hop, to_head, from_head))

    for hop in range(1, plan.reach + 1):
        link(-hop, True, False, heads, tails)
        link(hop, False, True, tails, heads)
        if plan.lone:
            link(-hop, False, False, tails, tails)
            link(hop, False, False, tails, tails)

    block = (2 * part, LANES)
    top = iota(block, 0) < part

    def mark(i, r):
        return jnp.broadcast_to(marks[i, pl.ds(r, 1), :], block)

    def two(i, r):
        return jnp.where(top, mark(i, r), mark(i + 1, r))

    def ends_of(r):
        return got[pl.ds(r * 3 * part + part, 2 * part), :]

    def turn(value):
        return pltpu.roll(value, part, 0)

    def gather(r, carry):
        inner, shrunk, sums = carry
        ends = ends_of(r)
        whole = halves(ends, plan.dims)
        for at, hop, to_head, from_head in links:
            if isinstance(r, int):
                if not 0 <= r + hop < plan.devices:
                    continue
                there = r + hop
            else:
                there = jnp.clip(r + hop, 0, plan.devices - 1)
            mass = halves(ends_of(there), plan.dims)
            if to_head != from_head:
                mass = turn(mass)
            whole = whole + jnp.where(top == to_head, mark(at, r) * mass, 0.0)
        ridge = two(0, r)
        shrunk = shrunk + ends * (ridge / (whole + ridge))
        inner = inner + got[pl.ds(r * 3 * part, part), :]
        sums = tuple(total + ends * two(2 + 2 * i, r) for i, total in enumerate(sums))
        return inner, shrunk, sums

    zero = jnp.zeros(block, f32)
    state = (zero[0:part], zero, (zero,) * 4)
    if plan.devices <= 32:
        for r in range(plan.devices):
            state = gather(r, state)
    else:
        state = lax.fori_loop(0, plan.devices, gather, state)
    inner, shrunk, sums = state

    def fold(value):
        return (value + turn(value))[0:part]

    right = inner + fold(shrunk)
    intercept = right / (1.0 + halves(right, plan.dims))
    mine[0] = jnp.concatenate([intercept, intercept], axis=0)
    theirs[0:part] = intercept
    for i in range(2):
        value = sums[i] + turn(sums[i])
        mine[1 + i] = value
        theirs[(1 + i) * part : (2 + i) * part] = fold(sums[2 + i])
    mine[3] = jnp.concatenate([inner, inner], axis=0)


def correct_kernel(
    plan, info, ridges, mine, theirs, a1, a2, moments, places, xs, out_hbm, centroids_hbm,
    slopes, rows, spread, out, centroids, sems, done,
):
    k, part = plan.clusters, plan.part
    first, last, segments = info[0], info[1], info[2]
    groups = lax.div(segments + plan.group - 1, plan.group)
    me = lax.axis_index("cells") * plan.cols + lax.axis_index("grp")
    odd = jnp.full((plan.pairs, LANES), lax.rem(me, 2)) == 1
    low = iota((plan.pairs, LANES), 0) < part

    def both(i):
        piece = theirs[i * part : (i + 1) * part]
        piece = jnp.concatenate([piece, piece], axis=0)
        return unpack_pairs(spread, jnp.where(low != odd, mine[i], piece))

    intercept, first_sum, last_sum = both(0), both(1), both(2)
    left = iota((k, LANES), 1) < HALF

    def slope(g, carry):
        start = pl.multiple_of(g * plan.depth, plan.depth)
        held = moments[pl.ds(start, plan.depth), :]
        made = []
        for j in range(plan.group):
            s = g * plan.group + j
            part = held[j * k : (j + 1) * k]
            part = jnp.where(s == 0, first_sum, part)
            part = jnp.where(s == segments - 1, last_sum, part)
            mass = lane_of(part, plan.dims)
            ridge = ridges[s]
            s1, s2 = split((part - mass * intercept) / (mass + ridge), 2)
            made.append(jnp.where(left, s1.astype(f32), s2.astype(f32)))
        slopes[g] = jnp.transpose(jnp.concatenate(made, axis=0)).astype(bf16)
        return carry

    lax.fori_loop(0, groups, slope, 0)

    def move(g, at):
        mine = slopes[g]
        moved = jnp.dot(
            jnp.concatenate([mine, mine], axis=1),
            masked(plan, a1, a2, places, g, at),
            preferred_element_type=f32,
        )
        return (moved[0:HALF] + moved[HALF:])[0 : plan.dims]

    rows[...] = mine[3]
    lanes = lax.rem(iota((1, LANES), 1), HALF)
    for q in range(plan.owned_pairs):
        every = jnp.zeros((1, LANES), f32)
        for j in range(plan.gap_rows):
            at = q * plan.gap_rows + j
            piece = jnp.where(lanes > plan.dims, rows[at : at + 1], 0.0)
            moved = pltpu.roll(piece, (plan.gap * j - plan.dims - 1) % LANES, 1)
            inside = (lanes >= plan.gap * j) & (lanes < plan.gap * (j + 1))
            every = every + jnp.where(inside, moved, 0.0)
        every = every / (1.0 + halves(every, plan.dims))
        centroids[2 * q : 2 * q + 1] = every[:, 0 : plan.dims]
        centroids[2 * q + 1 : 2 * q + 2] = pltpu.roll(every, HALF, 1)[:, 0 : plan.dims]
    last_copy = pltpu.make_async_copy(centroids, centroids_hbm, done)
    last_copy.start()
    copies = []
    for c in range(plan.chunks):
        at = plan.at(c)
        out[:, at] = xs[:, at]

        def again(g, carry):
            out[:, at] = out[:, at] - move(g, at)
            return carry

        lax.fori_loop(0, groups, again, 0)
        copies.append(pltpu.make_async_copy(out.at[:, at], out_hbm.at[:, at], sems.at[c]))
        copies[-1].start()

    for copy in copies:
        copy.wait()
    last_copy.wait()


VMEM = pl.BlockSpec(memory_space=pltpu.VMEM)
SMEM = pl.BlockSpec(memory_space=pltpu.SMEM)
WHERE = pl.BlockSpec(memory_space=pltpu.HBM)


def hold_scalars(value):
    return pltpu.with_memory_space_constraint(value, pltpu.SMEM)


def bound(kernel, plan, name):
    def run(*refs):
        kernel(plan, *refs)

    run.__name__ = name
    return run


def body(x, means, scale, lam, pop):
    plan = Plan(x, means, pop)
    k, cells = plan.clusters, plan.cells
    params = pltpu.CompilerParams(vmem_limit_bytes=(16 << 20) if plan.keep else None)

    def kept(shape, kind=f32):
        return pltpu.VMEM(shape, kind) if plan.keep else jax.ShapeDtypeStruct(shape, kind)

    def hold(value):
        return pltpu.with_memory_space_constraint(value, pltpu.VMEM) if plan.keep else value

    send, prior, counts, sizes, places, parts, xs, info, ridges = pl.pallas_call(
        bound(count_kernel, plan, "count"),
        name="count",
        out_shape=(
            kept((plan.devices, plan.width)),
            kept((k, cells)),
            kept((plan.tiles, k, LANES)),
            kept((plan.tiles, LANES)),
            kept((TILE, cells), bf16),
            kept((2 * HALF, cells), bf16),
            kept((plan.dims, cells)),
            pltpu.SMEM((4,), i32),
            pltpu.SMEM((plan.local,), f32),
        ),
        in_specs=[WHERE] * 5,
        out_specs=(VMEM,) * 7 + (SMEM,) * 2,
        scratch_shapes=[
            pltpu.SMEM(pop.shape, i32),
            pltpu.SMEM(lam.shape, f32),
            pltpu.SMEM(scale.shape, f32),
            pltpu.VMEM(means.shape, f32),
            pltpu.SMEM((plan.batches + 1,), i32),
            pltpu.VMEM((k, LANES), f32),
            pltpu.VMEM((8, cells), f32),
            pltpu.SemaphoreType.DMA((plan.chunks,)),
            pltpu.SemaphoreType.DMA((4,)),
        ],
    )(pop, lam, scale, means, x)
    prior, counts, sizes, places, parts, xs = map(hold, (prior, counts, sizes, places, parts, xs))
    info, ridges = hold_scalars(info), hold_scalars(ridges)
    ids = hold(lax.all_to_all(send, AXES, 0, 0, tiled=True))
    send, a1, a2, moments = pl.pallas_call(
        bound(moment_kernel, plan, "moment"),
        name="moment",
        compiler_params=params,
        out_shape=(
            kept((plan.devices * 3 * plan.part, LANES)),
            kept((k, cells), bf16),
            kept((k, cells), bf16),
            kept((plan.groups * plan.depth, LANES)),
        ),
        in_specs=[SMEM] * 2 + [VMEM] * 6,
        out_specs=(VMEM,) * 4,
        scratch_shapes=[
            pltpu.VMEM((k, cells), f32),
            pltpu.VMEM((4, k, LANES), f32),
            pltpu.VMEM((plan.gap_rows, plan.pairs, LANES), f32),
        ],
    )(info, ridges, ids, prior, counts, sizes, places, parts)
    a1, a2, moments = map(hold, (a1, a2, moments))
    rows = send.shape[0]
    got = lax.all_to_all(send.reshape(rows, 1, LANES), AXES, 0, 0, tiled=True)
    got = hold(got.reshape(rows, LANES))
    marks = plan.fixed_marks + plan.reach * (4 if plan.lone else 2)
    mine, theirs = pl.pallas_call(
        bound(reduce_kernel, plan, "reduce"),
        name="reduce",
        compiler_params=params,
        out_shape=(kept((4, plan.pairs, LANES)), kept((3 * plan.part, LANES))),
        in_specs=[SMEM] + [VMEM] * 2,
        out_specs=(VMEM,) * 2,
        scratch_shapes=[pltpu.VMEM((marks, plan.devices, LANES), f32)],
    )(info, got, ids)
    mine = hold(mine)
    swap = [(i, i + 1 - 2 * (i % 2)) for i in range(plan.devices)]
    theirs = hold(lax.ppermute(theirs, AXES, swap))
    corrected, centroids = pl.pallas_call(
        bound(correct_kernel, plan, "correct"),
        name="correct",
        compiler_params=params,
        out_shape=(
            jax.ShapeDtypeStruct(x.shape, f32),
            jax.ShapeDtypeStruct((k // plan.rows, plan.dims), f32),
        ),
        in_specs=[SMEM] * 2 + [VMEM] * 7,
        out_specs=(WHERE, WHERE),
        scratch_shapes=[
            pltpu.VMEM((plan.groups, LANES, plan.depth), bf16),
            pltpu.VMEM((plan.pairs, LANES), f32),
            pltpu.VMEM((k, LANES), f32),
            pltpu.VMEM((plan.dims, cells), f32),
            pltpu.VMEM((k // plan.rows, plan.dims), f32),
            pltpu.SemaphoreType.DMA((plan.chunks,)),
            pltpu.SemaphoreType.DMA,
        ],
    )(info, ridges, mine, theirs, a1, a2, moments, places, xs)
    return corrected, centroids


def solution(mesh):
    return jax.shard_map(
        body,
        mesh=mesh,
        in_specs=(P(None, AXES), P(), P(), P(), P()),
        out_specs=(P(None, AXES), P("cells", None)),
        check_vma=False,
    )
```

```python
import jax
import jax.numpy as jnp
from jax import lax
from jax.experimental import pallas as pl
from jax.experimental.pallas import tpu as pltpu
from jax.sharding import PartitionSpec as P

f32 = jnp.float32
bf16 = jnp.bfloat16
i32 = jnp.int32
HALF = 64
LANES = 128
TILE = 16
AXES = ("cells", "grp")
BY_CELLS = (((1,), (1,)), ((), ()))
BY_ROWS = (((0,), (0,)), ((), ()))


def iota(shape, axis):
    return lax.broadcasted_iota(i32, shape, axis)


def split(value, parts):
    out = []
    for i in range(parts):
        out.append(value.astype(bf16))
        if i + 1 < parts:
            value = value - out[-1].astype(f32)
    return out


def lane_of(value, lane):
    return jnp.broadcast_to(value[:, lane : lane + 1], value.shape)


def halves(value, lane):
    left = iota(value.shape, 1) < HALF
    return jnp.where(left, lane_of(value, lane), lane_of(value, HALF + lane))


def column(row, first, count):
    shape = (count, row.shape[1])
    pick = iota(shape, 1) == iota(shape, 0) + first
    return jnp.sum(jnp.where(pick, jnp.broadcast_to(row, shape), 0.0), axis=1, keepdims=True)


def pack_pairs(ref):
    pairs = ref.shape[0] // 2
    even = ref[pl.ds(0, pairs, stride=2), :]
    odd = ref[pl.ds(1, pairs, stride=2), :]
    return jnp.where(iota(even.shape, 1) < HALF, even, odd)


def unpack_pairs(ref, tile):
    pairs = tile.shape[0]
    left = iota(tile.shape, 1) < HALF
    turned = pltpu.roll(tile, HALF, 1)
    ref[pl.ds(0, pairs, stride=2), :] = jnp.where(left, tile, turned)
    ref[pl.ds(1, pairs, stride=2), :] = jnp.where(left, turned, tile)
    return ref[...]


def repeat(count, step):
    if count <= 32:
        for i in range(count):
            step(i, 0)
    else:
        lax.fori_loop(0, count, step, 0)


class Plan:
    def __init__(self, x, means, pop):
        self.dims, self.cells = x.shape
        self.clusters = means.shape[0]
        self.batches = pop.shape[0]
        self.rows = lax.axis_size("cells")
        self.cols = lax.axis_size("grp")
        self.devices = self.rows * self.cols
        self.total = self.cells * self.devices
        self.most = 2 * self.total // self.batches
        self.reach = (self.most - 2) // self.cells + 1
        self.lone = self.most >= self.cells
        outside = -(-(self.total - self.cells) // self.most)
        local = min(self.batches, self.batches - outside + 2)
        self.tiles = -(-local // TILE)
        self.local = self.tiles * TILE
        self.group = max(1, LANES // self.clusters)
        self.groups = self.local // self.group
        self.depth = self.group * self.clusters
        self.width = -(-(3 * self.clusters + 4) // LANES) * LANES
        self.pairs = self.clusters // 2
        self.part = self.pairs // 2
        self.gap = HALF - (self.dims + 1)
        self.gap_rows = -(-(self.dims + 1) // self.gap)
        self.owned_pairs = self.clusters // self.rows // 2
        self.keep = self.devices * self.pairs * 3 * LANES * 4 <= 1 << 20
        self.fixed_marks = 10
        self.window = min(self.group, 4)
        self.piece = min(self.cells, 512)
        self.pieces = self.cells // self.piece
        self.chunk = min(self.cells, 1024)
        self.chunks = self.cells // self.chunk

    def at(self, c):
        return slice(c * self.chunk, (c + 1) * self.chunk)


def count_kernel(
    plan, pop_hbm, lam_hbm, scale_hbm, means_hbm, x_hbm, send, prior, counts, sizes, places, parts, xs, info, ridges,
    pop, lam, scale, means, ends, ms, seg, sems, small,
):
    k = plan.clusters
    inputs = [
        pltpu.make_async_copy(source, target, small.at[i])
        for i, (source, target) in enumerate(
            ((pop_hbm, pop), (means_hbm, means), (scale_hbm, scale), (lam_hbm, lam))
        )
    ]
    copies = [
        pltpu.make_async_copy(x_hbm.at[:, plan.at(c)], xs.at[:, plan.at(c)], sems.at[c])
        for c in range(plan.chunks)
    ]
    for copy in inputs + copies:
        copy.start()
    offset = (lax.axis_index("cells") * plan.cols + lax.axis_index("grp")) * plan.cells
    for copy in inputs + copies:
        copy.wait()
    running, first = jnp.int32(0), jnp.int32(0)
    for b in range(plan.batches):
        running = running + pop[b]
        ends[b] = running
        first = first + (running <= offset).astype(i32)

    ms[...] = jnp.zeros_like(ms)
    ms[:, 0 : plan.dims] = means[...]
    m = ms[...]
    m1, m2, m3 = [part.astype(f32) for part in split(m, 3)]
    zero = jnp.zeros_like(m)

    def twice(value):
        return value + pltpu.roll(value, HALF, 1)

    weights = jnp.concatenate(
        [
            jnp.concatenate([twice(m1), m1], axis=1),
            jnp.concatenate([twice(m2), zero], axis=1),
            jnp.concatenate([m3, zero], axis=1),
        ],
        axis=0,
    ).astype(bf16)
    lengths = jnp.sum(m * m, axis=1, keepdims=True)
    soft = jnp.ones((k, 1), f32)
    row = iota((k, 1), 0)
    for c in range(k):
        soft = jnp.where(row == c, scale[c], soft)
    inverse = 1.0 / (2.0 * soft)
    low = plan.dims // 8 * 8
    over = plan.dims - low
    shape = (8, plan.chunk)
    tail_row = iota(shape, 0)
    constant = jnp.where(tail_row == over, 1.0, 0.0)
    rest = [jnp.zeros(shape, f32)] * ((HALF - low) // 8 - 1)
    for c in range(plan.chunks):
        at = plan.at(c)
        if over:
            moved = pltpu.roll(xs[plan.dims - 8 : plan.dims, at], over, 0)
            tail = jnp.where(tail_row < over, moved, constant)
        else:
            tail = constant
        x = jnp.concatenate([xs[0:low, at], tail] + rest, axis=0)
        x1, x2, x3 = split(x, 3)
        parts[0:HALF, at] = x1
        parts[HALF:, at] = x2
        stacked = jnp.concatenate([x1, x2, x3, jnp.zeros_like(x1)], axis=0)
        dots = jnp.dot(weights, stacked, preferred_element_type=f32)
        dots = dots[0:k] + dots[k : 2 * k] + dots[2 * k : 3 * k]
        scores = (2.0 * dots - lengths) * inverse
        raised = jnp.exp(scores - jnp.max(scores, axis=0, keepdims=True))
        chance = raised / jnp.sum(raised, axis=0, keepdims=True)
        prior[:, at] = chance

    last = first
    for c in range(plan.pieces + 1):
        bound = offset + min(c * plan.piece, plan.cells - 1)

        def beyond(b, bound=bound):
            return ends[b] <= bound

        last = lax.while_loop(beyond, lambda b: b + 1, last)
        info[4 + c] = last - first
    segments = last - first + 1
    tiles = lax.div(segments + TILE - 1, TILE)
    info[0], info[1], info[2] = first, last, segments

    lane = iota((1, LANES), 1)
    cell = iota((8, plan.cells), 1)
    half = TILE // 2
    seg[...] = jnp.zeros_like(seg)

    def locate(g, carry):
        held = seg[...]
        for j in range(half):
            s = g * half + j
            b = jnp.minimum(first + s, plan.batches - 1)
            held = jnp.where(cell >= ends[b] - offset, (s + 1).astype(f32), held)
        seg[...] = held
        return carry

    lax.fori_loop(0, lax.div(segments + half - 1, half), locate, 0)
    places[...] = jnp.concatenate([seg[...]] * (TILE // 8), axis=0).astype(bf16)

    def note(g, carry):
        row = jnp.zeros((1, LANES), f32)
        for j in range(TILE):
            b = jnp.minimum(first + g * TILE + j, plan.batches - 1)
            ridges[g * TILE + j] = lam[b]
            row = jnp.where(lane == j, pop[b].astype(f32), row)
        sizes[pl.ds(g, 1), :] = row
        return carry

    lax.fori_loop(0, tiles, note, 0)

    def settle(g, found):
        found = found[0:k] + found[k : 2 * k] + found[2 * k :]
        counts[g] = jnp.concatenate([found, jnp.zeros((k, LANES - TILE), f32)], axis=1)

    def count(g, carry):
        rows = (iota((TILE, plan.cells), 0) + g * TILE).astype(f32).astype(bf16)
        hot = jnp.where(places[...] == rows, bf16(1), bf16(0))
        settle(
            g,
            lax.dot_general(
                jnp.concatenate(split(prior[...], 3), axis=0), hot, BY_CELLS, preferred_element_type=f32
            ),
        )
        return carry

    lax.fori_loop(0, tiles, count, 0)

    every = lax.fori_loop(1, tiles, lambda g, total: total + counts[g], counts[0])
    total = jnp.sum(every, axis=1, keepdims=True)
    here = segments - 1
    end = counts[lax.div(here, TILE)]
    wide = iota((k, LANES), 1)
    last_count = jnp.sum(jnp.where(wide == lax.rem(here, TILE), end, 0.0), axis=1, keepdims=True)
    first_count = jnp.where(segments > 1, counts[0][:, 0:1], 0.0)
    spread = (k, plan.width)
    turn = iota(spread, 1) - iota(spread, 0)
    out = jnp.where(turn == 0, total, 0.0)
    out = jnp.where(turn == k, first_count, out)
    out = jnp.where(turn == 2 * k, last_count, out)
    out = jnp.sum(out, axis=0, keepdims=True)
    lanes = iota((1, plan.width), 1)
    out = jnp.where(lanes == 3 * k, first.astype(f32), out)
    out = jnp.where(lanes == 3 * k + 1, last.astype(f32), out)
    out = jnp.where(lanes == 3 * k + 2, lam[first], out)
    out = jnp.where(lanes == 3 * k + 3, lam[last], out)
    send[...] = jnp.broadcast_to(out, send.shape)


def masked(plan, a1, a2, places, base, at, order):
    base = jnp.full((TILE, plan.piece), base.astype(f32)).astype(bf16)
    relative = jnp.concatenate([places[:, at] - base] * (plan.clusters // TILE), axis=0)
    inside = [relative == bf16(j) for j in range(plan.window)]
    parts = [
        jnp.concatenate([jnp.where(here, a[:, at], bf16(0)) for here in inside], axis=0) for a in (a1, a2)
    ]
    return jnp.concatenate([parts[i] for i in order], axis=0)


def windows(plan, info, step):
    for c in range(plan.pieces):
        step(c, info[4 + c])
    more = [lax.div(info[5 + c] - info[4 + c], plan.window) for c in range(plan.pieces)]

    @pl.when(sum(more) > 0)
    def rest():
        for c in range(plan.pieces):

            def again(w, carry, c=c):
                step(c, info[4 + c] + w * plan.window)
                return carry

            lax.fori_loop(1, more[c] + 1, again, 0)


def moment_kernel(
    plan, info, ridges, got, prior, counts, sizes, places, parts, send, a1, a2, moments, wide, sums, turned
):
    k = plan.clusters
    first, last, segments = info[0], info[1], info[2]
    groups = lax.div(segments + plan.group - 1, plan.group)
    tiles = lax.div(segments + TILE - 1, TILE)

    table = got[...]
    total = column(jnp.sum(table, axis=0, keepdims=True), 0, k)
    heads, tails = table[:, 3 * k : 3 * k + 1], table[:, 3 * k + 1 : 3 * k + 2]

    def complete(batch):
        batch = batch.astype(f32)
        of_heads = jnp.sum(jnp.where(heads == batch, table, 0.0), axis=0, keepdims=True)
        of_tails = jnp.sum(jnp.where(tails == batch, table, 0.0), axis=0, keepdims=True)
        return column(of_heads, k, k) + column(of_tails, 2 * k, k)

    first_count, last_count = complete(first), complete(last)
    share = total / f32(plan.total)
    lane = iota((k, LANES), 1)

    def factors(g):
        held = counts[g]
        held = jnp.where(lane + g * TILE == 0, first_count, held)
        held = jnp.where(lane + g * TILE == segments - 1, last_count, held)
        ratio = (sizes[pl.ds(g, 1), :] * share + 1.0) / (held + 1.0)
        ratio = jnp.where(lane < TILE, ratio * ratio, 0.0)
        w1, w2, w3 = [part.astype(f32) for part in split(ratio, 3)]
        row = w1 + pltpu.roll(w2, TILE, 1) + pltpu.roll(w3, 2 * TILE, 1)
        return row.astype(bf16)[:, 0 : 4 * TILE]

    def factor_of(weights, g, at):
        shape = (TILE, at.stop - at.start)
        rows = (iota(shape, 0) + g * TILE).astype(f32).astype(bf16)
        hot = jnp.where(places[:, at] == rows, bf16(1), bf16(0))
        hot = jnp.concatenate([hot, hot, hot, jnp.zeros_like(hot)], axis=0)
        return jnp.dot(weights, hot, preferred_element_type=f32)

    weights = factors(0)
    for c in range(plan.chunks):
        wide[:, plan.at(c)] = factor_of(weights, 0, plan.at(c))

    def more(g, carry):
        weights = factors(g)
        for c in range(plan.chunks):
            wide[:, plan.at(c)] += factor_of(weights, g, plan.at(c))
        return carry

    lax.fori_loop(1, tiles, more, 0)
    for c in range(plan.chunks):
        at = plan.at(c)
        raised = prior[:, at] * wide[:, at]
        a1[:, at], a2[:, at] = split(raised / jnp.sum(raised, axis=0, keepdims=True), 2)

    sums[...] = jnp.zeros_like(sums)

    def clear(g, carry):
        moments[pl.ds(pl.multiple_of(g * plan.depth, plan.depth), plan.depth), :] = jnp.zeros(
            (plan.depth, LANES), f32
        )
        return carry

    lax.fori_loop(0, groups + 1, clear, 0)
    size = plan.window * k

    def collect(c, base):
        at = slice(c * plan.piece, (c + 1) * plan.piece)
        both = lax.dot_general(
            masked(plan, a1, a2, places, base, at, (0, 1)), parts[:, at], BY_CELLS, preferred_element_type=f32
        )
        to = pl.ds(pl.multiple_of(base * k, k), size)
        moments[to, :] = moments[to, :] + (both[0:size] + both[size:])

    windows(plan, info, collect)

    def gather(g, carry):
        to = pl.ds(pl.multiple_of(g * plan.depth, plan.depth), plan.depth)
        both = moments[to, :]
        both = both + pltpu.roll(both, HALF, 1)
        moments[to, :] = both
        mass = lane_of(both, plan.dims)
        inner, head, tail, every = sums[0], sums[1], sums[2], sums[3]
        for j in range(plan.group):
            s = g * plan.group + j
            at = slice(j * k, (j + 1) * k)
            ridge = ridges[s]
            part = both[at]
            every = every + part
            shrunk = part * (ridge / (mass[at] + ridge))
            inner = inner + jnp.where((s > 0) & (s < segments - 1), shrunk, 0.0)
            head = head + jnp.where((s == 0) & (segments > 1), part, 0.0)
            tail = tail + jnp.where(s == segments - 1, part, 0.0)
        sums[0], sums[1], sums[2], sums[3] = inner, head, tail, every
        return carry

    lax.fori_loop(0, groups, gather, 0)
    inner, head, tail, every = [pack_pairs(sums.at[i]) for i in range(4)]
    lanes = lax.rem(iota(inner.shape, 1), HALF)
    inner = jnp.where(lanes <= plan.dims, inner, 0.0)
    every = jnp.where(lanes <= plan.dims, every, 0.0)
    for j in range(plan.gap_rows):
        moved = pltpu.roll(every, (plan.dims + 1 - plan.gap * j) % LANES, 1)
        turned[j] = jnp.where(lanes > plan.dims, moved, 0.0)
    row = iota((plan.part, LANES), 0)

    def put(c, carry):
        gaps = jnp.zeros((plan.part, LANES), f32)
        for q in range(plan.owned_pairs):
            for j in range(plan.gap_rows):
                pair = c * plan.owned_pairs + q
                piece = jnp.broadcast_to(turned[j, pl.ds(pair, 1), :], gaps.shape)
                gaps = gaps + jnp.where(row == q * plan.gap_rows + j, piece, 0.0)
        for q in range(plan.cols):
            p = c * plan.cols + q
            for side in range(2):
                low = side * plan.part

                def write(low=low, p=p):
                    start = p * 3 * plan.part
                    send[pl.ds(start, plan.part), :] = inner[low : low + plan.part] + gaps
                    send[pl.ds(start + plan.part, plan.part), :] = head[low : low + plan.part]
                    send[pl.ds(start + 2 * plan.part, plan.part), :] = tail[low : low + plan.part]

                if isinstance(p, int):
                    if p % 2 == side:
                        write()
                else:
                    pl.when(lax.rem(p, 2) == side)(write)
        return carry

    repeat(plan.rows, put)


def reduce_kernel(plan, info, got, ids, mine, theirs, marks):
    k, part = plan.clusters, plan.part
    shape = (plan.devices, LANES)
    device = iota(shape, 0)

    def of(lane):
        return jnp.broadcast_to(ids[:, lane : lane + 1], shape)

    heads, tails = of(3 * k), of(3 * k + 1)
    me = lax.axis_index("cells") * plan.cols + lax.axis_index("grp")
    other = me + 1 - 2 * lax.rem(me, 2)

    def shifted(value, distance):
        return pltpu.roll(value, distance % plan.devices, 0)

    marks[0], marks[1] = of(3 * k + 2), of(3 * k + 3)
    own = ids[pl.ds(me, 1), :]
    pair = ids[pl.ds(other, 1), :]
    for i, (row, lane) in enumerate(((own, 3 * k), (own, 3 * k + 1), (pair, 3 * k), (pair, 3 * k + 1))):
        batch = jnp.broadcast_to(row[:, lane : lane + 1], shape)
        marks[2 + 2 * i] = jnp.where(heads == batch, 1.0, 0.0)
        marks[3 + 2 * i] = jnp.where(tails == batch, 1.0, 0.0)
    links = []

    def link(hop, to_head, from_head, mine, theirs):
        inside = (device + hop >= 0) & (device + hop < plan.devices)
        at = plan.fixed_marks + len(links)
        marks[at] = jnp.where(inside & (shifted(theirs, -hop) == mine), 1.0, 0.0)
        links.append((at, hop, to_head, from_head))

    for hop in range(1, plan.reach + 1):
        link(-hop, True, False, heads, tails)
        link(hop, False, True, tails, heads)
        if plan.lone:
            link(-hop, False, False, tails, tails)
            link(hop, False, False, tails, tails)

    block = (2 * part, LANES)
    top = iota(block, 0) < part

    def mark(i, r):
        return jnp.broadcast_to(marks[i, pl.ds(r, 1), :], block)

    def two(i, r):
        return jnp.where(top, mark(i, r), mark(i + 1, r))

    def ends_of(r):
        return got[pl.ds(r * 3 * part + part, 2 * part), :]

    def turn(value):
        return pltpu.roll(value, part, 0)

    def gather(r, carry):
        inner, shrunk, sums = carry
        ends = ends_of(r)
        whole = halves(ends, plan.dims)
        for at, hop, to_head, from_head in links:
            if isinstance(r, int):
                if not 0 <= r + hop < plan.devices:
                    continue
                there = r + hop
            else:
                there = jnp.clip(r + hop, 0, plan.devices - 1)
            mass = halves(ends_of(there), plan.dims)
            if to_head != from_head:
                mass = turn(mass)
            whole = whole + jnp.where(top == to_head, mark(at, r) * mass, 0.0)
        ridge = two(0, r)
        shrunk = shrunk + ends * (ridge / (whole + ridge))
        inner = inner + got[pl.ds(r * 3 * part, part), :]
        sums = tuple(total + ends * two(2 + 2 * i, r) for i, total in enumerate(sums))
        return inner, shrunk, sums

    zero = jnp.zeros(block, f32)
    state = (zero[0:part], zero, (zero,) * 4)
    if plan.devices <= 32:
        for r in range(plan.devices):
            state = gather(r, state)
    else:
        state = lax.fori_loop(0, plan.devices, gather, state)
    inner, shrunk, sums = state

    def fold(value):
        return (value + turn(value))[0:part]

    right = inner + fold(shrunk)
    intercept = right / (1.0 + halves(right, plan.dims))
    mine[0] = jnp.concatenate([intercept, intercept], axis=0)
    theirs[0:part] = intercept
    for i in range(2):
        value = sums[i] + turn(sums[i])
        mine[1 + i] = value
        theirs[(1 + i) * part : (2 + i) * part] = fold(sums[2 + i])
    mine[3] = jnp.concatenate([inner, inner], axis=0)


def correct_kernel(
    plan, info, ridges, mine, theirs, a1, a2, moments, places, xs, out_hbm, centroids_hbm,
    slopes, rows, spread, out, centroids, sems, done,
):
    k, part = plan.clusters, plan.part
    first, last, segments = info[0], info[1], info[2]
    groups = lax.div(segments + plan.group - 1, plan.group)
    me = lax.axis_index("cells") * plan.cols + lax.axis_index("grp")
    odd = jnp.full((plan.pairs, LANES), lax.rem(me, 2)) == 1
    low = iota((plan.pairs, LANES), 0) < part

    def both(i):
        piece = theirs[i * part : (i + 1) * part]
        piece = jnp.concatenate([piece, piece], axis=0)
        return unpack_pairs(spread, jnp.where(low != odd, mine[i], piece))

    intercept, first_sum, last_sum = both(0), both(1), both(2)
    def slope(g, carry):
        start = pl.multiple_of(g * plan.depth, plan.depth)
        held = moments[pl.ds(start, plan.depth), :]
        made = []
        for j in range(plan.group):
            s = g * plan.group + j
            part = held[j * k : (j + 1) * k]
            part = jnp.where(s == 0, first_sum, part)
            part = jnp.where(s == segments - 1, last_sum, part)
            mass = lane_of(part, plan.dims)
            ridge = ridges[s]
            made.append((part - mass * intercept) / (mass + ridge))
        for i, piece in enumerate(split(jnp.concatenate(made, axis=0), 2)):
            slopes[i, pl.ds(start, plan.depth), :] = piece
        return carry

    lax.fori_loop(0, groups, slope, 0)
    blank = jnp.zeros((plan.depth, LANES), bf16)
    for i in range(2):
        slopes[i, pl.ds(pl.multiple_of(groups * plan.depth, plan.depth), plan.depth), :] = blank
    size = plan.window * k

    rows[...] = mine[3]
    lanes = lax.rem(iota((1, LANES), 1), HALF)
    for q in range(plan.owned_pairs):
        every = jnp.zeros((1, LANES), f32)
        for j in range(plan.gap_rows):
            at = q * plan.gap_rows + j
            piece = jnp.where(lanes > plan.dims, rows[at : at + 1], 0.0)
            moved = pltpu.roll(piece, (plan.gap * j - plan.dims - 1) % LANES, 1)
            inside = (lanes >= plan.gap * j) & (lanes < plan.gap * (j + 1))
            every = every + jnp.where(inside, moved, 0.0)
        every = every / (1.0 + halves(every, plan.dims))
        centroids[2 * q : 2 * q + 1] = every[:, 0 : plan.dims]
        centroids[2 * q + 1 : 2 * q + 2] = pltpu.roll(every, HALF, 1)[:, 0 : plan.dims]
    last_copy = pltpu.make_async_copy(centroids, centroids_hbm, done)
    last_copy.start()
    out[...] = xs[...]

    def move(c, base):
        at = slice(c * plan.piece, (c + 1) * plan.piece)
        rows_of = pl.ds(pl.multiple_of(base * k, k), size)
        large, fine = slopes[0, rows_of, 0:HALF], slopes[1, rows_of, 0:HALF]
        moved = lax.dot_general(
            jnp.concatenate([large, fine, large], axis=0),
            masked(plan, a1, a2, places, base, at, (0, 0, 1)),
            BY_ROWS,
            preferred_element_type=f32,
        )
        out[:, at] = out[:, at] - moved[0 : plan.dims]

    windows(plan, info, move)
    copies = []
    for c in range(plan.chunks):
        at = plan.at(c)
        copies.append(pltpu.make_async_copy(out.at[:, at], out_hbm.at[:, at], sems.at[c]))
        copies[-1].start()
    for copy in copies:
        copy.wait()
    last_copy.wait()


VMEM = pl.BlockSpec(memory_space=pltpu.VMEM)
SMEM = pl.BlockSpec(memory_space=pltpu.SMEM)
WHERE = pl.BlockSpec(memory_space=pltpu.HBM)


def hold_scalars(value):
    return pltpu.with_memory_space_constraint(value, pltpu.SMEM)


def bound(kernel, plan, name):
    def run(*refs):
        kernel(plan, *refs)

    run.__name__ = name
    return run


def body(x, means, scale, lam, pop):
    plan = Plan(x, means, pop)
    k, cells = plan.clusters, plan.cells
    params = pltpu.CompilerParams(vmem_limit_bytes=(16 << 20) if plan.keep else None)

    def kept(shape, kind=f32):
        return pltpu.VMEM(shape, kind) if plan.keep else jax.ShapeDtypeStruct(shape, kind)

    def hold(value):
        return pltpu.with_memory_space_constraint(value, pltpu.VMEM) if plan.keep else value

    send, prior, counts, sizes, places, parts, xs, info, ridges = pl.pallas_call(
        bound(count_kernel, plan, "count"),
        name="count",
        out_shape=(
            kept((plan.devices, plan.width)),
            kept((k, cells)),
            kept((plan.tiles, k, LANES)),
            kept((plan.tiles, LANES)),
            kept((TILE, cells), bf16),
            kept((2 * HALF, cells), bf16),
            kept((plan.dims, cells)),
            pltpu.SMEM((5 + plan.pieces,), i32),
            pltpu.SMEM((plan.local,), f32),
        ),
        in_specs=[WHERE] * 5,
        out_specs=(VMEM,) * 7 + (SMEM,) * 2,
        scratch_shapes=[
            pltpu.SMEM(pop.shape, i32),
            pltpu.SMEM(lam.shape, f32),
            pltpu.SMEM(scale.shape, f32),
            pltpu.VMEM(means.shape, f32),
            pltpu.SMEM((plan.batches + 1,), i32),
            pltpu.VMEM((k, LANES), f32),
            pltpu.VMEM((8, cells), f32),
            pltpu.SemaphoreType.DMA((plan.chunks,)),
            pltpu.SemaphoreType.DMA((4,)),
        ],
    )(pop, lam, scale, means, x)
    prior, counts, sizes, places, parts, xs = map(hold, (prior, counts, sizes, places, parts, xs))
    info, ridges = hold_scalars(info), hold_scalars(ridges)
    ids = hold(lax.all_to_all(send, AXES, 0, 0, tiled=True))
    send, a1, a2, moments = pl.pallas_call(
        bound(moment_kernel, plan, "moment"),
        name="moment",
        compiler_params=params,
        out_shape=(
            kept((plan.devices * 3 * plan.part, LANES)),
            kept((k, cells), bf16),
            kept((k, cells), bf16),
            kept(((plan.groups + 1) * plan.depth, LANES)),
        ),
        in_specs=[SMEM] * 2 + [VMEM] * 6,
        out_specs=(VMEM,) * 4,
        scratch_shapes=[
            pltpu.VMEM((k, cells), f32),
            pltpu.VMEM((4, k, LANES), f32),
            pltpu.VMEM((plan.gap_rows, plan.pairs, LANES), f32),
        ],
    )(info, ridges, ids, prior, counts, sizes, places, parts)
    a1, a2, moments = map(hold, (a1, a2, moments))
    rows = send.shape[0]
    got = lax.all_to_all(send.reshape(rows, 1, LANES), AXES, 0, 0, tiled=True)
    got = hold(got.reshape(rows, LANES))
    marks = plan.fixed_marks + plan.reach * (4 if plan.lone else 2)
    mine, theirs = pl.pallas_call(
        bound(reduce_kernel, plan, "reduce"),
        name="reduce",
        compiler_params=params,
        out_shape=(kept((4, plan.pairs, LANES)), kept((3 * plan.part, LANES))),
        in_specs=[SMEM] + [VMEM] * 2,
        out_specs=(VMEM,) * 2,
        scratch_shapes=[pltpu.VMEM((marks, plan.devices, LANES), f32)],
    )(info, got, ids)
    mine = hold(mine)
    swap = [(i, i + 1 - 2 * (i % 2)) for i in range(plan.devices)]
    theirs = hold(lax.ppermute(theirs, AXES, swap))
    corrected, centroids = pl.pallas_call(
        bound(correct_kernel, plan, "correct"),
        name="correct",
        compiler_params=params,
        out_shape=(
            jax.ShapeDtypeStruct(x.shape, f32),
            jax.ShapeDtypeStruct((k // plan.rows, plan.dims), f32),
        ),
        in_specs=[SMEM] * 2 + [VMEM] * 7,
        out_specs=(WHERE, WHERE),
        scratch_shapes=[
            pltpu.VMEM((2, (plan.groups + 1) * plan.depth, LANES), bf16),
            pltpu.VMEM((plan.pairs, LANES), f32),
            pltpu.VMEM((k, LANES), f32),
            pltpu.VMEM((plan.dims, cells), f32),
            pltpu.VMEM((k // plan.rows, plan.dims), f32),
            pltpu.SemaphoreType.DMA((plan.chunks,)),
            pltpu.SemaphoreType.DMA,
        ],
    )(info, ridges, mine, theirs, a1, a2, moments, places, xs)
    return corrected, centroids


def solution(mesh):
    return jax.shard_map(
        body,
        mesh=mesh,
        in_specs=(P(None, AXES), P(), P(), P(), P()),
        out_specs=(P(None, AXES), P("cells", None)),
        check_vma=False,
    )
```

```python
import jax
import jax.numpy as jnp
from jax import lax
from jax.experimental import pallas as pl
from jax.experimental.pallas import tpu as pltpu
from jax.sharding import PartitionSpec as P

f32 = jnp.float32
bf16 = jnp.bfloat16
i32 = jnp.int32
HALF = 64
PIECE = 1024
LANES = 128
TILE = 16
AXES = ("cells", "grp")
BY_CELLS = (((1,), (1,)), ((), ()))
BY_ROWS = (((0,), (0,)), ((), ()))


def iota(shape, axis):
    return lax.broadcasted_iota(i32, shape, axis)


def split(value, parts):
    out = []
    for i in range(parts):
        out.append(value.astype(bf16))
        if i + 1 < parts:
            value = value - out[-1].astype(f32)
    return out


def lane_of(value, lane):
    return jnp.broadcast_to(value[:, lane : lane + 1], value.shape)


def halves(value, lane):
    left = iota(value.shape, 1) < HALF
    return jnp.where(left, lane_of(value, lane), lane_of(value, HALF + lane))


def column(row, first, count):
    shape = (count, row.shape[1])
    pick = iota(shape, 1) == iota(shape, 0) + first
    return jnp.sum(jnp.where(pick, jnp.broadcast_to(row, shape), 0.0), axis=1, keepdims=True)


def pack_pairs(ref):
    pairs = ref.shape[0] // 2
    even = ref[pl.ds(0, pairs, stride=2), :]
    odd = ref[pl.ds(1, pairs, stride=2), :]
    return jnp.where(iota(even.shape, 1) < HALF, even, odd)


def unpack_pairs(ref, tile):
    pairs = tile.shape[0]
    left = iota(tile.shape, 1) < HALF
    turned = pltpu.roll(tile, HALF, 1)
    ref[pl.ds(0, pairs, stride=2), :] = jnp.where(left, tile, turned)
    ref[pl.ds(1, pairs, stride=2), :] = jnp.where(left, turned, tile)
    return ref[...]


def repeat(count, step):
    if count <= 32:
        for i in range(count):
            step(i, 0)
    else:
        lax.fori_loop(0, count, step, 0)


class Plan:
    def __init__(self, x, means, pop):
        self.dims, self.cells = x.shape
        self.clusters = means.shape[0]
        self.batches = pop.shape[0]
        self.rows = lax.axis_size("cells")
        self.cols = lax.axis_size("grp")
        self.devices = self.rows * self.cols
        self.total = self.cells * self.devices
        self.most = 2 * self.total // self.batches
        self.reach = (self.most - 2) // self.cells + 1
        self.lone = self.most >= self.cells
        outside = -(-(self.total - self.cells) // self.most)
        local = min(self.batches, self.batches - outside + 2)
        self.tiles = -(-local // TILE)
        self.local = self.tiles * TILE
        self.group = max(1, LANES // self.clusters)
        self.groups = self.local // self.group
        self.depth = self.group * self.clusters
        self.table = (self.groups + 1) * self.depth
        self.width = -(-(3 * self.clusters + 4) // LANES) * LANES
        self.pairs = self.clusters // 2
        self.part = self.pairs // 2
        self.gap = HALF - (self.dims + 1)
        self.gap_rows = -(-(self.dims + 1) // self.gap)
        self.owned_pairs = self.clusters // self.rows // 2
        self.keep = self.devices * self.pairs * 3 * LANES * 4 <= 1 << 20
        self.fixed_marks = 10
        self.window = min(self.group, 4)
        self.piece = min(self.cells, 512)
        self.pieces = self.cells // self.piece
        self.chunk = min(self.cells, PIECE)
        self.chunks = self.cells // self.chunk

    def at(self, c):
        return slice(c * self.chunk, (c + 1) * self.chunk)


def count_kernel(
    plan, pop_hbm, lam_hbm, scale_hbm, means_hbm, x_hbm, send, prior, counts, sizes, places, parts, xs, info, ridges,
    pop, lam, scale, means, ends, ms, seg, sems, small,
):
    k = plan.clusters
    inputs = [
        pltpu.make_async_copy(source, target, small.at[i])
        for i, (source, target) in enumerate(
            ((pop_hbm, pop), (means_hbm, means), (scale_hbm, scale), (lam_hbm, lam))
        )
    ]
    copies = [
        pltpu.make_async_copy(x_hbm.at[:, plan.at(c)], xs.at[:, plan.at(c)], sems.at[c])
        for c in range(plan.chunks)
    ]
    for copy in inputs + copies:
        copy.start()
    offset = (lax.axis_index("cells") * plan.cols + lax.axis_index("grp")) * plan.cells
    inputs[0].wait()
    running, base, blocks = jnp.int32(0), jnp.int32(0), jnp.int32(0)
    for low in range(0, plan.batches, 8):
        held = [pop[b] for b in range(low, min(low + 8, plan.batches))]
        while len(held) > 1:
            held = [sum(held[i : i + 2]) for i in range(0, len(held), 2)]
        running = running + held[0]
        base = jnp.where(running <= offset, running, base)
        blocks = blocks + (running <= offset).astype(i32)
    first, running = blocks * 8, base
    for j in range(8):
        running = running + pop[jnp.minimum(blocks * 8 + j, plan.batches - 1)]
        base = jnp.where(running <= offset, running, base)
        first = first + (running <= offset).astype(i32)

    end = base + pop[first] - offset
    ends[0] = end
    here = jnp.int32(0)
    for c in range(plan.pieces + 1):
        place_of = min(c * plan.piece, plan.cells - 1)

        def onward(held):
            end = held[1] + pop[first + held[0] + 1]
            ends[held[0] + 1] = end
            return held[0] + 1, end

        here, end = lax.while_loop(lambda held, at=place_of: held[1] <= at, onward, (here, end))
        info[4 + c] = here
    segments = here + 1
    last = first + here
    tiles = lax.div(segments + TILE - 1, TILE)
    info[0], info[1], info[2] = first, last, segments

    lane = iota((1, LANES), 1)
    cell = iota((8, plan.cells), 1)
    half = TILE // 2

    def mark(g, held):
        for j in range(half):
            s = g * half + j
            after = jnp.float32(s + 1) if isinstance(s, int) else (s + 1).astype(f32)
            held = jnp.where(cell >= ends[jnp.minimum(s, here)], after, held)
        return held

    def place(held):
        places[...] = jnp.concatenate([held] * (TILE // 8), axis=0).astype(bf16)

    @pl.when(segments <= half)
    def few():
        place(mark(0, jnp.zeros(cell.shape, f32)))

    @pl.when(segments > half)
    def many():
        seg[...] = mark(0, jnp.zeros(cell.shape, f32))

        def locate(g, carry):
            seg[...] = mark(g, seg[...])
            return carry

        lax.fori_loop(1, lax.div(segments + half - 1, half), locate, 0)
        place(seg[...])

    for copy in inputs[1:]:
        copy.wait()

    def note(g, carry):
        row = jnp.zeros((1, LANES), f32)
        for j in range(TILE):
            b = jnp.minimum(first + g * TILE + j, plan.batches - 1)
            ridges[g * TILE + j] = lam[b]
            row = jnp.where(lane == j, pop[b].astype(f32), row)
        sizes[pl.ds(g, 1), :] = row
        return carry

    lax.fori_loop(1, tiles, note, 0)
    note(0, 0)
    ms[...] = jnp.zeros_like(ms)
    ms[:, 0 : plan.dims] = means[...]
    m = ms[...]
    m1, m2, m3 = [part.astype(f32) for part in split(m, 3)]
    zero = jnp.zeros_like(m)

    def twice(value):
        return value + pltpu.roll(value, HALF, 1)

    weights = jnp.concatenate(
        [
            jnp.concatenate([twice(m1), m1], axis=1),
            jnp.concatenate([twice(m2), zero], axis=1),
            jnp.concatenate([m3, zero], axis=1),
        ],
        axis=0,
    ).astype(bf16)
    lengths = jnp.sum(m * m, axis=1, keepdims=True)
    soft = jnp.ones((k, 1), f32)
    row = iota((k, 1), 0)
    for c in range(k):
        soft = jnp.where(row == c, scale[c], soft)
    inverse = 1.0 / (2.0 * soft)
    low = plan.dims // 8 * 8
    over = plan.dims - low
    shape = (8, plan.chunk)
    tail_row = iota(shape, 0)
    constant = jnp.where(tail_row == over, 1.0, 0.0)
    rest = [jnp.zeros(shape, f32)] * ((HALF - low) // 8 - 1)

    def affinity(c):
        at = plan.at(c)
        if over:
            moved = pltpu.roll(xs[plan.dims - 8 : plan.dims, at], over, 0)
            tail = jnp.where(tail_row < over, moved, constant)
        else:
            tail = constant
        x = jnp.concatenate([xs[0:low, at], tail] + rest, axis=0)
        x1, x2, x3 = split(x, 3)
        parts[0:HALF, at] = x1
        parts[HALF:, at] = x2
        stacked = jnp.concatenate([x1, x2, x3, jnp.zeros_like(x1)], axis=0)
        dots = jnp.dot(weights, stacked, preferred_element_type=f32)
        dots = dots[0:k] + dots[k : 2 * k] + dots[2 * k : 3 * k]
        return (2.0 * dots - lengths) * inverse

    spots = iota((TILE, plan.chunk), 0).astype(f32).astype(bf16)

    def finish(c, scores):
        at = plan.at(c)
        raised = jnp.exp(scores - jnp.max(scores, axis=0, keepdims=True))
        chance = raised / jnp.sum(raised, axis=0, keepdims=True)
        prior[:, at] = chance
        hot = jnp.where(places[:, at] == spots, bf16(1), bf16(0))
        return lax.dot_general(
            jnp.concatenate(split(chance, 3), axis=0), hot, BY_CELLS, preferred_element_type=f32
        )

    found = jnp.zeros((3 * k, TILE), f32)
    scores = following = None
    for c in range(plan.chunks + 1):
        if c < plan.chunks:
            copies[c].wait()
            following = affinity(c)
        if c:
            found = found + finish(c - 1, scores)
        scores = following

    def settle(g, found):
        found = found[0:k] + found[k : 2 * k] + found[2 * k :]
        counts[g] = jnp.concatenate([found, jnp.zeros((k, LANES - TILE), f32)], axis=1)

    settle(0, found)

    def count(g, carry):
        rows = (iota((TILE, plan.cells), 0) + g * TILE).astype(f32).astype(bf16)
        hot = jnp.where(places[...] == rows, bf16(1), bf16(0))
        settle(
            g,
            lax.dot_general(
                jnp.concatenate(split(prior[...], 3), axis=0), hot, BY_CELLS, preferred_element_type=f32
            ),
        )
        return carry

    lax.fori_loop(1, tiles, count, 0)

    every = lax.fori_loop(1, tiles, lambda g, total: total + counts[g], counts[0])
    total = jnp.sum(every, axis=1, keepdims=True)
    end = counts[lax.div(here, TILE)]
    wide = iota((k, LANES), 1)
    last_count = jnp.sum(jnp.where(wide == lax.rem(here, TILE), end, 0.0), axis=1, keepdims=True)
    first_count = jnp.where(segments > 1, counts[0][:, 0:1], 0.0)
    spread = (k, plan.width)
    turn = iota(spread, 1) - iota(spread, 0)
    out = jnp.where(turn == 0, total, 0.0)
    out = jnp.where(turn == k, first_count, out)
    out = jnp.where(turn == 2 * k, last_count, out)
    out = jnp.sum(out, axis=0, keepdims=True)
    lanes = iota((1, plan.width), 1)
    out = jnp.where(lanes == 3 * k, first.astype(f32), out)
    out = jnp.where(lanes == 3 * k + 1, last.astype(f32), out)
    out = jnp.where(lanes == 3 * k + 2, lam[first], out)
    out = jnp.where(lanes == 3 * k + 3, lam[last], out)
    send[...] = jnp.broadcast_to(out, send.shape)


def masked(plan, a1, a2, places, base, at, order):
    base = jnp.full((TILE, plan.piece), base.astype(f32)).astype(bf16)
    relative = jnp.concatenate([places[:, at] - base] * (plan.clusters // TILE), axis=0)
    inside = [relative == bf16(j) for j in range(plan.window)]
    parts = [
        jnp.concatenate([jnp.where(here, a[:, at], bf16(0)) for here in inside], axis=0) for a in (a1, a2)
    ]
    return jnp.concatenate([parts[i] for i in order], axis=0)


def extra_windows(plan, info):
    return [lax.div(info[5 + c] - info[4 + c], plan.window) for c in range(plan.pieces)]


def other_windows(plan, info, more, step):
    for c in range(plan.pieces):

        def again(w, carry, c=c):
            step(c, info[4 + c] + w * plan.window)
            return carry

        lax.fori_loop(1, more[c] + 1, again, 0)


def moment_kernel(
    plan, info, ridges, got, prior, counts, sizes, places, parts, send, a1, a2, moments, wide, sums, turned
):
    k = plan.clusters
    first, last, segments = info[0], info[1], info[2]
    groups = lax.div(segments + plan.group - 1, plan.group)
    tiles = lax.div(segments + TILE - 1, TILE)

    table = got[...]
    total = column(jnp.sum(table, axis=0, keepdims=True), 0, k)
    heads, tails = table[:, 3 * k : 3 * k + 1], table[:, 3 * k + 1 : 3 * k + 2]

    def complete(batch):
        batch = batch.astype(f32)
        of_heads = jnp.sum(jnp.where(heads == batch, table, 0.0), axis=0, keepdims=True)
        of_tails = jnp.sum(jnp.where(tails == batch, table, 0.0), axis=0, keepdims=True)
        return column(of_heads, k, k) + column(of_tails, 2 * k, k)

    first_count, last_count = complete(first), complete(last)
    share = total / f32(plan.total)
    lane = iota((k, LANES), 1)

    def factors(g):
        held = counts[g]
        held = jnp.where(lane + g * TILE == 0, first_count, held)
        held = jnp.where(lane + g * TILE == segments - 1, last_count, held)
        ratio = (sizes[pl.ds(g, 1), :] * share + 1.0) / (held + 1.0)
        ratio = jnp.where(lane < TILE, ratio * ratio, 0.0)
        w1, w2, w3 = [part.astype(f32) for part in split(ratio, 3)]
        row = w1 + pltpu.roll(w2, TILE, 1) + pltpu.roll(w3, 2 * TILE, 1)
        return row.astype(bf16)[:, 0 : 4 * TILE]

    def factor_of(weights, g, at):
        shape = (TILE, at.stop - at.start)
        rows = (iota(shape, 0) + g * TILE).astype(f32).astype(bf16)
        hot = jnp.where(places[:, at] == rows, bf16(1), bf16(0))
        hot = jnp.concatenate([hot, hot, hot, jnp.zeros_like(hot)], axis=0)
        return jnp.dot(weights, hot, preferred_element_type=f32)

    weights = factors(0)
    size = plan.window * k

    def settle(at, factor):
        raised = prior[:, at] * factor
        a1[:, at], a2[:, at] = split(raised / jnp.sum(raised, axis=0, keepdims=True), 2)

    def collect(c, base):
        at = slice(c * plan.piece, (c + 1) * plan.piece)
        both = lax.dot_general(
            masked(plan, a1, a2, places, base, at, (0, 1)), parts[:, at], BY_CELLS, preferred_element_type=f32
        )
        to = pl.ds(pl.multiple_of(base * k, k), size)
        moments[to, :] = moments[to, :] + (both[0:size] + both[size:])

    more = extra_windows(plan, info)

    @pl.when(tiles == 1)
    def straight():
        spare = (TILE + plan.window) * k
        moments[0:spare, :] = jnp.zeros((spare, LANES), f32)
        for c in range(plan.chunks):
            settle(plan.at(c), factor_of(weights, 0, plan.at(c)))
        for c in range(plan.pieces):
            collect(c, info[4 + c])

    @pl.when(tiles > 1)
    def general():
        def clear(g, carry):
            moments[pl.ds(pl.multiple_of(g * plan.depth, plan.depth), plan.depth), :] = jnp.zeros(
                (plan.depth, LANES), f32
            )
            return carry

        lax.fori_loop(0, groups + 1, clear, 0)
        wide[...] = jnp.zeros_like(wide)

        def add(g, carry):
            weights = factors(g)
            for c in range(plan.chunks):
                wide[:, plan.at(c)] += factor_of(weights, g, plan.at(c))
            return carry

        lax.fori_loop(0, tiles, add, 0)
        for c in range(plan.chunks):
            settle(plan.at(c), wide[:, plan.at(c)])
        for c in range(plan.pieces):
            collect(c, info[4 + c])

    @pl.when(sum(more) > 0)
    def others():
        other_windows(plan, info, more, collect)

    sums[...] = jnp.zeros_like(sums)

    def gather(g, carry):
        to = pl.ds(pl.multiple_of(g * plan.depth, plan.depth), plan.depth)
        both = moments[to, :]
        both = both + pltpu.roll(both, HALF, 1)
        moments[to, :] = both
        mass = lane_of(both, plan.dims)
        inner, head, tail, every = sums[0], sums[1], sums[2], sums[3]
        for j in range(plan.group):
            s = g * plan.group + j
            at = slice(j * k, (j + 1) * k)
            ridge = ridges[s]
            part = both[at]
            every = every + part
            shrunk = part * (ridge / (mass[at] + ridge))
            inner = inner + jnp.where((s > 0) & (s < segments - 1), shrunk, 0.0)
            head = head + jnp.where((s == 0) & (segments > 1), part, 0.0)
            tail = tail + jnp.where(s == segments - 1, part, 0.0)
        sums[0], sums[1], sums[2], sums[3] = inner, head, tail, every
        return carry

    lax.fori_loop(0, groups, gather, 0)
    inner, head, tail, every = [pack_pairs(sums.at[i]) for i in range(4)]
    lanes = lax.rem(iota(inner.shape, 1), HALF)
    inner = jnp.where(lanes <= plan.dims, inner, 0.0)
    every = jnp.where(lanes <= plan.dims, every, 0.0)
    for j in range(plan.gap_rows):
        moved = pltpu.roll(every, (plan.dims + 1 - plan.gap * j) % LANES, 1)
        turned[j] = jnp.where(lanes > plan.dims, moved, 0.0)
    row = iota((plan.part, LANES), 0)

    def put(c, carry):
        gaps = jnp.zeros((plan.part, LANES), f32)
        for q in range(plan.owned_pairs):
            for j in range(plan.gap_rows):
                pair = c * plan.owned_pairs + q
                piece = jnp.broadcast_to(turned[j, pl.ds(pair, 1), :], gaps.shape)
                gaps = gaps + jnp.where(row == q * plan.gap_rows + j, piece, 0.0)
        for q in range(plan.cols):
            p = c * plan.cols + q
            for side in range(2):
                low = side * plan.part

                def write(low=low, p=p):
                    start = p * 3 * plan.part
                    send[pl.ds(start, plan.part), :] = inner[low : low + plan.part] + gaps
                    send[pl.ds(start + plan.part, plan.part), :] = head[low : low + plan.part]
                    send[pl.ds(start + 2 * plan.part, plan.part), :] = tail[low : low + plan.part]

                if isinstance(p, int):
                    if p % 2 == side:
                        write()
                else:
                    pl.when(lax.rem(p, 2) == side)(write)
        return carry

    repeat(plan.rows, put)


def reduce_kernel(plan, info, got, ids, mine, theirs, marks):
    k, part = plan.clusters, plan.part
    shape = (plan.devices, LANES)
    device = iota(shape, 0)

    def of(lane):
        return jnp.broadcast_to(ids[:, lane : lane + 1], shape)

    heads, tails = of(3 * k), of(3 * k + 1)
    me = lax.axis_index("cells") * plan.cols + lax.axis_index("grp")
    other = me + 1 - 2 * lax.rem(me, 2)

    def shifted(value, distance):
        return pltpu.roll(value, distance % plan.devices, 0)

    marks[0], marks[1] = of(3 * k + 2), of(3 * k + 3)
    own = ids[pl.ds(me, 1), :]
    pair = ids[pl.ds(other, 1), :]
    for i, (row, lane) in enumerate(((own, 3 * k), (own, 3 * k + 1), (pair, 3 * k), (pair, 3 * k + 1))):
        batch = jnp.broadcast_to(row[:, lane : lane + 1], shape)
        marks[2 + 2 * i] = jnp.where(heads == batch, 1.0, 0.0)
        marks[3 + 2 * i] = jnp.where(tails == batch, 1.0, 0.0)
    links = []

    def link(hop, to_head, from_head, mine, theirs):
        inside = (device + hop >= 0) & (device + hop < plan.devices)
        at = plan.fixed_marks + len(links)
        marks[at] = jnp.where(inside & (shifted(theirs, -hop) == mine), 1.0, 0.0)
        links.append((at, hop, to_head, from_head))

    for hop in range(1, plan.reach + 1):
        link(-hop, True, False, heads, tails)
        link(hop, False, True, tails, heads)
        if plan.lone:
            link(-hop, False, False, tails, tails)
            link(hop, False, False, tails, tails)

    block = (2 * part, LANES)
    top = iota(block, 0) < part

    def mark(i, r):
        return jnp.broadcast_to(marks[i, pl.ds(r, 1), :], block)

    def two(i, r):
        return jnp.where(top, mark(i, r), mark(i + 1, r))

    def ends_of(r):
        return got[pl.ds(r * 3 * part + part, 2 * part), :]

    def turn(value):
        return pltpu.roll(value, part, 0)

    def gather(r, carry):
        inner, shrunk, sums = carry
        ends = ends_of(r)
        whole = halves(ends, plan.dims)
        for at, hop, to_head, from_head in links:
            if isinstance(r, int):
                if not 0 <= r + hop < plan.devices:
                    continue
                there = r + hop
            else:
                there = jnp.clip(r + hop, 0, plan.devices - 1)
            mass = halves(ends_of(there), plan.dims)
            if to_head != from_head:
                mass = turn(mass)
            whole = whole + jnp.where(top == to_head, mark(at, r) * mass, 0.0)
        ridge = two(0, r)
        shrunk = shrunk + ends * (ridge / (whole + ridge))
        inner = inner + got[pl.ds(r * 3 * part, part), :]
        sums = tuple(total + ends * two(2 + 2 * i, r) for i, total in enumerate(sums))
        return inner, shrunk, sums

    zero = jnp.zeros(block, f32)
    state = (zero[0:part], zero, (zero,) * 4)
    if plan.devices <= 32:
        for r in range(plan.devices):
            state = gather(r, state)
    else:
        state = lax.fori_loop(0, plan.devices, gather, state)
    inner, shrunk, sums = state

    def fold(value):
        return (value + turn(value))[0:part]

    right = inner + fold(shrunk)
    intercept = right / (1.0 + halves(right, plan.dims))
    mine[0] = jnp.concatenate([intercept, intercept], axis=0)
    theirs[0:part] = intercept
    for i in range(2):
        value = sums[i] + turn(sums[i])
        mine[1 + i] = value
        theirs[(1 + i) * part : (2 + i) * part] = fold(sums[2 + i])
    mine[3] = jnp.concatenate([inner, inner], axis=0)


def correct_kernel(
    plan, info, ridges, mine, theirs, a1, a2, moments, places, xs, out_hbm, centroids_hbm,
    slopes, rows, spread, out, centroids, sems, done,
):
    k, part = plan.clusters, plan.part
    first, last, segments = info[0], info[1], info[2]
    groups = lax.div(segments + plan.group - 1, plan.group)
    me = lax.axis_index("cells") * plan.cols + lax.axis_index("grp")
    odd = jnp.full((plan.pairs, LANES), lax.rem(me, 2)) == 1
    low = iota((plan.pairs, LANES), 0) < part

    def both(i):
        piece = theirs[i * part : (i + 1) * part]
        piece = jnp.concatenate([piece, piece], axis=0)
        return unpack_pairs(spread, jnp.where(low != odd, mine[i], piece))

    intercept, first_sum, last_sum = both(0), both(1), both(2)
    def slope(g, carry):
        start = pl.multiple_of(g * plan.depth, plan.depth)
        held = moments[pl.ds(start, plan.depth), :]
        made = []
        for j in range(plan.group):
            s = g * plan.group + j
            part = held[j * k : (j + 1) * k]
            part = jnp.where(s == 0, first_sum, part)
            part = jnp.where(s == segments - 1, last_sum, part)
            mass = lane_of(part, plan.dims)
            ridge = ridges[s]
            made.append((part - mass * intercept) / (mass + ridge))
        for i, piece in enumerate(split(jnp.concatenate(made, axis=0), 2)):
            slopes[i, pl.ds(start, plan.depth), :] = piece
        return carry

    lax.fori_loop(0, groups, slope, 0)
    blank = jnp.zeros((plan.depth, LANES), bf16)
    for i in range(2):
        slopes[i, pl.ds(pl.multiple_of(groups * plan.depth, plan.depth), plan.depth), :] = blank
    size = plan.window * k

    rows[...] = mine[3]
    lanes = lax.rem(iota((1, LANES), 1), HALF)
    for q in range(plan.owned_pairs):
        every = jnp.zeros((1, LANES), f32)
        for j in range(plan.gap_rows):
            at = q * plan.gap_rows + j
            piece = jnp.where(lanes > plan.dims, rows[at : at + 1], 0.0)
            moved = pltpu.roll(piece, (plan.gap * j - plan.dims - 1) % LANES, 1)
            inside = (lanes >= plan.gap * j) & (lanes < plan.gap * (j + 1))
            every = every + jnp.where(inside, moved, 0.0)
        every = every / (1.0 + halves(every, plan.dims))
        centroids[2 * q : 2 * q + 1] = every[:, 0 : plan.dims]
        centroids[2 * q + 1 : 2 * q + 2] = pltpu.roll(every, HALF, 1)[:, 0 : plan.dims]
    last_copy = pltpu.make_async_copy(centroids, centroids_hbm, done)
    last_copy.start()
    copies = []
    for c in range(plan.pieces):
        at = slice(c * plan.piece, (c + 1) * plan.piece)
        copies.append(pltpu.make_async_copy(out.at[:, at], out_hbm.at[:, at], sems.at[c]))

    def moved(c, base):
        at = slice(c * plan.piece, (c + 1) * plan.piece)
        rows_of = pl.ds(pl.multiple_of(base * k, k), size)
        large, fine = slopes[0, rows_of, 0:HALF], slopes[1, rows_of, 0:HALF]
        return lax.dot_general(
            jnp.concatenate([large, fine, large], axis=0),
            masked(plan, a1, a2, places, base, at, (0, 0, 1)),
            BY_ROWS,
            preferred_element_type=f32,
        )[0 : plan.dims]

    more = extra_windows(plan, info)

    @pl.when(sum(more) == 0)
    def straight():
        for c in range(plan.pieces):
            at = slice(c * plan.piece, (c + 1) * plan.piece)
            out[:, at] = xs[:, at] - moved(c, info[4 + c])
            copies[c].start()

    @pl.when(sum(more) > 0)
    def general():
        for c in range(plan.pieces):
            at = slice(c * plan.piece, (c + 1) * plan.piece)
            out[:, at] = xs[:, at] - moved(c, info[4 + c])

        def step(c, base):
            at = slice(c * plan.piece, (c + 1) * plan.piece)
            out[:, at] = out[:, at] - moved(c, base)

        other_windows(plan, info, more, step)
        for copy in copies:
            copy.start()

    for copy in copies:
        copy.wait()
    last_copy.wait()


VMEM = pl.BlockSpec(memory_space=pltpu.VMEM)
SMEM = pl.BlockSpec(memory_space=pltpu.SMEM)
WHERE = pl.BlockSpec(memory_space=pltpu.HBM)


def hold_scalars(value):
    return pltpu.with_memory_space_constraint(value, pltpu.SMEM)


def bound(kernel, plan, name):
    def run(*refs):
        kernel(plan, *refs)

    run.__name__ = name
    return run


def body(x, means, scale, lam, pop):
    plan = Plan(x, means, pop)
    k, cells = plan.clusters, plan.cells
    params = pltpu.CompilerParams(vmem_limit_bytes=(16 << 20) if plan.keep else None)

    def kept(shape, kind=f32):
        return pltpu.VMEM(shape, kind) if plan.keep else jax.ShapeDtypeStruct(shape, kind)

    def hold(value):
        return pltpu.with_memory_space_constraint(value, pltpu.VMEM) if plan.keep else value

    send, prior, counts, sizes, places, parts, xs, info, ridges = pl.pallas_call(
        bound(count_kernel, plan, "count"),
        name="count",
        out_shape=(
            kept((plan.devices, plan.width)),
            kept((k, cells)),
            kept((plan.tiles, k, LANES)),
            kept((plan.tiles, LANES)),
            kept((TILE, cells), bf16),
            kept((2 * HALF, cells), bf16),
            kept((plan.dims, cells)),
            pltpu.SMEM((5 + plan.pieces,), i32),
            pltpu.SMEM((plan.local,), f32),
        ),
        in_specs=[WHERE] * 5,
        out_specs=(VMEM,) * 7 + (SMEM,) * 2,
        scratch_shapes=[
            pltpu.SMEM(pop.shape, i32),
            pltpu.SMEM(lam.shape, f32),
            pltpu.SMEM(scale.shape, f32),
            pltpu.VMEM(means.shape, f32),
            pltpu.SMEM((plan.batches,), i32),
            pltpu.VMEM((k, LANES), f32),
            pltpu.VMEM((8, cells), f32),
            pltpu.SemaphoreType.DMA((plan.chunks,)),
            pltpu.SemaphoreType.DMA((4,)),
        ],
    )(pop, lam, scale, means, x)
    prior, counts, sizes, places, parts, xs = map(hold, (prior, counts, sizes, places, parts, xs))
    info, ridges = hold_scalars(info), hold_scalars(ridges)
    ids = hold(lax.all_to_all(send, AXES, 0, 0, tiled=True))
    send, a1, a2, moments = pl.pallas_call(
        bound(moment_kernel, plan, "moment"),
        name="moment",
        compiler_params=params,
        out_shape=(
            kept((plan.devices * 3 * plan.part, LANES)),
            kept((k, cells), bf16),
            kept((k, cells), bf16),
            kept((plan.table, LANES)),
        ),
        in_specs=[SMEM] * 2 + [VMEM] * 6,
        out_specs=(VMEM,) * 4,
        scratch_shapes=[
            pltpu.VMEM((k, cells), f32),
            pltpu.VMEM((4, k, LANES), f32),
            pltpu.VMEM((plan.gap_rows, plan.pairs, LANES), f32),
        ],
    )(info, ridges, ids, prior, counts, sizes, places, parts)
    a1, a2, moments = map(hold, (a1, a2, moments))
    rows = send.shape[0]
    got = lax.all_to_all(send.reshape(rows, 1, LANES), AXES, 0, 0, tiled=True)
    got = hold(got.reshape(rows, LANES))
    marks = plan.fixed_marks + plan.reach * (4 if plan.lone else 2)
    mine, theirs = pl.pallas_call(
        bound(reduce_kernel, plan, "reduce"),
        name="reduce",
        compiler_params=params,
        out_shape=(kept((4, plan.pairs, LANES)), kept((3 * plan.part, LANES))),
        in_specs=[SMEM] + [VMEM] * 2,
        out_specs=(VMEM,) * 2,
        scratch_shapes=[pltpu.VMEM((marks, plan.devices, LANES), f32)],
    )(info, got, ids)
    mine = hold(mine)
    swap = [(i, i + 1 - 2 * (i % 2)) for i in range(plan.devices)]
    theirs = hold(lax.ppermute(theirs, AXES, swap))
    corrected, centroids = pl.pallas_call(
        bound(correct_kernel, plan, "correct"),
        name="correct",
        compiler_params=params,
        out_shape=(
            jax.ShapeDtypeStruct(x.shape, f32),
            jax.ShapeDtypeStruct((k // plan.rows, plan.dims), f32),
        ),
        in_specs=[SMEM] * 2 + [VMEM] * 7,
        out_specs=(WHERE, WHERE),
        scratch_shapes=[
            pltpu.VMEM((2, plan.table, LANES), bf16),
            pltpu.VMEM((plan.pairs, LANES), f32),
            pltpu.VMEM((k, LANES), f32),
            pltpu.VMEM((plan.dims, cells), f32),
            pltpu.VMEM((k // plan.rows, plan.dims), f32),
            pltpu.SemaphoreType.DMA((plan.pieces,)),
            pltpu.SemaphoreType.DMA,
        ],
    )(info, ridges, mine, theirs, a1, a2, moments, places, xs)
    return corrected, centroids


def solution(mesh):
    return jax.shard_map(
        body,
        mesh=mesh,
        in_specs=(P(None, AXES), P(), P(), P(), P()),
        out_specs=(P(None, AXES), P("cells", None)),
        check_vma=False,
    )
```

```python
import jax
import jax.numpy as jnp
from jax import lax
from jax.experimental import pallas as pl
from jax.experimental.pallas import tpu as pltpu
from jax.sharding import PartitionSpec as P

f32 = jnp.float32
bf16 = jnp.bfloat16
i32 = jnp.int32
HALF = 64
PIECE = 4096
LANES = 128
TILE = 16
AXES = ("cells", "grp")
BY_CELLS = (((1,), (1,)), ((), ()))
BY_ROWS = (((0,), (0,)), ((), ()))


def iota(shape, axis):
    return lax.broadcasted_iota(i32, shape, axis)


def split(value, parts):
    out = []
    for i in range(parts):
        out.append(value.astype(bf16))
        if i + 1 < parts:
            value = value - out[-1].astype(f32)
    return out


def lane_of(value, lane):
    return jnp.broadcast_to(value[:, lane : lane + 1], value.shape)


def halves(value, lane):
    left = iota(value.shape, 1) < HALF
    return jnp.where(left, lane_of(value, lane), lane_of(value, HALF + lane))


def column(row, first, count):
    shape = (count, row.shape[1])
    pick = iota(shape, 1) == iota(shape, 0) + first
    return jnp.sum(jnp.where(pick, jnp.broadcast_to(row, shape), 0.0), axis=1, keepdims=True)


def pack_pairs(ref):
    pairs = ref.shape[0] // 2
    even = ref[pl.ds(0, pairs, stride=2), :]
    odd = ref[pl.ds(1, pairs, stride=2), :]
    return jnp.where(iota(even.shape, 1) < HALF, even, odd)


def unpack_pairs(ref, tile):
    pairs = tile.shape[0]
    left = iota(tile.shape, 1) < HALF
    turned = pltpu.roll(tile, HALF, 1)
    ref[pl.ds(0, pairs, stride=2), :] = jnp.where(left, tile, turned)
    ref[pl.ds(1, pairs, stride=2), :] = jnp.where(left, turned, tile)
    return ref[...]


def repeat(count, step):
    if count <= 32:
        for i in range(count):
            step(i, 0)
    else:
        lax.fori_loop(0, count, step, 0)


class Plan:
    def __init__(self, x, means, pop):
        self.dims, self.cells = x.shape
        self.clusters = means.shape[0]
        self.batches = pop.shape[0]
        self.rows = lax.axis_size("cells")
        self.cols = lax.axis_size("grp")
        self.devices = self.rows * self.cols
        self.total = self.cells * self.devices
        self.most = 2 * self.total // self.batches
        self.reach = (self.most - 2) // self.cells + 1
        self.lone = self.most >= self.cells
        outside = -(-(self.total - self.cells) // self.most)
        local = min(self.batches, self.batches - outside + 2)
        self.tiles = -(-local // TILE)
        self.local = self.tiles * TILE
        self.group = max(1, LANES // self.clusters)
        self.groups = self.local // self.group
        self.depth = self.group * self.clusters
        self.table = (self.groups + 1) * self.depth
        self.width = -(-(3 * self.clusters + 4) // LANES) * LANES
        self.pairs = self.clusters // 2
        self.part = self.pairs // 2
        self.gap = HALF - (self.dims + 1)
        self.gap_rows = -(-(self.dims + 1) // self.gap)
        self.owned_pairs = self.clusters // self.rows // 2
        self.keep = self.devices * self.pairs * 3 * LANES * 4 <= 1 << 20
        self.fixed_marks = 10
        self.window = min(self.group, 4)
        self.piece = min(self.cells, 256)
        self.pieces = self.cells // self.piece
        self.sends = min(self.pieces, 4)
        self.chunk = min(self.cells, PIECE)
        self.chunks = self.cells // self.chunk

    def at(self, c):
        return slice(c * self.chunk, (c + 1) * self.chunk)


def count_kernel(
    plan, pop_hbm, lam_hbm, scale_hbm, means_hbm, x_hbm, send, prior, counts, sizes, places, parts, xs, info, ridges,
    pop, lam, scale, means, ends, ms, seg, sems, small,
):
    k = plan.clusters
    inputs = [
        pltpu.make_async_copy(source, target, small.at[i])
        for i, (source, target) in enumerate(
            ((pop_hbm, pop), (means_hbm, means), (scale_hbm, scale), (lam_hbm, lam))
        )
    ]
    copies = [
        pltpu.make_async_copy(x_hbm.at[:, plan.at(c)], xs.at[:, plan.at(c)], sems.at[c])
        for c in range(plan.chunks)
    ]
    for copy in inputs + copies:
        copy.start()
    offset = (lax.axis_index("cells") * plan.cols + lax.axis_index("grp")) * plan.cells
    inputs[0].wait()
    running, base, blocks = jnp.int32(0), jnp.int32(0), jnp.int32(0)
    for low in range(0, plan.batches, 8):
        held = [pop[b] for b in range(low, min(low + 8, plan.batches))]
        while len(held) > 1:
            held = [sum(held[i : i + 2]) for i in range(0, len(held), 2)]
        running = running + held[0]
        base = jnp.where(running <= offset, running, base)
        blocks = blocks + (running <= offset).astype(i32)
    first, running = blocks * 8, base
    for j in range(8):
        running = running + pop[jnp.minimum(blocks * 8 + j, plan.batches - 1)]
        base = jnp.where(running <= offset, running, base)
        first = first + (running <= offset).astype(i32)

    end = base + pop[first] - offset
    ends[0] = end
    here = jnp.int32(0)
    for c in range(plan.pieces + 1):
        place_of = min(c * plan.piece, plan.cells - 1)

        def onward(held):
            end = held[1] + pop[first + held[0] + 1]
            ends[held[0] + 1] = end
            return held[0] + 1, end

        here, end = lax.while_loop(lambda held, at=place_of: held[1] <= at, onward, (here, end))
        info[4 + c] = here
    segments = here + 1
    last = first + here
    tiles = lax.div(segments + TILE - 1, TILE)
    info[0], info[1], info[2] = first, last, segments

    lane = iota((1, LANES), 1)
    cell = iota((8, plan.cells), 1)
    half = TILE // 2

    def mark(g, held):
        for j in range(half):
            s = g * half + j
            after = jnp.float32(s + 1) if isinstance(s, int) else (s + 1).astype(f32)
            held = jnp.where(cell >= ends[jnp.minimum(s, here)], after, held)
        return held

    def place(held):
        places[...] = jnp.concatenate([held] * (TILE // 8), axis=0).astype(bf16)

    @pl.when(segments <= half)
    def few():
        place(mark(0, jnp.zeros(cell.shape, f32)))

    @pl.when(segments > half)
    def many():
        seg[...] = mark(0, jnp.zeros(cell.shape, f32))

        def locate(g, carry):
            seg[...] = mark(g, seg[...])
            return carry

        lax.fori_loop(1, lax.div(segments + half - 1, half), locate, 0)
        place(seg[...])

    for copy in inputs[1:]:
        copy.wait()

    def note(g, carry):
        row = jnp.zeros((1, LANES), f32)
        for j in range(TILE):
            b = jnp.minimum(first + g * TILE + j, plan.batches - 1)
            ridges[g * TILE + j] = lam[b]
            row = jnp.where(lane == j, pop[b].astype(f32), row)
        sizes[pl.ds(g, 1), :] = row
        return carry

    lax.fori_loop(1, tiles, note, 0)
    note(0, 0)
    ms[...] = jnp.zeros_like(ms)
    ms[:, 0 : plan.dims] = means[...]
    m = ms[...]
    m1, m2, m3 = [part.astype(f32) for part in split(m, 3)]
    zero = jnp.zeros_like(m)

    def twice(value):
        return value + pltpu.roll(value, HALF, 1)

    weights = jnp.concatenate(
        [
            jnp.concatenate([twice(m1), m1], axis=1),
            jnp.concatenate([twice(m2), zero], axis=1),
            jnp.concatenate([m3, zero], axis=1),
        ],
        axis=0,
    ).astype(bf16)
    lengths = jnp.sum(m * m, axis=1, keepdims=True)
    soft = jnp.ones((k, 1), f32)
    row = iota((k, 1), 0)
    for c in range(k):
        soft = jnp.where(row == c, scale[c], soft)
    inverse = 1.0 / (2.0 * soft)
    low = plan.dims // 8 * 8
    over = plan.dims - low
    shape = (8, plan.chunk)
    tail_row = iota(shape, 0)
    constant = jnp.where(tail_row == over, 1.0, 0.0)
    rest = [jnp.zeros(shape, f32)] * ((HALF - low) // 8 - 1)

    def affinity(c):
        at = plan.at(c)
        if over:
            moved = pltpu.roll(xs[plan.dims - 8 : plan.dims, at], over, 0)
            tail = jnp.where(tail_row < over, moved, constant)
        else:
            tail = constant
        x = jnp.concatenate([xs[0:low, at], tail] + rest, axis=0)
        x1, x2, x3 = split(x, 3)
        parts[0:HALF, at] = x1
        parts[HALF:, at] = x2
        stacked = jnp.concatenate([x1, x2, x3, jnp.zeros_like(x1)], axis=0)
        dots = jnp.dot(weights, stacked, preferred_element_type=f32)
        dots = dots[0:k] + dots[k : 2 * k] + dots[2 * k : 3 * k]
        return (2.0 * dots - lengths) * inverse

    spots = iota((TILE, plan.chunk), 0).astype(f32).astype(bf16)

    def finish(c, scores):
        at = plan.at(c)
        raised = jnp.exp(scores - jnp.max(scores, axis=0, keepdims=True))
        chance = raised / jnp.sum(raised, axis=0, keepdims=True)
        prior[:, at] = chance
        hot = jnp.where(places[:, at] == spots, bf16(1), bf16(0))
        return lax.dot_general(
            jnp.concatenate(split(chance, 3), axis=0), hot, BY_CELLS, preferred_element_type=f32
        )

    found = jnp.zeros((3 * k, TILE), f32)
    scores = following = None
    for c in range(plan.chunks + 1):
        if c < plan.chunks:
            copies[c].wait()
            following = affinity(c)
        if c:
            found = found + finish(c - 1, scores)
        scores = following

    def settle(g, found):
        found = found[0:k] + found[k : 2 * k] + found[2 * k :]
        counts[g] = jnp.concatenate([found, jnp.zeros((k, LANES - TILE), f32)], axis=1)

    settle(0, found)

    def count(g, carry):
        rows = (iota((TILE, plan.cells), 0) + g * TILE).astype(f32).astype(bf16)
        hot = jnp.where(places[...] == rows, bf16(1), bf16(0))
        settle(
            g,
            lax.dot_general(
                jnp.concatenate(split(prior[...], 3), axis=0), hot, BY_CELLS, preferred_element_type=f32
            ),
        )
        return carry

    lax.fori_loop(1, tiles, count, 0)

    every = lax.fori_loop(1, tiles, lambda g, total: total + counts[g], counts[0])
    total = jnp.sum(every, axis=1, keepdims=True)
    end = counts[lax.div(here, TILE)]
    wide = iota((k, LANES), 1)
    last_count = jnp.sum(jnp.where(wide == lax.rem(here, TILE), end, 0.0), axis=1, keepdims=True)
    first_count = jnp.where(segments > 1, counts[0][:, 0:1], 0.0)
    spread = (k, plan.width)
    turn = iota(spread, 1) - iota(spread, 0)
    out = jnp.where(turn == 0, total, 0.0)
    out = jnp.where(turn == k, first_count, out)
    out = jnp.where(turn == 2 * k, last_count, out)
    out = jnp.sum(out, axis=0, keepdims=True)
    lanes = iota((1, plan.width), 1)
    out = jnp.where(lanes == 3 * k, first.astype(f32), out)
    out = jnp.where(lanes == 3 * k + 1, last.astype(f32), out)
    out = jnp.where(lanes == 3 * k + 2, lam[first], out)
    out = jnp.where(lanes == 3 * k + 3, lam[last], out)
    send[...] = jnp.broadcast_to(out, send.shape)


def masked(plan, a1, a2, places, base, at, order):
    base = jnp.full((TILE, plan.piece), base.astype(f32)).astype(bf16)
    relative = jnp.concatenate([places[:, at] - base] * (plan.clusters // TILE), axis=0)
    inside = [relative == bf16(j) for j in range(plan.window)]
    parts = [
        jnp.concatenate([jnp.where(here, a[:, at], bf16(0)) for here in inside], axis=0) for a in (a1, a2)
    ]
    return jnp.concatenate([parts[i] for i in order], axis=0)


def extra_windows(plan, info):
    return [lax.div(info[5 + c] - info[4 + c], plan.window) for c in range(plan.pieces)]


def other_windows(plan, info, more, step):
    for c in range(plan.pieces):

        def again(w, carry, c=c):
            step(c, info[4 + c] + w * plan.window)
            return carry

        lax.fori_loop(1, more[c] + 1, again, 0)


def moment_kernel(
    plan, info, ridges, got, prior, counts, sizes, places, parts, send, a1, a2, moments, wide, sums, turned
):
    k = plan.clusters
    first, last, segments = info[0], info[1], info[2]
    groups = lax.div(segments + plan.group - 1, plan.group)
    tiles = lax.div(segments + TILE - 1, TILE)

    table = got[...]
    total = column(jnp.sum(table, axis=0, keepdims=True), 0, k)
    heads, tails = table[:, 3 * k : 3 * k + 1], table[:, 3 * k + 1 : 3 * k + 2]

    def complete(batch):
        batch = batch.astype(f32)
        of_heads = jnp.sum(jnp.where(heads == batch, table, 0.0), axis=0, keepdims=True)
        of_tails = jnp.sum(jnp.where(tails == batch, table, 0.0), axis=0, keepdims=True)
        return column(of_heads, k, k) + column(of_tails, 2 * k, k)

    first_count, last_count = complete(first), complete(last)
    share = total / f32(plan.total)
    lane = iota((k, LANES), 1)

    def factors(g):
        held = counts[g]
        held = jnp.where(lane + g * TILE == 0, first_count, held)
        held = jnp.where(lane + g * TILE == segments - 1, last_count, held)
        ratio = (sizes[pl.ds(g, 1), :] * share + 1.0) / (held + 1.0)
        ratio = jnp.where(lane < TILE, ratio * ratio, 0.0)
        w1, w2, w3 = [part.astype(f32) for part in split(ratio, 3)]
        row = w1 + pltpu.roll(w2, TILE, 1) + pltpu.roll(w3, 2 * TILE, 1)
        return row.astype(bf16)[:, 0 : 4 * TILE]

    def factor_of(weights, g, at):
        shape = (TILE, at.stop - at.start)
        rows = (iota(shape, 0) + g * TILE).astype(f32).astype(bf16)
        hot = jnp.where(places[:, at] == rows, bf16(1), bf16(0))
        hot = jnp.concatenate([hot, hot, hot, jnp.zeros_like(hot)], axis=0)
        return jnp.dot(weights, hot, preferred_element_type=f32)

    weights = factors(0)
    size = plan.window * k

    def settle(at, factor):
        raised = prior[:, at] * factor
        a1[:, at], a2[:, at] = split(raised / jnp.sum(raised, axis=0, keepdims=True), 2)

    def collect(c, base):
        at = slice(c * plan.piece, (c + 1) * plan.piece)
        both = lax.dot_general(
            masked(plan, a1, a2, places, base, at, (0, 1)), parts[:, at], BY_CELLS, preferred_element_type=f32
        )
        to = pl.ds(pl.multiple_of(base * k, k), size)
        moments[to, :] = moments[to, :] + (both[0:size] + both[size:])

    more = extra_windows(plan, info)

    @pl.when(tiles == 1)
    def straight():
        spare = (TILE + plan.window) * k
        moments[0:spare, :] = jnp.zeros((spare, LANES), f32)
        for c in range(plan.chunks):
            settle(plan.at(c), factor_of(weights, 0, plan.at(c)))
        for c in range(plan.pieces):
            collect(c, info[4 + c])

    @pl.when(tiles > 1)
    def general():
        def clear(g, carry):
            moments[pl.ds(pl.multiple_of(g * plan.depth, plan.depth), plan.depth), :] = jnp.zeros(
                (plan.depth, LANES), f32
            )
            return carry

        lax.fori_loop(0, groups + 1, clear, 0)
        wide[...] = jnp.zeros_like(wide)

        def add(g, carry):
            weights = factors(g)
            for c in range(plan.chunks):
                wide[:, plan.at(c)] += factor_of(weights, g, plan.at(c))
            return carry

        lax.fori_loop(0, tiles, add, 0)
        for c in range(plan.chunks):
            settle(plan.at(c), wide[:, plan.at(c)])
        for c in range(plan.pieces):
            collect(c, info[4 + c])

    @pl.when(sum(more) > 0)
    def others():
        other_windows(plan, info, more, collect)

    sums[...] = jnp.zeros_like(sums)

    def gather(g, carry):
        to = pl.ds(pl.multiple_of(g * plan.depth, plan.depth), plan.depth)
        both = moments[to, :]
        both = both + pltpu.roll(both, HALF, 1)
        moments[to, :] = both
        mass = lane_of(both, plan.dims)
        inner, head, tail, every = sums[0], sums[1], sums[2], sums[3]
        for j in range(plan.group):
            s = g * plan.group + j
            at = slice(j * k, (j + 1) * k)
            ridge = ridges[s]
            part = both[at]
            every = every + part
            shrunk = part * (ridge / (mass[at] + ridge))
            inner = inner + jnp.where((s > 0) & (s < segments - 1), shrunk, 0.0)
            head = head + jnp.where((s == 0) & (segments > 1), part, 0.0)
            tail = tail + jnp.where(s == segments - 1, part, 0.0)
        sums[0], sums[1], sums[2], sums[3] = inner, head, tail, every
        return carry

    lax.fori_loop(0, groups, gather, 0)
    inner, head, tail, every = [pack_pairs(sums.at[i]) for i in range(4)]
    lanes = lax.rem(iota(inner.shape, 1), HALF)
    inner = jnp.where(lanes <= plan.dims, inner, 0.0)
    every = jnp.where(lanes <= plan.dims, every, 0.0)
    for j in range(plan.gap_rows):
        moved = pltpu.roll(every, (plan.dims + 1 - plan.gap * j) % LANES, 1)
        turned[j] = jnp.where(lanes > plan.dims, moved, 0.0)
    row = iota((plan.part, LANES), 0)

    def put(c, carry):
        gaps = jnp.zeros((plan.part, LANES), f32)
        for q in range(plan.owned_pairs):
            for j in range(plan.gap_rows):
                pair = c * plan.owned_pairs + q
                piece = jnp.broadcast_to(turned[j, pl.ds(pair, 1), :], gaps.shape)
                gaps = gaps + jnp.where(row == q * plan.gap_rows + j, piece, 0.0)
        for q in range(plan.cols):
            p = c * plan.cols + q
            for side in range(2):
                low = side * plan.part

                def write(low=low, p=p):
                    start = p * 3 * plan.part
                    send[pl.ds(start, plan.part), :] = inner[low : low + plan.part] + gaps
                    send[pl.ds(start + plan.part, plan.part), :] = head[low : low + plan.part]
                    send[pl.ds(start + 2 * plan.part, plan.part), :] = tail[low : low + plan.part]

                if isinstance(p, int):
                    if p % 2 == side:
                        write()
                else:
                    pl.when(lax.rem(p, 2) == side)(write)
        return carry

    repeat(plan.rows, put)


def reduce_kernel(plan, info, got, ids, mine, theirs, marks):
    k, part = plan.clusters, plan.part
    shape = (plan.devices, LANES)
    device = iota(shape, 0)

    def of(lane):
        return jnp.broadcast_to(ids[:, lane : lane + 1], shape)

    heads, tails = of(3 * k), of(3 * k + 1)
    me = lax.axis_index("cells") * plan.cols + lax.axis_index("grp")
    other = me + 1 - 2 * lax.rem(me, 2)

    def shifted(value, distance):
        return pltpu.roll(value, distance % plan.devices, 0)

    marks[0], marks[1] = of(3 * k + 2), of(3 * k + 3)
    own = ids[pl.ds(me, 1), :]
    pair = ids[pl.ds(other, 1), :]
    for i, (row, lane) in enumerate(((own, 3 * k), (own, 3 * k + 1), (pair, 3 * k), (pair, 3 * k + 1))):
        batch = jnp.broadcast_to(row[:, lane : lane + 1], shape)
        marks[2 + 2 * i] = jnp.where(heads == batch, 1.0, 0.0)
        marks[3 + 2 * i] = jnp.where(tails == batch, 1.0, 0.0)
    links = []

    def link(hop, to_head, from_head, mine, theirs):
        inside = (device + hop >= 0) & (device + hop < plan.devices)
        at = plan.fixed_marks + len(links)
        marks[at] = jnp.where(inside & (shifted(theirs, -hop) == mine), 1.0, 0.0)
        links.append((at, hop, to_head, from_head))

    for hop in range(1, plan.reach + 1):
        link(-hop, True, False, heads, tails)
        link(hop, False, True, tails, heads)
        if plan.lone:
            link(-hop, False, False, tails, tails)
            link(hop, False, False, tails, tails)

    block = (2 * part, LANES)
    top = iota(block, 0) < part

    def mark(i, r):
        return jnp.broadcast_to(marks[i, pl.ds(r, 1), :], block)

    def two(i, r):
        return jnp.where(top, mark(i, r), mark(i + 1, r))

    def ends_of(r):
        return got[pl.ds(r * 3 * part + part, 2 * part), :]

    def turn(value):
        return pltpu.roll(value, part, 0)

    def gather(r, carry):
        inner, shrunk, sums = carry
        ends = ends_of(r)
        whole = halves(ends, plan.dims)
        for at, hop, to_head, from_head in links:
            if isinstance(r, int):
                if not 0 <= r + hop < plan.devices:
                    continue
                there = r + hop
            else:
                there = jnp.clip(r + hop, 0, plan.devices - 1)
            mass = halves(ends_of(there), plan.dims)
            if to_head != from_head:
                mass = turn(mass)
            whole = whole + jnp.where(top == to_head, mark(at, r) * mass, 0.0)
        ridge = two(0, r)
        shrunk = shrunk + ends * (ridge / (whole + ridge))
        inner = inner + got[pl.ds(r * 3 * part, part), :]
        sums = tuple(total + ends * two(2 + 2 * i, r) for i, total in enumerate(sums))
        return inner, shrunk, sums

    zero = jnp.zeros(block, f32)
    state = (zero[0:part], zero, (zero,) * 4)
    if plan.devices <= 32:
        for r in range(plan.devices):
            state = gather(r, state)
    else:
        state = lax.fori_loop(0, plan.devices, gather, state)
    inner, shrunk, sums = state

    def fold(value):
        return (value + turn(value))[0:part]

    right = inner + fold(shrunk)
    intercept = right / (1.0 + halves(right, plan.dims))
    mine[0] = jnp.concatenate([intercept, intercept], axis=0)
    theirs[0:part] = intercept
    for i in range(2):
        value = sums[i] + turn(sums[i])
        mine[1 + i] = value
        theirs[(1 + i) * part : (2 + i) * part] = fold(sums[2 + i])
    mine[3] = jnp.concatenate([inner, inner], axis=0)


def correct_kernel(
    plan, info, ridges, mine, theirs, a1, a2, moments, places, xs, out_hbm, centroids_hbm,
    slopes, rows, spread, out, centroids, sems, done,
):
    k, part = plan.clusters, plan.part
    first, last, segments = info[0], info[1], info[2]
    groups = lax.div(segments + plan.group - 1, plan.group)
    me = lax.axis_index("cells") * plan.cols + lax.axis_index("grp")
    odd = jnp.full((plan.pairs, LANES), lax.rem(me, 2)) == 1
    low = iota((plan.pairs, LANES), 0) < part

    def both(i):
        piece = theirs[i * part : (i + 1) * part]
        piece = jnp.concatenate([piece, piece], axis=0)
        return unpack_pairs(spread, jnp.where(low != odd, mine[i], piece))

    intercept, first_sum, last_sum = both(0), both(1), both(2)
    def slope(g, carry):
        start = pl.multiple_of(g * plan.depth, plan.depth)
        held = moments[pl.ds(start, plan.depth), :]
        made = []
        for j in range(plan.group):
            s = g * plan.group + j
            part = held[j * k : (j + 1) * k]
            part = jnp.where(s == 0, first_sum, part)
            part = jnp.where(s == segments - 1, last_sum, part)
            mass = lane_of(part, plan.dims)
            ridge = ridges[s]
            made.append((part - mass * intercept) / (mass + ridge))
        for i, piece in enumerate(split(jnp.concatenate(made, axis=0), 2)):
            slopes[i, pl.ds(start, plan.depth), :] = piece
        return carry

    lax.fori_loop(0, groups, slope, 0)
    blank = jnp.zeros((plan.depth, LANES), bf16)
    for i in range(2):
        slopes[i, pl.ds(pl.multiple_of(groups * plan.depth, plan.depth), plan.depth), :] = blank
    size = plan.window * k

    rows[...] = mine[3]
    lanes = lax.rem(iota((1, LANES), 1), HALF)
    for q in range(plan.owned_pairs):
        every = jnp.zeros((1, LANES), f32)
        for j in range(plan.gap_rows):
            at = q * plan.gap_rows + j
            piece = jnp.where(lanes > plan.dims, rows[at : at + 1], 0.0)
            moved = pltpu.roll(piece, (plan.gap * j - plan.dims - 1) % LANES, 1)
            inside = (lanes >= plan.gap * j) & (lanes < plan.gap * (j + 1))
            every = every + jnp.where(inside, moved, 0.0)
        every = every / (1.0 + halves(every, plan.dims))
        centroids[2 * q : 2 * q + 1] = every[:, 0 : plan.dims]
        centroids[2 * q + 1 : 2 * q + 2] = pltpu.roll(every, HALF, 1)[:, 0 : plan.dims]
    last_copy = pltpu.make_async_copy(centroids, centroids_hbm, done)
    last_copy.start()
    copies = []
    span = plan.cells // plan.sends
    for c in range(plan.sends):
        at = slice(c * span, (c + 1) * span)
        copies.append(pltpu.make_async_copy(out.at[:, at], out_hbm.at[:, at], sems.at[c]))

    def moved(c, base):
        at = slice(c * plan.piece, (c + 1) * plan.piece)
        rows_of = pl.ds(pl.multiple_of(base * k, k), size)
        large, fine = slopes[0, rows_of, 0:HALF], slopes[1, rows_of, 0:HALF]
        return lax.dot_general(
            jnp.concatenate([large, fine, large], axis=0),
            masked(plan, a1, a2, places, base, at, (0, 0, 1)),
            BY_ROWS,
            preferred_element_type=f32,
        )[0 : plan.dims]

    more = extra_windows(plan, info)

    @pl.when(sum(more) == 0)
    def straight():
        for c in range(plan.pieces):
            at = slice(c * plan.piece, (c + 1) * plan.piece)
            out[:, at] = xs[:, at] - moved(c, info[4 + c])
            if (c + 1) * plan.sends % plan.pieces == 0:
                copies[(c + 1) * plan.sends // plan.pieces - 1].start()

    @pl.when(sum(more) > 0)
    def general():
        for c in range(plan.pieces):
            at = slice(c * plan.piece, (c + 1) * plan.piece)
            out[:, at] = xs[:, at] - moved(c, info[4 + c])

        def step(c, base):
            at = slice(c * plan.piece, (c + 1) * plan.piece)
            out[:, at] = out[:, at] - moved(c, base)

        other_windows(plan, info, more, step)
        for copy in copies:
            copy.start()

    for copy in copies:
        copy.wait()
    last_copy.wait()


VMEM = pl.BlockSpec(memory_space=pltpu.VMEM)
SMEM = pl.BlockSpec(memory_space=pltpu.SMEM)
WHERE = pl.BlockSpec(memory_space=pltpu.HBM)


def hold_scalars(value):
    return pltpu.with_memory_space_constraint(value, pltpu.SMEM)


def bound(kernel, plan, name):
    def run(*refs):
        kernel(plan, *refs)

    run.__name__ = name
    return run


def body(x, means, scale, lam, pop):
    plan = Plan(x, means, pop)
    k, cells = plan.clusters, plan.cells
    params = pltpu.CompilerParams(vmem_limit_bytes=(16 << 20) if plan.keep else None)

    def kept(shape, kind=f32):
        return pltpu.VMEM(shape, kind) if plan.keep else jax.ShapeDtypeStruct(shape, kind)

    def hold(value):
        return pltpu.with_memory_space_constraint(value, pltpu.VMEM) if plan.keep else value

    send, prior, counts, sizes, places, parts, xs, info, ridges = pl.pallas_call(
        bound(count_kernel, plan, "count"),
        name="count",
        out_shape=(
            kept((plan.devices, plan.width)),
            kept((k, cells)),
            kept((plan.tiles, k, LANES)),
            kept((plan.tiles, LANES)),
            kept((TILE, cells), bf16),
            kept((2 * HALF, cells), bf16),
            kept((plan.dims, cells)),
            pltpu.SMEM((5 + plan.pieces,), i32),
            pltpu.SMEM((plan.local,), f32),
        ),
        in_specs=[WHERE] * 5,
        out_specs=(VMEM,) * 7 + (SMEM,) * 2,
        scratch_shapes=[
            pltpu.SMEM(pop.shape, i32),
            pltpu.SMEM(lam.shape, f32),
            pltpu.SMEM(scale.shape, f32),
            pltpu.VMEM(means.shape, f32),
            pltpu.SMEM((plan.batches,), i32),
            pltpu.VMEM((k, LANES), f32),
            pltpu.VMEM((8, cells), f32),
            pltpu.SemaphoreType.DMA((plan.chunks,)),
            pltpu.SemaphoreType.DMA((4,)),
        ],
    )(pop, lam, scale, means, x)
    prior, counts, sizes, places, parts, xs = map(hold, (prior, counts, sizes, places, parts, xs))
    info, ridges = hold_scalars(info), hold_scalars(ridges)
    ids = hold(lax.all_to_all(send, AXES, 0, 0, tiled=True))
    send, a1, a2, moments = pl.pallas_call(
        bound(moment_kernel, plan, "moment"),
        name="moment",
        compiler_params=params,
        out_shape=(
            kept((plan.devices * 3 * plan.part, LANES)),
            kept((k, cells), bf16),
            kept((k, cells), bf16),
            kept((plan.table, LANES)),
        ),
        in_specs=[SMEM] * 2 + [VMEM] * 6,
        out_specs=(VMEM,) * 4,
        scratch_shapes=[
            pltpu.VMEM((k, cells), f32),
            pltpu.VMEM((4, k, LANES), f32),
            pltpu.VMEM((plan.gap_rows, plan.pairs, LANES), f32),
        ],
    )(info, ridges, ids, prior, counts, sizes, places, parts)
    a1, a2, moments = map(hold, (a1, a2, moments))
    rows = send.shape[0]
    got = lax.all_to_all(send.reshape(rows, 1, LANES), AXES, 0, 0, tiled=True)
    got = hold(got.reshape(rows, LANES))
    marks = plan.fixed_marks + plan.reach * (4 if plan.lone else 2)
    mine, theirs = pl.pallas_call(
        bound(reduce_kernel, plan, "reduce"),
        name="reduce",
        compiler_params=params,
        out_shape=(kept((4, plan.pairs, LANES)), kept((3 * plan.part, LANES))),
        in_specs=[SMEM] + [VMEM] * 2,
        out_specs=(VMEM,) * 2,
        scratch_shapes=[pltpu.VMEM((marks, plan.devices, LANES), f32)],
    )(info, got, ids)
    mine = hold(mine)
    swap = [(i, i + 1 - 2 * (i % 2)) for i in range(plan.devices)]
    theirs = hold(lax.ppermute(theirs, AXES, swap))
    corrected, centroids = pl.pallas_call(
        bound(correct_kernel, plan, "correct"),
        name="correct",
        compiler_params=params,
        out_shape=(
            jax.ShapeDtypeStruct(x.shape, f32),
            jax.ShapeDtypeStruct((k // plan.rows, plan.dims), f32),
        ),
        in_specs=[SMEM] * 2 + [VMEM] * 7,
        out_specs=(WHERE, WHERE),
        scratch_shapes=[
            pltpu.VMEM((2, plan.table, LANES), bf16),
            pltpu.VMEM((plan.pairs, LANES), f32),
            pltpu.VMEM((k, LANES), f32),
            pltpu.VMEM((plan.dims, cells), f32),
            pltpu.VMEM((k // plan.rows, plan.dims), f32),
            pltpu.SemaphoreType.DMA((plan.sends,)),
            pltpu.SemaphoreType.DMA,
        ],
    )(info, ridges, mine, theirs, a1, a2, moments, places, xs)
    return corrected, centroids


def solution(mesh):
    return jax.shard_map(
        body,
        mesh=mesh,
        in_specs=(P(None, AXES), P(), P(), P(), P()),
        out_specs=(P(None, AXES), P("cells", None)),
        check_vma=False,
    )
```

```python
import jax
import jax.numpy as jnp
from jax import lax
from jax.experimental import pallas as pl
from jax.experimental.pallas import tpu as pltpu
from jax.sharding import PartitionSpec as P

f32 = jnp.float32
bf16 = jnp.bfloat16
i32 = jnp.int32
HALF = 64
PIECE = 4096
LANES = 128
TILE = 16
AXES = ("cells", "grp")
BY_CELLS = (((1,), (1,)), ((), ()))
BY_ROWS = (((0,), (0,)), ((), ()))


def iota(shape, axis):
    return lax.broadcasted_iota(i32, shape, axis)


def split(value, parts):
    out = []
    for i in range(parts):
        out.append(value.astype(bf16))
        if i + 1 < parts:
            value = value - out[-1].astype(f32)
    return out


def lane_of(value, lane):
    return jnp.broadcast_to(value[:, lane : lane + 1], value.shape)


def halves(value, lane):
    left = iota(value.shape, 1) < HALF
    return jnp.where(left, lane_of(value, lane), lane_of(value, HALF + lane))


def column(row, first, count):
    shape = (count, row.shape[1])
    pick = iota(shape, 1) == iota(shape, 0) + first
    return jnp.sum(jnp.where(pick, jnp.broadcast_to(row, shape), 0.0), axis=1, keepdims=True)


def pack_pairs(ref):
    pairs = ref.shape[0] // 2
    even = ref[pl.ds(0, pairs, stride=2), :]
    odd = ref[pl.ds(1, pairs, stride=2), :]
    return jnp.where(iota(even.shape, 1) < HALF, even, odd)


def unpack_pairs(ref, tile):
    pairs = tile.shape[0]
    left = iota(tile.shape, 1) < HALF
    turned = pltpu.roll(tile, HALF, 1)
    ref[pl.ds(0, pairs, stride=2), :] = jnp.where(left, tile, turned)
    ref[pl.ds(1, pairs, stride=2), :] = jnp.where(left, turned, tile)
    return ref[...]


def repeat(count, step):
    if count <= 32:
        for i in range(count):
            step(i, 0)
    else:
        lax.fori_loop(0, count, step, 0)


class Plan:
    def __init__(self, x, means, pop):
        self.dims, self.cells = x.shape
        self.clusters = means.shape[0]
        self.batches = pop.shape[0]
        self.rows = lax.axis_size("cells")
        self.cols = lax.axis_size("grp")
        self.devices = self.rows * self.cols
        self.total = self.cells * self.devices
        self.most = 2 * self.total // self.batches
        self.reach = (self.most - 2) // self.cells + 1
        self.lone = self.most >= self.cells
        outside = -(-(self.total - self.cells) // self.most)
        local = min(self.batches, self.batches - outside + 2)
        self.tiles = -(-local // TILE)
        self.local = self.tiles * TILE
        self.group = max(1, LANES // self.clusters)
        self.groups = self.local // self.group
        self.depth = self.group * self.clusters
        self.table = (self.groups + 1) * self.depth
        self.width = -(-(3 * self.clusters + 4) // LANES) * LANES
        self.pairs = self.clusters // 2
        self.part = self.pairs // 2
        self.gap = HALF - (self.dims + 1)
        self.gap_rows = -(-(self.dims + 1) // self.gap)
        self.owned_pairs = self.clusters // self.rows // 2
        self.keep = self.devices * self.pairs * 3 * LANES * 4 <= 1 << 20
        self.fixed_marks = 10
        self.window = min(self.group, 4)
        self.piece = min(self.cells, 256)
        self.pieces = self.cells // self.piece
        self.sends = min(self.pieces, 4)
        self.chunk = min(self.cells, PIECE)
        self.chunks = self.cells // self.chunk

    def at(self, c):
        return slice(c * self.chunk, (c + 1) * self.chunk)


def count_kernel(
    plan, pop_hbm, lam_hbm, scale_hbm, means_hbm, x_hbm, send, prior, counts, sizes, places, parts, xs, info, ridges,
    pop, lam, scale, means, ends, ms, seg, sems, small,
):
    k = plan.clusters
    inputs = [
        pltpu.make_async_copy(source, target, small.at[i])
        for i, (source, target) in enumerate(
            ((pop_hbm, pop), (means_hbm, means), (scale_hbm, scale), (lam_hbm, lam))
        )
    ]
    copies = [
        pltpu.make_async_copy(x_hbm.at[:, plan.at(c)], xs.at[:, plan.at(c)], sems.at[c])
        for c in range(plan.chunks)
    ]
    for copy in inputs + copies:
        copy.start()
    offset = (lax.axis_index("cells") * plan.cols + lax.axis_index("grp")) * plan.cells
    inputs[0].wait()
    running, base, blocks = jnp.int32(0), jnp.int32(0), jnp.int32(0)
    for low in range(0, plan.batches, 8):
        held = [pop[b] for b in range(low, min(low + 8, plan.batches))]
        while len(held) > 1:
            held = [sum(held[i : i + 2]) for i in range(0, len(held), 2)]
        running = running + held[0]
        base = jnp.where(running <= offset, running, base)
        blocks = blocks + (running <= offset).astype(i32)
    first, running = blocks * 8, base
    for j in range(8):
        running = running + pop[jnp.minimum(blocks * 8 + j, plan.batches - 1)]
        base = jnp.where(running <= offset, running, base)
        first = first + (running <= offset).astype(i32)

    end = base + pop[first] - offset
    ends[0] = end
    here = jnp.int32(0)
    for c in range(plan.pieces + 1):
        place_of = min(c * plan.piece, plan.cells - 1)

        def onward(held):
            end = held[1] + pop[first + held[0] + 1]
            ends[held[0] + 1] = end
            return held[0] + 1, end

        here, end = lax.while_loop(lambda held, at=place_of: held[1] <= at, onward, (here, end))
        info[4 + c] = here
    segments = here + 1
    last = first + here
    tiles = lax.div(segments + TILE - 1, TILE)
    info[0], info[1], info[2] = first, last, segments

    lane = iota((1, LANES), 1)
    cell = iota((8, plan.cells), 1)
    half = TILE // 2

    def mark(g, held):
        for j in range(half):
            s = g * half + j
            after = jnp.float32(s + 1) if isinstance(s, int) else (s + 1).astype(f32)
            held = jnp.where(cell >= ends[jnp.minimum(s, here)], after, held)
        return held

    def place(held):
        places[...] = jnp.concatenate([held] * (TILE // 8), axis=0).astype(bf16)

    @pl.when(segments <= half)
    def few():
        place(mark(0, jnp.zeros(cell.shape, f32)))

    @pl.when(segments > half)
    def many():
        seg[...] = mark(0, jnp.zeros(cell.shape, f32))

        def locate(g, carry):
            seg[...] = mark(g, seg[...])
            return carry

        lax.fori_loop(1, lax.div(segments + half - 1, half), locate, 0)
        place(seg[...])

    for copy in inputs[1:]:
        copy.wait()

    def note(g, carry):
        row = jnp.zeros((1, LANES), f32)
        for j in range(TILE):
            b = jnp.minimum(first + g * TILE + j, plan.batches - 1)
            ridges[g * TILE + j] = lam[b]
            row = jnp.where(lane == j, pop[b].astype(f32), row)
        sizes[pl.ds(g, 1), :] = row
        return carry

    lax.fori_loop(1, tiles, note, 0)
    note(0, 0)
    ms[...] = jnp.zeros_like(ms)
    ms[:, 0 : plan.dims] = means[...]
    m = ms[...]
    m1, m2, m3 = [part.astype(f32) for part in split(m, 3)]
    zero = jnp.zeros_like(m)

    def twice(value):
        return value + pltpu.roll(value, HALF, 1)

    weights = jnp.concatenate(
        [
            jnp.concatenate([twice(m1), m1], axis=1),
            jnp.concatenate([twice(m2), zero], axis=1),
            jnp.concatenate([m3, zero], axis=1),
        ],
        axis=0,
    ).astype(bf16)
    lengths = jnp.sum(m * m, axis=1, keepdims=True)
    soft = jnp.ones((k, 1), f32)
    row = iota((k, 1), 0)
    for c in range(k):
        soft = jnp.where(row == c, scale[c], soft)
    inverse = 1.0 / (2.0 * soft)
    low = plan.dims // 8 * 8
    over = plan.dims - low
    shape = (8, plan.chunk)
    tail_row = iota(shape, 0)
    constant = jnp.where(tail_row == over, 1.0, 0.0)
    rest = [jnp.zeros(shape, f32)] * ((HALF - low) // 8 - 1)

    def affinity(c):
        at = plan.at(c)
        if over:
            moved = pltpu.roll(xs[plan.dims - 8 : plan.dims, at], over, 0)
            tail = jnp.where(tail_row < over, moved, constant)
        else:
            tail = constant
        x = jnp.concatenate([xs[0:low, at], tail] + rest, axis=0)
        x1, x2, x3 = split(x, 3)
        parts[0:HALF, at] = x1
        parts[HALF:, at] = x2
        stacked = jnp.concatenate([x1, x2, x3, jnp.zeros_like(x1)], axis=0)
        dots = jnp.dot(weights, stacked, preferred_element_type=f32)
        dots = dots[0:k] + dots[k : 2 * k] + dots[2 * k : 3 * k]
        return (2.0 * dots - lengths) * inverse

    spots = iota((TILE, plan.chunk), 0).astype(f32).astype(bf16)

    def finish(c, scores):
        at = plan.at(c)
        raised = jnp.exp(scores - jnp.max(scores, axis=0, keepdims=True))
        chance = raised / jnp.sum(raised, axis=0, keepdims=True)
        prior[:, at] = chance
        hot = jnp.where(places[:, at] == spots, bf16(1), bf16(0))
        return lax.dot_general(
            jnp.concatenate(split(chance, 3), axis=0), hot, BY_CELLS, preferred_element_type=f32
        )

    found = jnp.zeros((3 * k, TILE), f32)
    scores = following = None
    for c in range(plan.chunks + 1):
        if c < plan.chunks:
            copies[c].wait()
            following = affinity(c)
        if c:
            found = found + finish(c - 1, scores)
        scores = following

    def settle(g, found):
        found = found[0:k] + found[k : 2 * k] + found[2 * k :]
        counts[g] = jnp.concatenate([found, jnp.zeros((k, LANES - TILE), f32)], axis=1)

    settle(0, found)

    def count(g, carry):
        rows = (iota((TILE, plan.cells), 0) + g * TILE).astype(f32).astype(bf16)
        hot = jnp.where(places[...] == rows, bf16(1), bf16(0))
        settle(
            g,
            lax.dot_general(
                jnp.concatenate(split(prior[...], 3), axis=0), hot, BY_CELLS, preferred_element_type=f32
            ),
        )
        return carry

    lax.fori_loop(1, tiles, count, 0)

    every = lax.fori_loop(1, tiles, lambda g, total: total + counts[g], counts[0])
    total = jnp.sum(every, axis=1, keepdims=True)
    end = counts[lax.div(here, TILE)]
    wide = iota((k, LANES), 1)
    last_count = jnp.sum(jnp.where(wide == lax.rem(here, TILE), end, 0.0), axis=1, keepdims=True)
    first_count = jnp.where(segments > 1, counts[0][:, 0:1], 0.0)
    spread = (k, plan.width)
    turn = iota(spread, 1) - iota(spread, 0)
    out = jnp.where(turn == 0, total, 0.0)
    out = jnp.where(turn == k, first_count, out)
    out = jnp.where(turn == 2 * k, last_count, out)
    out = jnp.sum(out, axis=0, keepdims=True)
    lanes = iota((1, plan.width), 1)
    out = jnp.where(lanes == 3 * k, first.astype(f32), out)
    out = jnp.where(lanes == 3 * k + 1, last.astype(f32), out)
    out = jnp.where(lanes == 3 * k + 2, lam[first], out)
    out = jnp.where(lanes == 3 * k + 3, lam[last], out)
    send[...] = jnp.broadcast_to(out, send.shape)


def masked(plan, a1, a2, places, base, at, order):
    base = jnp.full((TILE, plan.piece), base.astype(f32)).astype(bf16)
    relative = jnp.concatenate([places[:, at] - base] * (plan.clusters // TILE), axis=0)
    inside = [relative == bf16(j) for j in range(plan.window)]
    parts = [
        jnp.concatenate([jnp.where(here, a[:, at], bf16(0)) for here in inside], axis=0) for a in (a1, a2)
    ]
    return jnp.concatenate([parts[i] for i in order], axis=0)


def extra_windows(plan, info):
    return [lax.div(info[5 + c] - info[4 + c], plan.window) for c in range(plan.pieces)]


def other_windows(plan, info, more, step):
    for c in range(plan.pieces):

        def again(w, carry, c=c):
            step(c, info[4 + c] + w * plan.window)
            return carry

        lax.fori_loop(1, more[c] + 1, again, 0)


def moment_kernel(
    plan, info, ridges, got, prior, counts, sizes, places, parts, send, a1, a2, moments, wide, sums, turned
):
    k = plan.clusters
    first, last, segments = info[0], info[1], info[2]
    groups = lax.div(segments + plan.group - 1, plan.group)
    tiles = lax.div(segments + TILE - 1, TILE)

    table = got[...]
    total = column(jnp.sum(table, axis=0, keepdims=True), 0, k)
    heads, tails = table[:, 3 * k : 3 * k + 1], table[:, 3 * k + 1 : 3 * k + 2]

    def complete(batch):
        batch = batch.astype(f32)
        of_heads = jnp.sum(jnp.where(heads == batch, table, 0.0), axis=0, keepdims=True)
        of_tails = jnp.sum(jnp.where(tails == batch, table, 0.0), axis=0, keepdims=True)
        return column(of_heads, k, k) + column(of_tails, 2 * k, k)

    first_count, last_count = complete(first), complete(last)
    share = total / f32(plan.total)
    lane = iota((k, LANES), 1)

    def factors(g):
        held = counts[g]
        held = jnp.where(lane + g * TILE == 0, first_count, held)
        held = jnp.where(lane + g * TILE == segments - 1, last_count, held)
        ratio = (sizes[pl.ds(g, 1), :] * share + 1.0) / (held + 1.0)
        ratio = jnp.where(lane < TILE, ratio * ratio, 0.0)
        w1, w2, w3 = [part.astype(f32) for part in split(ratio, 3)]
        row = w1 + pltpu.roll(w2, TILE, 1) + pltpu.roll(w3, 2 * TILE, 1)
        return row.astype(bf16)[:, 0 : 4 * TILE]

    def factor_of(weights, g, at):
        shape = (TILE, at.stop - at.start)
        rows = (iota(shape, 0) + g * TILE).astype(f32).astype(bf16)
        hot = jnp.where(places[:, at] == rows, bf16(1), bf16(0))
        hot = jnp.concatenate([hot, hot, hot, jnp.zeros_like(hot)], axis=0)
        return jnp.dot(weights, hot, preferred_element_type=f32)

    weights = factors(0)
    size = plan.window * k

    def settle(at, factor):
        raised = prior[:, at] * factor
        a1[:, at], a2[:, at] = split(raised / jnp.sum(raised, axis=0, keepdims=True), 2)

    def collect(c, base):
        at = slice(c * plan.piece, (c + 1) * plan.piece)
        both = lax.dot_general(
            masked(plan, a1, a2, places, base, at, (0, 1)), parts[:, at], BY_CELLS, preferred_element_type=f32
        )
        to = pl.ds(pl.multiple_of(base * k, k), size)
        moments[to, :] = moments[to, :] + (both[0:size] + both[size:])

    sums[...] = jnp.zeros_like(sums)

    def gather(g, carry):
        start = g * plan.depth if isinstance(g, int) else pl.multiple_of(g * plan.depth, plan.depth)
        to = pl.ds(start, plan.depth)
        both = moments[to, :]
        both = both + pltpu.roll(both, HALF, 1)
        moments[to, :] = both
        mass = lane_of(both, plan.dims)
        inner, head, tail, every = sums[0], sums[1], sums[2], sums[3]
        for j in range(plan.group):
            s = g * plan.group + j
            at = slice(j * k, (j + 1) * k)
            ridge = ridges[s]
            part = both[at]
            every = every + part
            shrunk = part * (ridge / (mass[at] + ridge))
            inner = inner + jnp.where((s > 0) & (s < segments - 1), shrunk, 0.0)
            head = head + jnp.where((s == 0) & (segments > 1), part, 0.0)
            tail = tail + jnp.where(s == segments - 1, part, 0.0)
        sums[0], sums[1], sums[2], sums[3] = inner, head, tail, every
        return carry

    more = extra_windows(plan, info)
    simple = (tiles == 1) & (sum(more) == 0)

    def first_windows():
        spare = (TILE + plan.window) * k
        moments[0:spare, :] = jnp.zeros((spare, LANES), f32)
        for c in range(plan.chunks):
            settle(plan.at(c), factor_of(weights, 0, plan.at(c)))
        for c in range(plan.pieces):
            collect(c, info[4 + c])

    @pl.when(simple)
    def straight():
        first_windows()
        for g in range(TILE // plan.group):
            gather(g, 0)

    @pl.when(jnp.logical_not(simple) & (tiles == 1))
    def crowded():
        first_windows()

    @pl.when(tiles > 1)
    def general():
        def clear(g, carry):
            moments[pl.ds(pl.multiple_of(g * plan.depth, plan.depth), plan.depth), :] = jnp.zeros(
                (plan.depth, LANES), f32
            )
            return carry

        lax.fori_loop(0, groups + 1, clear, 0)
        wide[...] = jnp.zeros_like(wide)

        def add(g, carry):
            weights = factors(g)
            for c in range(plan.chunks):
                wide[:, plan.at(c)] += factor_of(weights, g, plan.at(c))
            return carry

        lax.fori_loop(0, tiles, add, 0)
        for c in range(plan.chunks):
            settle(plan.at(c), wide[:, plan.at(c)])
        for c in range(plan.pieces):
            collect(c, info[4 + c])

    @pl.when(sum(more) > 0)
    def others():
        other_windows(plan, info, more, collect)

    @pl.when(jnp.logical_not(simple))
    def looped():
        lax.fori_loop(0, groups, gather, 0)

    inner, head, tail, every = [pack_pairs(sums.at[i]) for i in range(4)]
    lanes = lax.rem(iota(inner.shape, 1), HALF)
    inner = jnp.where(lanes <= plan.dims, inner, 0.0)
    every = jnp.where(lanes <= plan.dims, every, 0.0)
    for j in range(plan.gap_rows):
        moved = pltpu.roll(every, (plan.dims + 1 - plan.gap * j) % LANES, 1)
        turned[j] = jnp.where(lanes > plan.dims, moved, 0.0)
    row = iota((plan.part, LANES), 0)

    def put(c, carry):
        gaps = jnp.zeros((plan.part, LANES), f32)
        for q in range(plan.owned_pairs):
            for j in range(plan.gap_rows):
                pair = c * plan.owned_pairs + q
                piece = jnp.broadcast_to(turned[j, pl.ds(pair, 1), :], gaps.shape)
                gaps = gaps + jnp.where(row == q * plan.gap_rows + j, piece, 0.0)
        for q in range(plan.cols):
            p = c * plan.cols + q
            for side in range(2):
                low = side * plan.part

                def write(low=low, p=p):
                    start = p * 3 * plan.part
                    send[pl.ds(start, plan.part), :] = inner[low : low + plan.part] + gaps
                    send[pl.ds(start + plan.part, plan.part), :] = head[low : low + plan.part]
                    send[pl.ds(start + 2 * plan.part, plan.part), :] = tail[low : low + plan.part]

                if isinstance(p, int):
                    if p % 2 == side:
                        write()
                else:
                    pl.when(lax.rem(p, 2) == side)(write)
        return carry

    repeat(plan.rows, put)


def reduce_kernel(plan, info, got, ids, mine, theirs, marks):
    k, part = plan.clusters, plan.part
    shape = (plan.devices, LANES)
    device = iota(shape, 0)

    def of(lane):
        return jnp.broadcast_to(ids[:, lane : lane + 1], shape)

    heads, tails = of(3 * k), of(3 * k + 1)
    me = lax.axis_index("cells") * plan.cols + lax.axis_index("grp")
    other = me + 1 - 2 * lax.rem(me, 2)

    def shifted(value, distance):
        return pltpu.roll(value, distance % plan.devices, 0)

    marks[0], marks[1] = of(3 * k + 2), of(3 * k + 3)
    own = ids[pl.ds(me, 1), :]
    pair = ids[pl.ds(other, 1), :]
    for i, (row, lane) in enumerate(((own, 3 * k), (own, 3 * k + 1), (pair, 3 * k), (pair, 3 * k + 1))):
        batch = jnp.broadcast_to(row[:, lane : lane + 1], shape)
        marks[2 + 2 * i] = jnp.where(heads == batch, 1.0, 0.0)
        marks[3 + 2 * i] = jnp.where(tails == batch, 1.0, 0.0)
    links = []

    def link(hop, to_head, from_head, mine, theirs):
        inside = (device + hop >= 0) & (device + hop < plan.devices)
        at = plan.fixed_marks + len(links)
        marks[at] = jnp.where(inside & (shifted(theirs, -hop) == mine), 1.0, 0.0)
        links.append((at, hop, to_head, from_head))

    for hop in range(1, plan.reach + 1):
        link(-hop, True, False, heads, tails)
        link(hop, False, True, tails, heads)
        if plan.lone:
            link(-hop, False, False, tails, tails)
            link(hop, False, False, tails, tails)

    block = (2 * part, LANES)
    top = iota(block, 0) < part

    def mark(i, r):
        return jnp.broadcast_to(marks[i, pl.ds(r, 1), :], block)

    def two(i, r):
        return jnp.where(top, mark(i, r), mark(i + 1, r))

    def ends_of(r):
        return got[pl.ds(r * 3 * part + part, 2 * part), :]

    def turn(value):
        return pltpu.roll(value, part, 0)

    def gather(r, carry):
        inner, shrunk, sums = carry
        ends = ends_of(r)
        whole = halves(ends, plan.dims)
        for at, hop, to_head, from_head in links:
            if isinstance(r, int):
                if not 0 <= r + hop < plan.devices:
                    continue
                there = r + hop
            else:
                there = jnp.clip(r + hop, 0, plan.devices - 1)
            mass = halves(ends_of(there), plan.dims)
            if to_head != from_head:
                mass = turn(mass)
            whole = whole + jnp.where(top == to_head, mark(at, r) * mass, 0.0)
        ridge = two(0, r)
        shrunk = shrunk + ends * (ridge / (whole + ridge))
        inner = inner + got[pl.ds(r * 3 * part, part), :]
        sums = tuple(total + ends * two(2 + 2 * i, r) for i, total in enumerate(sums))
        return inner, shrunk, sums

    zero = jnp.zeros(block, f32)
    state = (zero[0:part], zero, (zero,) * 4)
    if plan.devices <= 32:
        for r in range(plan.devices):
            state = gather(r, state)
    else:
        state = lax.fori_loop(0, plan.devices, gather, state)
    inner, shrunk, sums = state

    def fold(value):
        return (value + turn(value))[0:part]

    right = inner + fold(shrunk)
    intercept = right / (1.0 + halves(right, plan.dims))
    mine[0] = jnp.concatenate([intercept, intercept], axis=0)
    theirs[0:part] = intercept
    for i in range(2):
        value = sums[i] + turn(sums[i])
        mine[1 + i] = value
        theirs[(1 + i) * part : (2 + i) * part] = fold(sums[2 + i])
    mine[3] = jnp.concatenate([inner, inner], axis=0)


def correct_kernel(
    plan, info, ridges, mine, theirs, a1, a2, moments, places, xs, out_hbm, centroids_hbm,
    slopes, rows, spread, out, centroids, sems, done,
):
    k, part = plan.clusters, plan.part
    first, last, segments = info[0], info[1], info[2]
    groups = lax.div(segments + plan.group - 1, plan.group)
    me = lax.axis_index("cells") * plan.cols + lax.axis_index("grp")
    odd = jnp.full((plan.pairs, LANES), lax.rem(me, 2)) == 1
    low = iota((plan.pairs, LANES), 0) < part

    def both(i):
        piece = theirs[i * part : (i + 1) * part]
        piece = jnp.concatenate([piece, piece], axis=0)
        return unpack_pairs(spread, jnp.where(low != odd, mine[i], piece))

    intercept, first_sum, last_sum = both(0), both(1), both(2)
    def slope(g, carry):
        start = g * plan.depth if isinstance(g, int) else pl.multiple_of(g * plan.depth, plan.depth)
        held = moments[pl.ds(start, plan.depth), :]
        made = []
        for j in range(plan.group):
            s = g * plan.group + j
            part = held[j * k : (j + 1) * k]
            part = jnp.where(s == 0, first_sum, part)
            part = jnp.where(s == segments - 1, last_sum, part)
            mass = lane_of(part, plan.dims)
            ridge = ridges[s]
            made.append((part - mass * intercept) / (mass + ridge))
        for i, piece in enumerate(split(jnp.concatenate(made, axis=0), 2)):
            slopes[i, pl.ds(start, plan.depth), :] = piece
        return carry

    size = plan.window * k

    rows[...] = mine[3]
    lanes = lax.rem(iota((1, LANES), 1), HALF)
    for q in range(plan.owned_pairs):
        every = jnp.zeros((1, LANES), f32)
        for j in range(plan.gap_rows):
            at = q * plan.gap_rows + j
            piece = jnp.where(lanes > plan.dims, rows[at : at + 1], 0.0)
            moved = pltpu.roll(piece, (plan.gap * j - plan.dims - 1) % LANES, 1)
            inside = (lanes >= plan.gap * j) & (lanes < plan.gap * (j + 1))
            every = every + jnp.where(inside, moved, 0.0)
        every = every / (1.0 + halves(every, plan.dims))
        centroids[2 * q : 2 * q + 1] = every[:, 0 : plan.dims]
        centroids[2 * q + 1 : 2 * q + 2] = pltpu.roll(every, HALF, 1)[:, 0 : plan.dims]
    last_copy = pltpu.make_async_copy(centroids, centroids_hbm, done)
    last_copy.start()
    copies = []
    span = plan.cells // plan.sends
    for c in range(plan.sends):
        at = slice(c * span, (c + 1) * span)
        copies.append(pltpu.make_async_copy(out.at[:, at], out_hbm.at[:, at], sems.at[c]))

    def moved(c, base):
        at = slice(c * plan.piece, (c + 1) * plan.piece)
        rows_of = pl.ds(pl.multiple_of(base * k, k), size)
        large, fine = slopes[0, rows_of, 0:HALF], slopes[1, rows_of, 0:HALF]
        return lax.dot_general(
            jnp.concatenate([large, fine, large], axis=0),
            masked(plan, a1, a2, places, base, at, (0, 0, 1)),
            BY_ROWS,
            preferred_element_type=f32,
        )[0 : plan.dims]

    more = extra_windows(plan, info)

    at_once = TILE // plan.group
    blank = jnp.zeros((plan.depth, LANES), bf16)
    simple = (sum(more) == 0) & (groups <= at_once)

    @pl.when(simple)
    def straight():
        for g in range(at_once):
            slope(g, 0)
        for i in range(2):
            slopes[i, at_once * plan.depth : (at_once + 1) * plan.depth, :] = blank
        for c in range(plan.pieces):
            at = slice(c * plan.piece, (c + 1) * plan.piece)
            out[:, at] = xs[:, at] - moved(c, info[4 + c])
            if (c + 1) * plan.sends % plan.pieces == 0:
                copies[(c + 1) * plan.sends // plan.pieces - 1].start()

    @pl.when(jnp.logical_not(simple))
    def general():
        lax.fori_loop(0, groups, slope, 0)
        for i in range(2):
            slopes[i, pl.ds(pl.multiple_of(groups * plan.depth, plan.depth), plan.depth), :] = blank
        for c in range(plan.pieces):
            at = slice(c * plan.piece, (c + 1) * plan.piece)
            out[:, at] = xs[:, at] - moved(c, info[4 + c])

        def step(c, base):
            at = slice(c * plan.piece, (c + 1) * plan.piece)
            out[:, at] = out[:, at] - moved(c, base)

        other_windows(plan, info, more, step)
        for copy in copies:
            copy.start()

    for copy in copies:
        copy.wait()
    last_copy.wait()


VMEM = pl.BlockSpec(memory_space=pltpu.VMEM)
SMEM = pl.BlockSpec(memory_space=pltpu.SMEM)
WHERE = pl.BlockSpec(memory_space=pltpu.HBM)


def hold_scalars(value):
    return pltpu.with_memory_space_constraint(value, pltpu.SMEM)


def bound(kernel, plan, name):
    def run(*refs):
        kernel(plan, *refs)

    run.__name__ = name
    return run


def body(x, means, scale, lam, pop):
    plan = Plan(x, means, pop)
    k, cells = plan.clusters, plan.cells
    params = pltpu.CompilerParams(vmem_limit_bytes=(16 << 20) if plan.keep else None)

    def kept(shape, kind=f32):
        return pltpu.VMEM(shape, kind) if plan.keep else jax.ShapeDtypeStruct(shape, kind)

    def hold(value):
        return pltpu.with_memory_space_constraint(value, pltpu.VMEM) if plan.keep else value

    send, prior, counts, sizes, places, parts, xs, info, ridges = pl.pallas_call(
        bound(count_kernel, plan, "count"),
        name="count",
        out_shape=(
            kept((plan.devices, plan.width)),
            kept((k, cells)),
            kept((plan.tiles, k, LANES)),
            kept((plan.tiles, LANES)),
            kept((TILE, cells), bf16),
            kept((2 * HALF, cells), bf16),
            kept((plan.dims, cells)),
            pltpu.SMEM((5 + plan.pieces,), i32),
            pltpu.SMEM((plan.local,), f32),
        ),
        in_specs=[WHERE] * 5,
        out_specs=(VMEM,) * 7 + (SMEM,) * 2,
        scratch_shapes=[
            pltpu.SMEM(pop.shape, i32),
            pltpu.SMEM(lam.shape, f32),
            pltpu.SMEM(scale.shape, f32),
            pltpu.VMEM(means.shape, f32),
            pltpu.SMEM((plan.batches,), i32),
            pltpu.VMEM((k, LANES), f32),
            pltpu.VMEM((8, cells), f32),
            pltpu.SemaphoreType.DMA((plan.chunks,)),
            pltpu.SemaphoreType.DMA((4,)),
        ],
    )(pop, lam, scale, means, x)
    prior, counts, sizes, places, parts, xs = map(hold, (prior, counts, sizes, places, parts, xs))
    info, ridges = hold_scalars(info), hold_scalars(ridges)
    ids = hold(lax.all_to_all(send, AXES, 0, 0, tiled=True))
    send, a1, a2, moments = pl.pallas_call(
        bound(moment_kernel, plan, "moment"),
        name="moment",
        compiler_params=params,
        out_shape=(
            kept((plan.devices * 3 * plan.part, LANES)),
            kept((k, cells), bf16),
            kept((k, cells), bf16),
            kept((plan.table, LANES)),
        ),
        in_specs=[SMEM] * 2 + [VMEM] * 6,
        out_specs=(VMEM,) * 4,
        scratch_shapes=[
            pltpu.VMEM((k, cells), f32),
            pltpu.VMEM((4, k, LANES), f32),
            pltpu.VMEM((plan.gap_rows, plan.pairs, LANES), f32),
        ],
    )(info, ridges, ids, prior, counts, sizes, places, parts)
    a1, a2, moments = map(hold, (a1, a2, moments))
    rows = send.shape[0]
    got = lax.all_to_all(send.reshape(rows, 1, LANES), AXES, 0, 0, tiled=True)
    got = hold(got.reshape(rows, LANES))
    marks = plan.fixed_marks + plan.reach * (4 if plan.lone else 2)
    mine, theirs = pl.pallas_call(
        bound(reduce_kernel, plan, "reduce"),
        name="reduce",
        compiler_params=params,
        out_shape=(kept((4, plan.pairs, LANES)), kept((3 * plan.part, LANES))),
        in_specs=[SMEM] + [VMEM] * 2,
        out_specs=(VMEM,) * 2,
        scratch_shapes=[pltpu.VMEM((marks, plan.devices, LANES), f32)],
    )(info, got, ids)
    mine = hold(mine)
    swap = [(i, i + 1 - 2 * (i % 2)) for i in range(plan.devices)]
    theirs = hold(lax.ppermute(theirs, AXES, swap))
    corrected, centroids = pl.pallas_call(
        bound(correct_kernel, plan, "correct"),
        name="correct",
        compiler_params=params,
        out_shape=(
            jax.ShapeDtypeStruct(x.shape, f32),
            jax.ShapeDtypeStruct((k // plan.rows, plan.dims), f32),
        ),
        in_specs=[SMEM] * 2 + [VMEM] * 7,
        out_specs=(WHERE, WHERE),
        scratch_shapes=[
            pltpu.VMEM((2, plan.table, LANES), bf16),
            pltpu.VMEM((plan.pairs, LANES), f32),
            pltpu.VMEM((k, LANES), f32),
            pltpu.VMEM((plan.dims, cells), f32),
            pltpu.VMEM((k // plan.rows, plan.dims), f32),
            pltpu.SemaphoreType.DMA((plan.sends,)),
            pltpu.SemaphoreType.DMA,
        ],
    )(info, ridges, mine, theirs, a1, a2, moments, places, xs)
    return corrected, centroids


def solution(mesh):
    return jax.shard_map(
        body,
        mesh=mesh,
        in_specs=(P(None, AXES), P(), P(), P(), P()),
        out_specs=(P(None, AXES), P("cells", None)),
        check_vma=False,
    )
```

```python
import jax
import jax.numpy as jnp
from jax import lax
from jax.experimental import pallas as pl
from jax.experimental.pallas import tpu as pltpu
from jax.sharding import PartitionSpec as P

f32 = jnp.float32
bf16 = jnp.bfloat16
i32 = jnp.int32
HALF = 64
PIECE = 4096
LANES = 128
TILE = 16
AXES = ("cells", "grp")
BY_CELLS = (((1,), (1,)), ((), ()))
BY_ROWS = (((0,), (0,)), ((), ()))


def iota(shape, axis):
    return lax.broadcasted_iota(i32, shape, axis)


def split(value, parts):
    out = []
    for i in range(parts):
        out.append(value.astype(bf16))
        if i + 1 < parts:
            value = value - out[-1].astype(f32)
    return out


def lane_of(value, lane):
    return jnp.broadcast_to(value[:, lane : lane + 1], value.shape)


def halves(value, lane):
    left = iota(value.shape, 1) < HALF
    return jnp.where(left, lane_of(value, lane), lane_of(value, HALF + lane))


def column(row, first, count):
    shape = (count, row.shape[1])
    pick = iota(shape, 1) == iota(shape, 0) + first
    return jnp.sum(jnp.where(pick, jnp.broadcast_to(row, shape), 0.0), axis=1, keepdims=True)


def pack_pairs(ref):
    pairs = ref.shape[0] // 2
    even = ref[pl.ds(0, pairs, stride=2), :]
    odd = ref[pl.ds(1, pairs, stride=2), :]
    return jnp.where(iota(even.shape, 1) < HALF, even, odd)


def unpack_pairs(ref, tile):
    pairs = tile.shape[0]
    left = iota(tile.shape, 1) < HALF
    turned = pltpu.roll(tile, HALF, 1)
    ref[pl.ds(0, pairs, stride=2), :] = jnp.where(left, tile, turned)
    ref[pl.ds(1, pairs, stride=2), :] = jnp.where(left, turned, tile)
    return ref[...]


def repeat(count, step):
    if count <= 32:
        for i in range(count):
            step(i, 0)
    else:
        lax.fori_loop(0, count, step, 0)


class Plan:
    def __init__(self, x, means, pop):
        self.dims, self.cells = x.shape
        self.clusters = means.shape[0]
        self.batches = pop.shape[0]
        self.rows = lax.axis_size("cells")
        self.cols = lax.axis_size("grp")
        self.devices = self.rows * self.cols
        self.total = self.cells * self.devices
        self.most = 2 * self.total // self.batches
        self.reach = (self.most - 2) // self.cells + 1
        self.lone = self.most >= self.cells
        outside = -(-(self.total - self.cells) // self.most)
        local = min(self.batches, self.batches - outside + 2)
        self.tiles = -(-local // TILE)
        self.local = self.tiles * TILE
        self.group = max(1, LANES // self.clusters)
        self.groups = self.local // self.group
        self.depth = self.group * self.clusters
        self.table = (self.groups + 1) * self.depth
        self.width = -(-(3 * self.clusters + 4) // LANES) * LANES
        self.pairs = self.clusters // 2
        self.part = self.pairs // 2
        self.gap = HALF - (self.dims + 1)
        self.gap_rows = -(-(self.dims + 1) // self.gap)
        self.owned_pairs = self.clusters // self.rows // 2
        self.keep = self.devices * self.pairs * 3 * LANES * 4 <= 1 << 20
        self.fixed_marks = 10
        self.window = min(self.group, 4)
        self.piece = min(self.cells, 256)
        self.pieces = self.cells // self.piece
        self.sends = min(self.pieces, 4)
        self.chunk = min(self.cells, PIECE)
        self.chunks = self.cells // self.chunk

    def at(self, c):
        return slice(c * self.chunk, (c + 1) * self.chunk)


def count_kernel(
    plan, pop_hbm, lam_hbm, scale_hbm, means_hbm, x_hbm, send, prior, counts, sizes, places, parts, xs, info, ridges,
    pop, lam, scale, means, ends, ms, seg, sems, small,
):
    k = plan.clusters
    inputs = [
        pltpu.make_async_copy(source, target, small.at[i])
        for i, (source, target) in enumerate(
            ((pop_hbm, pop), (means_hbm, means), (scale_hbm, scale), (lam_hbm, lam))
        )
    ]
    copies = [
        pltpu.make_async_copy(x_hbm.at[:, plan.at(c)], xs.at[:, plan.at(c)], sems.at[c])
        for c in range(plan.chunks)
    ]
    for copy in inputs + copies:
        copy.start()
    offset = (lax.axis_index("cells") * plan.cols + lax.axis_index("grp")) * plan.cells
    inputs[0].wait()
    running, base, blocks = jnp.int32(0), jnp.int32(0), jnp.int32(0)
    for low in range(0, plan.batches, 8):
        held = [pop[b] for b in range(low, min(low + 8, plan.batches))]
        while len(held) > 1:
            held = [sum(held[i : i + 2]) for i in range(0, len(held), 2)]
        running = running + held[0]
        base = jnp.where(running <= offset, running, base)
        blocks = blocks + (running <= offset).astype(i32)
    first, running = blocks * 8, base
    for j in range(8):
        running = running + pop[jnp.minimum(blocks * 8 + j, plan.batches - 1)]
        base = jnp.where(running <= offset, running, base)
        first = first + (running <= offset).astype(i32)

    end = base + pop[first] - offset
    ends[0] = end
    here = jnp.int32(0)
    for c in range(plan.pieces + 1):
        place_of = min(c * plan.piece, plan.cells - 1)

        def onward(held):
            end = held[1] + pop[first + held[0] + 1]
            ends[held[0] + 1] = end
            return held[0] + 1, end

        here, end = lax.while_loop(lambda held, at=place_of: held[1] <= at, onward, (here, end))
        info[4 + c] = here
    segments = here + 1
    last = first + here
    tiles = lax.div(segments + TILE - 1, TILE)
    info[0], info[1], info[2] = first, last, segments

    lane = iota((1, LANES), 1)
    cell = iota((8, plan.cells), 1)
    half = TILE // 2

    def mark(g, held):
        for j in range(half):
            s = g * half + j
            after = jnp.float32(s + 1) if isinstance(s, int) else (s + 1).astype(f32)
            held = jnp.where(cell >= ends[jnp.minimum(s, here)], after, held)
        return held

    def place(held):
        places[...] = jnp.concatenate([held] * (TILE // 8), axis=0).astype(bf16)

    @pl.when(segments <= half)
    def few():
        place(mark(0, jnp.zeros(cell.shape, f32)))

    @pl.when(segments > half)
    def many():
        seg[...] = mark(0, jnp.zeros(cell.shape, f32))

        def locate(g, carry):
            seg[...] = mark(g, seg[...])
            return carry

        lax.fori_loop(1, lax.div(segments + half - 1, half), locate, 0)
        place(seg[...])

    for copy in inputs[1:]:
        copy.wait()

    def note(g, carry):
        row = jnp.zeros((1, LANES), f32)
        for j in range(TILE):
            b = jnp.minimum(first + g * TILE + j, plan.batches - 1)
            ridges[g * TILE + j] = lam[b]
            row = jnp.where(lane == j, pop[b].astype(f32), row)
        sizes[pl.ds(g, 1), :] = row
        return carry

    lax.fori_loop(1, tiles, note, 0)
    note(0, 0)
    ms[...] = jnp.zeros_like(ms)
    ms[:, 0 : plan.dims] = means[...]
    m = ms[...]
    m1, m2, m3 = [part.astype(f32) for part in split(m, 3)]
    zero = jnp.zeros_like(m)

    def twice(value):
        return value + pltpu.roll(value, HALF, 1)

    weights = jnp.concatenate(
        [
            jnp.concatenate([twice(m1), m1], axis=1),
            jnp.concatenate([twice(m2), zero], axis=1),
            jnp.concatenate([m3, zero], axis=1),
        ],
        axis=0,
    ).astype(bf16)
    lengths = jnp.sum(m * m, axis=1, keepdims=True)
    soft = jnp.ones((k, 1), f32)
    row = iota((k, 1), 0)
    for c in range(k):
        soft = jnp.where(row == c, scale[c], soft)
    inverse = 1.0 / (2.0 * soft)
    low = plan.dims // 8 * 8
    over = plan.dims - low
    shape = (8, plan.chunk)
    tail_row = iota(shape, 0)
    constant = jnp.where(tail_row == over, 1.0, 0.0)
    rest = [jnp.zeros(shape, f32)] * ((HALF - low) // 8 - 1)

    def affinity(c):
        at = plan.at(c)
        if over:
            moved = pltpu.roll(xs[plan.dims - 8 : plan.dims, at], over, 0)
            tail = jnp.where(tail_row < over, moved, constant)
        else:
            tail = constant
        x = jnp.concatenate([xs[0:low, at], tail] + rest, axis=0)
        x1, x2, x3 = split(x, 3)
        parts[0:HALF, at] = x1
        parts[HALF:, at] = x2
        stacked = jnp.concatenate([x1, x2, x3], axis=0)
        dots = jnp.dot(weights[:, 0 : 3 * HALF], stacked, preferred_element_type=f32)
        dots = dots[0:k] + dots[k : 2 * k] + dots[2 * k : 3 * k]
        return (2.0 * dots - lengths) * inverse

    spots = iota((TILE, plan.chunk), 0).astype(f32).astype(bf16)

    def finish(c, scores):
        at = plan.at(c)
        raised = jnp.exp(scores - jnp.max(scores, axis=0, keepdims=True))
        chance = raised / jnp.sum(raised, axis=0, keepdims=True)
        prior[:, at] = chance
        hot = jnp.where(places[:, at] == spots, bf16(1), bf16(0))
        return lax.dot_general(
            jnp.concatenate(split(chance, 3), axis=0), hot, BY_CELLS, preferred_element_type=f32
        )

    found = jnp.zeros((3 * k, TILE), f32)
    scores = following = None
    for c in range(plan.chunks + 1):
        if c < plan.chunks:
            copies[c].wait()
            following = affinity(c)
        if c:
            found = found + finish(c - 1, scores)
        scores = following

    def settle(g, found):
        found = found[0:k] + found[k : 2 * k] + found[2 * k :]
        counts[g] = jnp.concatenate([found, jnp.zeros((k, LANES - TILE), f32)], axis=1)

    settle(0, found)

    def count(g, carry):
        rows = (iota((TILE, plan.cells), 0) + g * TILE).astype(f32).astype(bf16)
        hot = jnp.where(places[...] == rows, bf16(1), bf16(0))
        settle(
            g,
            lax.dot_general(
                jnp.concatenate(split(prior[...], 3), axis=0), hot, BY_CELLS, preferred_element_type=f32
            ),
        )
        return carry

    lax.fori_loop(1, tiles, count, 0)

    every = lax.fori_loop(1, tiles, lambda g, total: total + counts[g], counts[0])
    total = jnp.sum(every, axis=1, keepdims=True)
    end = counts[lax.div(here, TILE)]
    wide = iota((k, LANES), 1)
    last_count = jnp.sum(jnp.where(wide == lax.rem(here, TILE), end, 0.0), axis=1, keepdims=True)
    first_count = jnp.where(segments > 1, counts[0][:, 0:1], 0.0)
    spread = (k, plan.width)
    turn = iota(spread, 1) - iota(spread, 0)
    out = jnp.where(turn == 0, total, 0.0)
    out = jnp.where(turn == k, first_count, out)
    out = jnp.where(turn == 2 * k, last_count, out)
    out = jnp.sum(out, axis=0, keepdims=True)
    lanes = iota((1, plan.width), 1)
    out = jnp.where(lanes == 3 * k, first.astype(f32), out)
    out = jnp.where(lanes == 3 * k + 1, last.astype(f32), out)
    out = jnp.where(lanes == 3 * k + 2, lam[first], out)
    out = jnp.where(lanes == 3 * k + 3, lam[last], out)
    send[...] = jnp.broadcast_to(out, send.shape)


def masked(plan, a1, a2, places, base, at, order):
    base = jnp.full((TILE, plan.piece), base.astype(f32)).astype(bf16)
    relative = jnp.concatenate([places[:, at] - base] * (plan.clusters // TILE), axis=0)
    inside = [relative == bf16(j) for j in range(plan.window)]
    parts = [
        jnp.concatenate([jnp.where(here, a[:, at], bf16(0)) for here in inside], axis=0) for a in (a1, a2)
    ]
    return jnp.concatenate([parts[i] for i in order], axis=0)


def extra_windows(plan, info):
    return [lax.div(info[5 + c] - info[4 + c], plan.window) for c in range(plan.pieces)]


def other_windows(plan, info, more, step):
    for c in range(plan.pieces):

        def again(w, carry, c=c):
            step(c, info[4 + c] + w * plan.window)
            return carry

        lax.fori_loop(1, more[c] + 1, again, 0)


def moment_kernel(
    plan, info, ridges, got, prior, counts, sizes, places, parts, send, a1, a2, moments, wide, sums, turned
):
    k = plan.clusters
    first, last, segments = info[0], info[1], info[2]
    groups = lax.div(segments + plan.group - 1, plan.group)
    tiles = lax.div(segments + TILE - 1, TILE)

    table = got[...]
    total = column(jnp.sum(table, axis=0, keepdims=True), 0, k)
    heads, tails = table[:, 3 * k : 3 * k + 1], table[:, 3 * k + 1 : 3 * k + 2]

    def complete(batch):
        batch = batch.astype(f32)
        of_heads = jnp.sum(jnp.where(heads == batch, table, 0.0), axis=0, keepdims=True)
        of_tails = jnp.sum(jnp.where(tails == batch, table, 0.0), axis=0, keepdims=True)
        return column(of_heads, k, k) + column(of_tails, 2 * k, k)

    first_count, last_count = complete(first), complete(last)
    share = total / f32(plan.total)
    lane = iota((k, LANES), 1)

    def factors(g):
        held = counts[g]
        held = jnp.where(lane + g * TILE == 0, first_count, held)
        held = jnp.where(lane + g * TILE == segments - 1, last_count, held)
        ratio = (sizes[pl.ds(g, 1), :] * share + 1.0) / (held + 1.0)
        ratio = jnp.where(lane < TILE, ratio * ratio, 0.0)
        w1, w2, w3 = [part.astype(f32) for part in split(ratio, 3)]
        row = w1 + pltpu.roll(w2, TILE, 1) + pltpu.roll(w3, 2 * TILE, 1)
        return row.astype(bf16)[:, 0 : 3 * TILE]

    def factor_of(weights, g, at):
        shape = (TILE, at.stop - at.start)
        rows = (iota(shape, 0) + g * TILE).astype(f32).astype(bf16)
        hot = jnp.where(places[:, at] == rows, bf16(1), bf16(0))
        hot = jnp.concatenate([hot, hot, hot], axis=0)
        return jnp.dot(weights, hot, preferred_element_type=f32)

    weights = factors(0)
    size = plan.window * k

    def settle(at, factor):
        raised = prior[:, at] * factor
        a1[:, at], a2[:, at] = split(raised / jnp.sum(raised, axis=0, keepdims=True), 2)

    def collect(c, base):
        at = slice(c * plan.piece, (c + 1) * plan.piece)
        both = lax.dot_general(
            masked(plan, a1, a2, places, base, at, (0, 1)), parts[:, at], BY_CELLS, preferred_element_type=f32
        )
        to = pl.ds(pl.multiple_of(base * k, k), size)
        moments[to, :] = moments[to, :] + (both[0:size] + both[size:])

    sums[...] = jnp.zeros_like(sums)

    def gather(g, carry):
        start = g * plan.depth if isinstance(g, int) else pl.multiple_of(g * plan.depth, plan.depth)
        to = pl.ds(start, plan.depth)
        both = moments[to, :]
        both = both + pltpu.roll(both, HALF, 1)
        moments[to, :] = both
        mass = lane_of(both, plan.dims)
        inner, head, tail, every = sums[0], sums[1], sums[2], sums[3]
        for j in range(plan.group):
            s = g * plan.group + j
            at = slice(j * k, (j + 1) * k)
            ridge = ridges[s]
            part = both[at]
            every = every + part
            shrunk = part * (ridge / (mass[at] + ridge))
            inner = inner + jnp.where((s > 0) & (s < segments - 1), shrunk, 0.0)
            head = head + jnp.where((s == 0) & (segments > 1), part, 0.0)
            tail = tail + jnp.where(s == segments - 1, part, 0.0)
        sums[0], sums[1], sums[2], sums[3] = inner, head, tail, every
        return carry

    more = extra_windows(plan, info)
    simple = (tiles == 1) & (sum(more) == 0)

    def first_windows():
        spare = (TILE + plan.window) * k
        moments[0:spare, :] = jnp.zeros((spare, LANES), f32)
        for c in range(plan.chunks):
            settle(plan.at(c), factor_of(weights, 0, plan.at(c)))
        for c in range(plan.pieces):
            collect(c, info[4 + c])

    @pl.when(simple)
    def straight():
        first_windows()
        for g in range(TILE // plan.group):
            gather(g, 0)

    @pl.when(jnp.logical_not(simple) & (tiles == 1))
    def crowded():
        first_windows()

    @pl.when(tiles > 1)
    def general():
        def clear(g, carry):
            moments[pl.ds(pl.multiple_of(g * plan.depth, plan.depth), plan.depth), :] = jnp.zeros(
                (plan.depth, LANES), f32
            )
            return carry

        lax.fori_loop(0, groups + 1, clear, 0)
        wide[...] = jnp.zeros_like(wide)

        def add(g, carry):
            weights = factors(g)
            for c in range(plan.chunks):
                wide[:, plan.at(c)] += factor_of(weights, g, plan.at(c))
            return carry

        lax.fori_loop(0, tiles, add, 0)
        for c in range(plan.chunks):
            settle(plan.at(c), wide[:, plan.at(c)])
        for c in range(plan.pieces):
            collect(c, info[4 + c])

    @pl.when(sum(more) > 0)
    def others():
        other_windows(plan, info, more, collect)

    @pl.when(jnp.logical_not(simple))
    def looped():
        lax.fori_loop(0, groups, gather, 0)

    inner, head, tail, every = [pack_pairs(sums.at[i]) for i in range(4)]
    lanes = lax.rem(iota(inner.shape, 1), HALF)
    inner = jnp.where(lanes <= plan.dims, inner, 0.0)
    every = jnp.where(lanes <= plan.dims, every, 0.0)
    for j in range(plan.gap_rows):
        moved = pltpu.roll(every, (plan.dims + 1 - plan.gap * j) % LANES, 1)
        turned[j] = jnp.where(lanes > plan.dims, moved, 0.0)
    row = iota((plan.part, LANES), 0)

    def put(c, carry):
        gaps = jnp.zeros((plan.part, LANES), f32)
        for q in range(plan.owned_pairs):
            for j in range(plan.gap_rows):
                pair = c * plan.owned_pairs + q
                piece = jnp.broadcast_to(turned[j, pl.ds(pair, 1), :], gaps.shape)
                gaps = gaps + jnp.where(row == q * plan.gap_rows + j, piece, 0.0)
        for q in range(plan.cols):
            p = c * plan.cols + q
            for side in range(2):
                low = side * plan.part

                def write(low=low, p=p):
                    start = p * 3 * plan.part
                    send[pl.ds(start, plan.part), :] = inner[low : low + plan.part] + gaps
                    send[pl.ds(start + plan.part, plan.part), :] = head[low : low + plan.part]
                    send[pl.ds(start + 2 * plan.part, plan.part), :] = tail[low : low + plan.part]

                if isinstance(p, int):
                    if p % 2 == side:
                        write()
                else:
                    pl.when(lax.rem(p, 2) == side)(write)
        return carry

    repeat(plan.rows, put)


def reduce_kernel(plan, info, got, ids, mine, theirs, marks):
    k, part = plan.clusters, plan.part
    shape = (plan.devices, LANES)
    device = iota(shape, 0)

    def of(lane):
        return jnp.broadcast_to(ids[:, lane : lane + 1], shape)

    heads, tails = of(3 * k), of(3 * k + 1)
    me = lax.axis_index("cells") * plan.cols + lax.axis_index("grp")
    other = me + 1 - 2 * lax.rem(me, 2)

    def shifted(value, distance):
        return pltpu.roll(value, distance % plan.devices, 0)

    marks[0], marks[1] = of(3 * k + 2), of(3 * k + 3)
    own = ids[pl.ds(me, 1), :]
    pair = ids[pl.ds(other, 1), :]
    for i, (row, lane) in enumerate(((own, 3 * k), (own, 3 * k + 1), (pair, 3 * k), (pair, 3 * k + 1))):
        batch = jnp.broadcast_to(row[:, lane : lane + 1], shape)
        marks[2 + 2 * i] = jnp.where(heads == batch, 1.0, 0.0)
        marks[3 + 2 * i] = jnp.where(tails == batch, 1.0, 0.0)
    links = []

    def link(hop, to_head, from_head, mine, theirs):
        inside = (device + hop >= 0) & (device + hop < plan.devices)
        at = plan.fixed_marks + len(links)
        marks[at] = jnp.where(inside & (shifted(theirs, -hop) == mine), 1.0, 0.0)
        links.append((at, hop, to_head, from_head))

    for hop in range(1, plan.reach + 1):
        link(-hop, True, False, heads, tails)
        link(hop, False, True, tails, heads)
        if plan.lone:
            link(-hop, False, False, tails, tails)
            link(hop, False, False, tails, tails)

    block = (2 * part, LANES)
    top = iota(block, 0) < part

    def mark(i, r):
        return jnp.broadcast_to(marks[i, pl.ds(r, 1), :], block)

    def two(i, r):
        return jnp.where(top, mark(i, r), mark(i + 1, r))

    def ends_of(r):
        return got[pl.ds(r * 3 * part + part, 2 * part), :]

    def turn(value):
        return pltpu.roll(value, part, 0)

    def gather(r, carry):
        inner, shrunk, sums = carry
        ends = ends_of(r)
        whole = halves(ends, plan.dims)
        for at, hop, to_head, from_head in links:
            if isinstance(r, int):
                if not 0 <= r + hop < plan.devices:
                    continue
                there = r + hop
            else:
                there = jnp.clip(r + hop, 0, plan.devices - 1)
            mass = halves(ends_of(there), plan.dims)
            if to_head != from_head:
                mass = turn(mass)
            whole = whole + jnp.where(top == to_head, mark(at, r) * mass, 0.0)
        ridge = two(0, r)
        shrunk = shrunk + ends * (ridge / (whole + ridge))
        inner = inner + got[pl.ds(r * 3 * part, part), :]
        sums = tuple(total + ends * two(2 + 2 * i, r) for i, total in enumerate(sums))
        return inner, shrunk, sums

    zero = jnp.zeros(block, f32)
    state = (zero[0:part], zero, (zero,) * 4)
    if plan.devices <= 32:
        for r in range(plan.devices):
            state = gather(r, state)
    else:
        state = lax.fori_loop(0, plan.devices, gather, state)
    inner, shrunk, sums = state

    def fold(value):
        return (value + turn(value))[0:part]

    right = inner + fold(shrunk)
    intercept = right / (1.0 + halves(right, plan.dims))
    mine[0] = jnp.concatenate([intercept, intercept], axis=0)
    theirs[0:part] = intercept
    for i in range(2):
        value = sums[i] + turn(sums[i])
        mine[1 + i] = value
        theirs[(1 + i) * part : (2 + i) * part] = fold(sums[2 + i])
    mine[3] = jnp.concatenate([inner, inner], axis=0)


def correct_kernel(
    plan, info, ridges, mine, theirs, a1, a2, moments, places, xs, out_hbm, centroids_hbm,
    slopes, rows, spread, out, centroids, sems, done,
):
    k, part = plan.clusters, plan.part
    first, last, segments = info[0], info[1], info[2]
    groups = lax.div(segments + plan.group - 1, plan.group)
    me = lax.axis_index("cells") * plan.cols + lax.axis_index("grp")
    odd = jnp.full((plan.pairs, LANES), lax.rem(me, 2)) == 1
    low = iota((plan.pairs, LANES), 0) < part

    def both(i):
        piece = theirs[i * part : (i + 1) * part]
        piece = jnp.concatenate([piece, piece], axis=0)
        return unpack_pairs(spread, jnp.where(low != odd, mine[i], piece))

    intercept, first_sum, last_sum = both(0), both(1), both(2)
    def slope(g, carry):
        start = g * plan.depth if isinstance(g, int) else pl.multiple_of(g * plan.depth, plan.depth)
        held = moments[pl.ds(start, plan.depth), :]
        made = []
        for j in range(plan.group):
            s = g * plan.group + j
            part = held[j * k : (j + 1) * k]
            part = jnp.where(s == 0, first_sum, part)
            part = jnp.where(s == segments - 1, last_sum, part)
            mass = lane_of(part, plan.dims)
            ridge = ridges[s]
            made.append((part - mass * intercept) / (mass + ridge))
        for i, piece in enumerate(split(jnp.concatenate(made, axis=0), 2)):
            slopes[i, pl.ds(start, plan.depth), :] = piece
        return carry

    size = plan.window * k

    rows[...] = mine[3]
    lanes = lax.rem(iota((1, LANES), 1), HALF)
    for q in range(plan.owned_pairs):
        every = jnp.zeros((1, LANES), f32)
        for j in range(plan.gap_rows):
            at = q * plan.gap_rows + j
            piece = jnp.where(lanes > plan.dims, rows[at : at + 1], 0.0)
            moved = pltpu.roll(piece, (plan.gap * j - plan.dims - 1) % LANES, 1)
            inside = (lanes >= plan.gap * j) & (lanes < plan.gap * (j + 1))
            every = every + jnp.where(inside, moved, 0.0)
        every = every / (1.0 + halves(every, plan.dims))
        centroids[2 * q : 2 * q + 1] = every[:, 0 : plan.dims]
        centroids[2 * q + 1 : 2 * q + 2] = pltpu.roll(every, HALF, 1)[:, 0 : plan.dims]
    last_copy = pltpu.make_async_copy(centroids, centroids_hbm, done)
    last_copy.start()
    copies = []
    span = plan.cells // plan.sends
    for c in range(plan.sends):
        at = slice(c * span, (c + 1) * span)
        copies.append(pltpu.make_async_copy(out.at[:, at], out_hbm.at[:, at], sems.at[c]))

    def moved(c, base):
        at = slice(c * plan.piece, (c + 1) * plan.piece)
        rows_of = pl.ds(pl.multiple_of(base * k, k), size)
        large, fine = slopes[0, rows_of, 0:HALF], slopes[1, rows_of, 0:HALF]
        return lax.dot_general(
            jnp.concatenate([large, fine, large], axis=0),
            masked(plan, a1, a2, places, base, at, (0, 0, 1)),
            BY_ROWS,
            preferred_element_type=f32,
        )[0 : plan.dims]

    more = extra_windows(plan, info)

    at_once = TILE // plan.group
    blank = jnp.zeros((plan.depth, LANES), bf16)
    simple = (sum(more) == 0) & (groups <= at_once)

    @pl.when(simple)
    def straight():
        for g in range(at_once):
            slope(g, 0)
        for i in range(2):
            slopes[i, at_once * plan.depth : (at_once + 1) * plan.depth, :] = blank
        for c in range(plan.pieces):
            at = slice(c * plan.piece, (c + 1) * plan.piece)
            out[:, at] = xs[:, at] - moved(c, info[4 + c])
            if (c + 1) * plan.sends % plan.pieces == 0:
                copies[(c + 1) * plan.sends // plan.pieces - 1].start()

    @pl.when(jnp.logical_not(simple))
    def general():
        lax.fori_loop(0, groups, slope, 0)
        for i in range(2):
            slopes[i, pl.ds(pl.multiple_of(groups * plan.depth, plan.depth), plan.depth), :] = blank
        for c in range(plan.pieces):
            at = slice(c * plan.piece, (c + 1) * plan.piece)
            out[:, at] = xs[:, at] - moved(c, info[4 + c])

        def step(c, base):
            at = slice(c * plan.piece, (c + 1) * plan.piece)
            out[:, at] = out[:, at] - moved(c, base)

        other_windows(plan, info, more, step)
        for copy in copies:
            copy.start()

    for copy in copies:
        copy.wait()
    last_copy.wait()


VMEM = pl.BlockSpec(memory_space=pltpu.VMEM)
SMEM = pl.BlockSpec(memory_space=pltpu.SMEM)
WHERE = pl.BlockSpec(memory_space=pltpu.HBM)


def hold_scalars(value):
    return pltpu.with_memory_space_constraint(value, pltpu.SMEM)


def bound(kernel, plan, name):
    def run(*refs):
        kernel(plan, *refs)

    run.__name__ = name
    return run


def body(x, means, scale, lam, pop):
    plan = Plan(x, means, pop)
    k, cells = plan.clusters, plan.cells
    params = pltpu.CompilerParams(vmem_limit_bytes=(16 << 20) if plan.keep else None)

    def kept(shape, kind=f32):
        return pltpu.VMEM(shape, kind) if plan.keep else jax.ShapeDtypeStruct(shape, kind)

    def hold(value):
        return pltpu.with_memory_space_constraint(value, pltpu.VMEM) if plan.keep else value

    send, prior, counts, sizes, places, parts, xs, info, ridges = pl.pallas_call(
        bound(count_kernel, plan, "count"),
        name="count",
        out_shape=(
            kept((plan.devices, plan.width)),
            kept((k, cells)),
            kept((plan.tiles, k, LANES)),
            kept((plan.tiles, LANES)),
            kept((TILE, cells), bf16),
            kept((2 * HALF, cells), bf16),
            kept((plan.dims, cells)),
            pltpu.SMEM((5 + plan.pieces,), i32),
            pltpu.SMEM((plan.local,), f32),
        ),
        in_specs=[WHERE] * 5,
        out_specs=(VMEM,) * 7 + (SMEM,) * 2,
        scratch_shapes=[
            pltpu.SMEM(pop.shape, i32),
            pltpu.SMEM(lam.shape, f32),
            pltpu.SMEM(scale.shape, f32),
            pltpu.VMEM(means.shape, f32),
            pltpu.SMEM((plan.batches,), i32),
            pltpu.VMEM((k, LANES), f32),
            pltpu.VMEM((8, cells), f32),
            pltpu.SemaphoreType.DMA((plan.chunks,)),
            pltpu.SemaphoreType.DMA((4,)),
        ],
    )(pop, lam, scale, means, x)
    prior, counts, sizes, places, parts, xs = map(hold, (prior, counts, sizes, places, parts, xs))
    info, ridges = hold_scalars(info), hold_scalars(ridges)
    ids = hold(lax.all_to_all(send, AXES, 0, 0, tiled=True))
    send, a1, a2, moments = pl.pallas_call(
        bound(moment_kernel, plan, "moment"),
        name="moment",
        compiler_params=params,
        out_shape=(
            kept((plan.devices * 3 * plan.part, LANES)),
            kept((k, cells), bf16),
            kept((k, cells), bf16),
            kept((plan.table, LANES)),
        ),
        in_specs=[SMEM] * 2 + [VMEM] * 6,
        out_specs=(VMEM,) * 4,
        scratch_shapes=[
            pltpu.VMEM((k, cells), f32),
            pltpu.VMEM((4, k, LANES), f32),
            pltpu.VMEM((plan.gap_rows, plan.pairs, LANES), f32),
        ],
    )(info, ridges, ids, prior, counts, sizes, places, parts)
    a1, a2, moments = map(hold, (a1, a2, moments))
    rows = send.shape[0]
    got = lax.all_to_all(send.reshape(rows, 1, LANES), AXES, 0, 0, tiled=True)
    got = hold(got.reshape(rows, LANES))
    marks = plan.fixed_marks + plan.reach * (4 if plan.lone else 2)
    mine, theirs = pl.pallas_call(
        bound(reduce_kernel, plan, "reduce"),
        name="reduce",
        compiler_params=params,
        out_shape=(kept((4, plan.pairs, LANES)), kept((3 * plan.part, LANES))),
        in_specs=[SMEM] + [VMEM] * 2,
        out_specs=(VMEM,) * 2,
        scratch_shapes=[pltpu.VMEM((marks, plan.devices, LANES), f32)],
    )(info, got, ids)
    mine = hold(mine)
    swap = [(i, i + 1 - 2 * (i % 2)) for i in range(plan.devices)]
    theirs = hold(lax.ppermute(theirs, AXES, swap))
    corrected, centroids = pl.pallas_call(
        bound(correct_kernel, plan, "correct"),
        name="correct",
        compiler_params=params,
        out_shape=(
            jax.ShapeDtypeStruct(x.shape, f32),
            jax.ShapeDtypeStruct((k // plan.rows, plan.dims), f32),
        ),
        in_specs=[SMEM] * 2 + [VMEM] * 7,
        out_specs=(WHERE, WHERE),
        scratch_shapes=[
            pltpu.VMEM((2, plan.table, LANES), bf16),
            pltpu.VMEM((plan.pairs, LANES), f32),
            pltpu.VMEM((k, LANES), f32),
            pltpu.VMEM((plan.dims, cells), f32),
            pltpu.VMEM((k // plan.rows, plan.dims), f32),
            pltpu.SemaphoreType.DMA((plan.sends,)),
            pltpu.SemaphoreType.DMA,
        ],
    )(info, ridges, mine, theirs, a1, a2, moments, places, xs)
    return corrected, centroids


def solution(mesh):
    return jax.shard_map(
        body,
        mesh=mesh,
        in_specs=(P(None, AXES), P(), P(), P(), P()),
        out_specs=(P(None, AXES), P("cells", None)),
        check_vma=False,
    )
```
